256 devices in a mesh: head: 64 (over x, z, y_lo), client: 4 (over y_hi, core).
Axes of the slice: x: 4, y: 4 (y_hi: 2, y_lo: 2; y = y_hi * 2 + y_lo), z: 8, core: 2. Of those that a mesh axis runs over, the one named last changes fastest.
Arguments:
- client_ids: int32 [256], replicated, may hold values from 0 to 1023, as said below
- client_table: bfloat16 [1024, 256], replicated, may hold values from -6 to 6
- in_weight: bfloat16 [256, 4096], P(None, 'client'), may hold values from -0.375 to 0.375
- in_bias: float32 [4096], P('client'), may hold values from -3 to 3
- head_weight: bfloat16 [4096, 131072], P('client', 'head'), may hold values from -0.09375 to 0.09375
- tokens: int32 [256, 256], P(('head', 'client')), may hold values from 0 to 255
- labels: int32 [256, 256], P(('head', 'client')), may hold values from 0 to 255
- byte_table: bfloat16 [256, 4096], P(None, 'client'), may hold values from -5.5 to 6.7
- out_table: bfloat16 [256, 4096], P(None, 'client'), may hold values from -5.625 to 5.625
Outputs:
- head_grad: bfloat16 [4096, 131072], P('client', 'head')
- in_grad: float32 [256, 4096], P(None, 'client')
- losses: float32 [256], P(('head', 'client'))
The draws below stay inside these ranges and needn't reach their ends.
Inputs may be any that keep to these rules, and one draw needn't show every extreme that they name: `client_ids`: distinct population indices.
All inputs are finite; a program needn't handle non-finite values.
Results may differ from the reference program's by a relative error of at most 0.0085.
Values may be sent and summed in bfloat16 or wider, within the bound.
A program may use at most 64 MiB of HBM per device.

```python
import jax
import jax.numpy as jnp
from jax import lax

H = 4096
E = 256
D = 4096
VOCAB = 256
SEQ = 256
CLIENTS = 256
NPOP = 1024
P_SIZE = 131072


def draw_client_ids(key, part):
    return jax.random.permutation(key, NPOP)[:CLIENTS].astype(jnp.int32)


def table_parts(key):
    noise_key = jax.random.fold_in(jax.random.fold_in(key, 7), 0)
    values = jnp.clip(jax.random.normal(noise_key, (VOCAB, D), jnp.float32), -5.5, 5.5)
    return values


def draw_byte_table(key, part):
    values = table_parts(key)
    return values.astype(jnp.bfloat16)


def draw_out_table(key, part):
    values = jnp.clip(jax.random.normal(jax.random.fold_in(key, 11), (VOCAB, D), jnp.float32), -5.5, 5.5)
    return values.astype(jnp.bfloat16)


def touch_ends(entries, key, low, largest):
    spot = [jax.random.randint(jax.random.fold_in(key, axis), (), 0, length) for axis, length in enumerate(entries.shape)]
    widest = entries.shape.index(max(entries.shape))
    next_to = spot[:widest] + [(spot[widest] + 1) % entries.shape[widest]] + spot[widest + 1:]
    return entries.at[tuple(spot)].set(low).at[tuple(next_to)].set(largest)


def level_of(stream_key, dims, pieces, low, top_value):
    level, own = 1.0, jax.random.fold_in(stream_key, 6)
    for position, shards_of in pieces:
        heights = jnp.exp(jax.random.uniform(jax.random.fold_in(own, position), (shards_of,), jnp.float32, low / len(pieces), top_value / len(pieces)))
        level = level * jnp.repeat(heights, dims[position] // shards_of).reshape([-1 if axis == position else 1 for axis in range(len(dims))])
    return level


def scatter_about(own_key, dims, scale, limit, shards=(), held_as=jnp.bfloat16):
    loudness = level_of(own_key, dims, shards, -0.22, 0.18) if shards else 1.0
    entries = jax.random.normal(own_key, dims, jnp.float32) * scale * loudness
    return jnp.minimum(jnp.maximum(entries, -limit), limit).astype(held_as)


def setup_inputs(seed: int = 0) -> dict:
    keys = jax.random.split(jax.random.key(seed), 10)
    client_ids = draw_client_ids(jax.random.fold_in(keys[9], 71), 0)
    client_table = scatter_about(keys[1], (NPOP, E), 1.0, 6.0)
    in_weight = scatter_about(keys[2], (E, H), E ** -0.5, 0.375, ((1, 4),))
    in_bias = scatter_about(keys[3], (H,), 0.5, 3.0, ((0, 4),), jnp.float32)
    head_weight = scatter_about(keys[4], (H, P_SIZE), H ** -0.5, 0.09375, ((0, 4), (1, 64)))
    tokens = touch_ends(jax.random.randint(keys[5], (CLIENTS, SEQ), 0, VOCAB), jax.random.fold_in(keys[5], 1), 0, VOCAB - 1).astype(jnp.int32)
    labels = touch_ends(jax.random.randint(keys[6], (CLIENTS, SEQ), 0, VOCAB), jax.random.fold_in(keys[6], 1), 0, VOCAB - 1).astype(jnp.int32)
    byte_table = draw_byte_table(jax.random.fold_in(keys[9], 71), 0)
    out_table = draw_out_table(jax.random.fold_in(keys[9], 71), 0)
    return dict(client_ids=client_ids, client_table=client_table, in_weight=in_weight, in_bias=in_bias, head_weight=head_weight, tokens=tokens, labels=labels, byte_table=byte_table, out_table=out_table)


EPSILON = 1e-06
learn_rate = 0.1

def client_loss(factor_a, factor_b, inputs, label_row, out_table):
    depth = factor_a.shape[0]
    rank_size = factor_a.shape[1]
    normed_in = inputs * lax.rsqrt(lax.optimization_barrier(jnp.mean(inputs * inputs, -1, keepdims=True)) + EPSILON)
    low_rank = jnp.dot(normed_in, factor_a, precision=lax.Precision.HIGHEST)
    adapted = inputs + jnp.dot(low_rank, factor_b, precision=lax.Precision.HIGHEST) / jnp.sqrt(jnp.float32(depth * rank_size))
    normed = (adapted * lax.rsqrt(lax.optimization_barrier(jnp.mean(adapted * adapted, -1, keepdims=True)) + EPSILON)).astype(jnp.bfloat16)
    logits = lax.dot_general(normed, out_table, (((1,), (1,)), ((), ())), preferred_element_type=jnp.float32)
    logits = logits * (4.0 / jnp.sqrt(jnp.float32(depth)))
    log_total = jax.nn.logsumexp(logits, -1)
    vocab_ids = lax.broadcasted_iota(jnp.int32, logits.shape, 1)
    picked = lax.optimization_barrier(jnp.sum(jnp.where(vocab_ids == label_row[:, None], logits, 0.0), -1))
    return jnp.sum(log_total - picked)

def train_client(factor_row, token_row, label_row, byte_table, out_table):
    depth = byte_table.shape[1]
    split_at = factor_row.shape[0] // 2
    rank_size = split_at // depth
    start_a = factor_row[:split_at].reshape(depth, rank_size).astype(jnp.float32)
    start_b = factor_row[split_at:].reshape(rank_size, depth).astype(jnp.float32)
    onehot = (token_row[:, None] == lax.broadcasted_iota(jnp.int32, (token_row.shape[0], byte_table.shape[0]), 1)).astype(jnp.bfloat16)
    inputs = jnp.dot(onehot, byte_table, preferred_element_type=jnp.float32)
    loss_grad = jax.value_and_grad(client_loss, argnums=(0, 1))
    first_loss, (grad_a, grad_b) = loss_grad(start_a, start_b, inputs, label_row, out_table)
    middle_a = start_a - learn_rate * grad_a
    middle_b = start_b - learn_rate * grad_b
    second_loss, (grad_a, grad_b) = loss_grad(middle_a, middle_b, inputs, label_row, out_table)
    final_a = middle_a - learn_rate * grad_a
    final_b = middle_b - learn_rate * grad_b
    deltas = jnp.concatenate([(final_a - start_a).reshape(-1), (final_b - start_b).reshape(-1)]).astype(jnp.bfloat16)
    return (deltas, first_loss / token_row.shape[0])

def reference(client_ids, client_table, in_weight, in_bias, head_weight, tokens, labels, byte_table, out_table):
    chosen = client_table[client_ids]
    preact = jnp.dot(chosen, in_weight, preferred_element_type=jnp.float32) + in_bias
    hidden = jnp.maximum(preact, 0.0).astype(jnp.bfloat16)
    factors = jnp.dot(hidden, head_weight, preferred_element_type=jnp.float32).astype(jnp.bfloat16)
    blocks = CLIENTS // 8

    def run_block(record):
        return jax.vmap(lambda fac, tok, lab: train_client(fac, tok, lab, byte_table, out_table))(record[0], record[1], record[2])
    deltas, losses = lax.map(run_block, (factors.reshape(blocks, 8, -1), tokens.reshape(blocks, 8, -1), labels.reshape(blocks, 8, -1)))
    deltas = deltas.reshape(CLIENTS, -1)
    losses = losses.reshape(CLIENTS)
    head_grad = lax.dot_general(hidden, deltas, (((0,), (0,)), ((), ())), preferred_element_type=jnp.float32).astype(jnp.bfloat16)
    hidden_back = lax.dot_general(deltas, head_weight, (((1,), (1,)), ((), ())), preferred_element_type=jnp.float32)
    masked = jnp.where(preact > 0, hidden_back, 0.0)
    in_grad = lax.dot_general(chosen.astype(jnp.float32), masked, (((0,), (0,)), ((), ())), precision=lax.Precision.HIGHEST)
    return (head_grad, in_grad, losses)
```

```python
import jax
import jax.numpy as jnp
from jax import lax
from jax.experimental import pallas as pl
from jax.experimental.pallas import tpu as pltpu
from jax.sharding import PartitionSpec as P

EPS = 1e-6
ETA = 0.1
F32 = jnp.float32
BF = jnp.bfloat16
MESH = pl.DeviceIdType.MESH
CH = 4
CW = 2048 // CH


def mm(a, b, ca, cb):
    return lax.dot_general(
        a.astype(BF), b.astype(BF), (((ca,), (cb,)), ((), ())), preferred_element_type=F32
    )


def iota(shape, dim):
    return lax.broadcasted_iota(jnp.int32, shape, dim)


def gradients(pt, qt, rt, s_mat, obt, bb, scale, ct, cnt):
    tt = pt * (scale * (1 / 256))
    st = mm(s_mat, tt, 1, 0)
    msq = (bb + jnp.sum(tt * (2 * rt + st), 0, keepdims=True)) * (1 / 4096)
    q = lax.rsqrt(msq + EPS)
    mt = obt + mm(qt, tt, 0, 0)
    lg = mt * (q * (1 / 16))
    top = jnp.max(lg, 0, keepdims=True)
    ex = jnp.exp(lg - top)
    total = jnp.sum(ex, 0, keepdims=True)
    gt = (ex * (cnt / total) - ct) * (1 / 16)
    along = jnp.sum(gt * mt, 0, keepdims=True)
    e = q * q * q * along * (1 / 4096)
    ht = gt * q
    dt = mm(qt, ht, 1, 0) - e * (rt + st)
    ut = dt * (scale * (1 / 256))
    xt = mm(tt, ht, 1, 1)
    yt = tt * e
    z = mm(yt, tt, 1, 1)
    loss = jnp.sum(cnt * (top + jnp.log(total)) - jnp.sum(ct * lg, 0, keepdims=True))
    return ut, xt, yt, z, loss


def two_steps(pt, qt, rt, s_mat, obt, oo, bbm, bb, scale, ct, cnt):
    u1, x1, y1, z1, loss = gradients(pt, qt, rt, s_mat, obt, bb, scale, ct, cnt)
    vo = -ETA * mm(x1, oo, 1, 0) + ETA * mm(y1, obt, 1, 1)
    vb = -ETA * mm(x1, obt, 1, 0) + ETA * mm(y1, bbm, 1, 0)
    z1 = ETA * z1
    p2 = pt - ETA * mm(u1, bbm, 1, 0)
    q2 = qt + mm(z1, qt, 1, 0) + vo
    r2 = rt + mm(z1, rt, 1, 0) + vb
    h = -ETA * mm(qt, x1, 1, 1) + ETA * mm(rt, y1, 1, 1)
    ht = -ETA * mm(x1, qt, 1, 1) + ETA * mm(y1, rt, 1, 1)
    vv = -ETA * mm(x1, vo, 1, 1) + ETA * mm(y1, vb, 1, 1)
    zs = mm(z1, s_mat, 1, 0)
    s2 = s_mat + zs + mm(s_mat, z1, 1, 1) + mm(zs, z1, 1, 1)
    s2 = s2 + h + mm(z1, h, 1, 0) + ht + mm(ht, z1, 1, 1) + vv
    u2, x2, y2, z2, _ = gradients(p2, q2, r2, s2, obt, bb, scale, ct, cnt)
    z2 = ETA * z2
    u = -ETA * (u1 + u2)
    x = -ETA * (x1 + mm(z2, x1, 1, 0) + x2)
    y = ETA * (y1 + mm(z2, y1, 1, 0) + y2)
    z = z1 + z2 + mm(z2, z1, 1, 0)
    return u, x, y, z, loss


def kernel(
    ids, table, inw, bias, w_hbm, tok, lab, byte, outt,
    ing_o, dn, hid, loss_o,
    w, fs, fr, sb, r2, ft, f, rx, la, lb, xf, bp, gp, gq, gn, ms, er, cm, cr, ta, tx, g_in, d_in,
    hb, a1, a1s, a2, ag, hidt, chosen_s,
    sw, r1s, r1r, r2s, r2r, gss, gsr, r3s, r3r, e1s, e1r, e2s, e2r, r4s, r4r, r5s, r5r, r6s, r6r,
    p1s, p1r, p2s, p2r, p3s, p3r, p4s, p4r,
):
    head = lax.axis_index("head")
    grp = lax.axis_index("client")
    x, z, lo = head // 16, (head // 2) % 8, head % 2
    hi, k = grp // 2, grp % 2
    p = (hi + lo) % 2

    def dev(x_, z_, lo_, hi_, k_):
        return (x_ * 16 + z_ * 2 + lo_, hi_ * 2 + k_)

    def remote(src, dst, ss, rs, to):
        return pltpu.make_async_remote_copy(
            src_ref=src, dst_ref=dst, send_sem=ss, recv_sem=rs, device_id=to, device_id_type=MESH
        )

    partner = dev(x, z, lo, hi, 1 - k)
    n1 = dev(x, z, 1 - lo, hi, k)
    n2 = dev(x, z, 1 - lo, 1 - hi, k)

    wc = []
    for i in range(CH):
        c = pltpu.make_async_copy(
            w_hbm.at[:, pl.ds(i * CW, CW)], w.at[:, pl.ds(i * CW, CW)], sw.at[i]
        )
        c.start()
        wc.append(c)

    bar = pltpu.get_barrier_semaphore()

    def greet(i, _):
        x_, z_ = i // 32, (i // 4) % 8
        hi_, k_ = (i // 2) % 2, i % 2
        lo_ = (p + hi_) % 2
        same = (x_ == x) & (z_ == z) & (hi_ == hi) & (k_ == k)

        @pl.when(jnp.logical_not(same))
        def _():
            pl.semaphore_signal(bar, inc=1, device_id=dev(x_, z_, lo_, hi_, k_), device_id_type=MESH)

        return 0

    lax.fori_loop(0, 128, greet, 0)
    for dx in range(4):
        pl.semaphore_signal(
            bar, inc=1, device_id=dev((x + dx) % 4, z, 1 - lo, hi, k), device_id_type=MESH
        )

    m = iota((256, 256), 1)
    mhi, mxz, mp, mk = m % 2, (m // 2) % 32, (m // 64) % 2, m // 128
    owner = (mxz * 2 + (mp + mhi) % 2) * 4 + mhi * 2 + mk
    order = (iota((256, 256), 0) == owner).astype(BF)
    picks = (iota((1024, 256), 0) == ids[...]).astype(F32).astype(BF)
    picks = mm(picks, order, 1, 0)
    chosen = mm(picks, table[...], 0, 0).astype(BF)
    chosen_s[...] = chosen
    pre = mm(chosen, inw[...], 1, 0) + bias[...]
    hidden = jnp.maximum(pre, 0.0)
    hid[...] = hidden.astype(BF)

    pl.semaphore_wait(bar, 131)

    c1 = []
    for i in range(CH):
        cols = pl.ds(i * CW, CW)
        wc[i].wait()
        fs[:, cols] = jnp.dot(hid[...], w[:, cols], preferred_element_type=F32)
        c = remote(
            fs.at[pl.ds((1 - k) * 128, 128), cols], fr.at[:, cols], r1s.at[i], r1r.at[i], partner
        )
        c.start()
        c1.append(c)
    c2 = []
    for i in range(CH):
        cols = pl.ds(i * CW, CW)
        c1[i].wait_recv()
        sb[:, cols] = (fs[pl.ds(pl.multiple_of(k * 128, 128), 128), cols] + fr[:, cols]).astype(BF)
        a = remote(
            sb.at[pl.ds((1 - p) * 64, 64), cols], r2.at[0, :, cols], r2s.at[0, i], r2r.at[0, i], n1
        )
        b = remote(
            sb.at[pl.ds(p * 64, 64), cols], r2.at[1, :, cols], r2s.at[1, i], r2r.at[1, i], n2
        )
        a.start()
        b.start()
        c2.append((a, b))

    gp[0:256, :] = mm(outt[...], byte[...], 1, 1)
    gp[256:512, :] = mm(outt[...], outt[...], 1, 1)
    gp[512:768, :] = mm(byte[...], byte[...], 1, 1)
    cg = remote(gp, gq, gss.at[0], gsr.at[0], partner)
    cg.start()
    for d8 in range(8):
        perm = (iota((1024, 128), 0) == 8 * iota((1024, 128), 1) + d8).astype(F32)
        bp[:, d8 * 128 : (d8 + 1) * 128] = mm(byte[...], perm, 1, 0).astype(BF)
    hidt[...] = jnp.transpose(hidden).astype(BF)
    cg.wait()
    gp[...] = gp[...] + gq[...]
    half = pl.ds(pl.multiple_of(k * 384, 384), 384)
    cg2 = remote(gp.at[half], gn.at[half], gss.at[1], gsr.at[1], n2)
    cg2.start()

    is_a = x < 2
    slots = [jnp.where(is_a, ((z % 4) * 2 + 1 - lo) * 2 + q, 16 + 8 * (x - 2) + z) for q in range(2)]
    hi_d = jnp.where(is_a, x, 1 - lo)
    lo_d = (p + hi_d) % 2
    cores = [jnp.where(is_a, z // 4, q) for q in range(2)]
    per = CH // 2
    for q in range(2):
        for i in range(q * per, (q + 1) * per):
            cols = pl.ds(i * CW, CW)
            c2[i][0].wait_recv()
            c2[i][1].wait_recv()
            both = r2[0, :, cols].astype(F32) + r2[1, :, cols].astype(F32)
            for jj in range(CW // 128):
                j = (i * (CW // 128) + jj) % 8
                ft[q, pl.ds(j, 64, stride=8), :] = both[:, jj * 128 : (jj + 1) * 128]
        f[pl.ds(q * 32, 32)] = ft[q].astype(BF).reshape(32, 2, 8, 128)

        def send(i, _, q=q):
            x_, z_ = (x + i // 8) % 4, (z + i % 8) % 8
            same = (i == 0) & (hi_d == hi) & (cores[q] == k)

            @pl.when(jnp.logical_not(same))
            def _():
                remote(
                    f.at[q * 32 + x_ * 8 + z_], rx.at[k, :, slots[q]], r3s, r3r,
                    dev(x_, z_, lo_d, hi_d, cores[q]),
                ).start()

            return 0

        lax.fori_loop(0, 32, send, 0)
    mine = [(hi_d == hi) & (cores[q] == k) for q in range(2)]
    n_self = mine[0].astype(jnp.int32) + mine[1].astype(jnp.int32)
    for q in range(2):

        @pl.when(mine[q])
        def _(q=q):
            rx[k, :, slots[q]] = f[q * 32 + x * 8 + z]

    def wait_all(n_self, sem):
        for n in range(3):

            @pl.when(n_self == n)
            def _(n=n):
                piece = f.at[pl.ds(0, 64 - n)]
                pltpu.make_async_copy(piece, piece, sem).wait()

    wait_all(n_self, r3r)

    for c in range(4):
        at = jnp.transpose(rx[c // 2, c % 2, 0:16].astype(F32).reshape(128, 128))
        for d8 in range(8):
            la[c * 16 : (c + 1) * 16, d8 * 128 : (d8 + 1) * 128] = at[d8 * 16 : (d8 + 1) * 16].astype(BF)
        xf[c * 128 : (c + 1) * 128, :] = rx[c // 2, c % 2, 16:32].astype(F32).reshape(128, 128)
    for j in range(8):
        lb[:, j * 128 : (j + 1) * 128] = xf[pl.ds(j, 64, stride=8), :].astype(BF)
    pt = mm(la[...], bp[...], 1, 1)
    qt = mm(lb[...], outt[...], 1, 1)
    rt = mm(lb[...], byte[...], 1, 1)
    ss = mm(lb[...], lb[...], 1, 1)
    for c in range(4):
        rows = slice(c * 16, (c + 1) * 16)
        ms[c, 0:16, :] = pt[rows].astype(BF)
        ms[c, 16:32, :] = qt[rows].astype(BF)
        ms[c, 32:48, :] = rt[rows].astype(BF)
        ms[c, 48:64, :] = jnp.zeros((16, 256), BF)
        ms[c, 48:64, 0:16] = ss[rows, c * 16 : (c + 1) * 16].astype(BF)
    me = k * 2 + hi

    def member(o):
        k_, hi_ = (k + o // 2) % 2, (hi + o % 2) % 2
        return k_ * 2 + hi_, dev(x, z, (p + hi_) % 2, hi_, k_)

    ce = []
    for o in range(1, 4):
        c_, to = member(o)
        c = remote(ms.at[c_], er.at[o], e1s.at[o], e1r.at[o], to)
        c.start()
        ce.append(c)

    cg2.wait()
    cg3 = remote(gn.at[half], gn.at[half], gss.at[2], gsr.at[2], partner)
    cg3.start()
    tok_hot = (iota((256, 256), 0) == tok[...]).astype(F32)
    lab_hot = (iota((256, 256), 0) == lab[...]).astype(F32)
    ct = mm(lab_hot, tok_hot, 1, 1)
    cnt = jnp.sum(ct, 0, keepdims=True)
    cg3.wait()
    gram = gp[...] + gn[...]
    obt, oo, bbm = gram[0:256], gram[256:512], gram[512:768]
    diag = iota((256, 256), 0) == iota((256, 256), 1)
    bb = jnp.sum(jnp.where(diag, bbm, 0.0), 0, keepdims=True)
    scale = lax.rsqrt(bb * (1 / 4096) + EPS)
    own = ms[me].astype(F32)
    for c in ce:
        c.wait_recv()
    for o in range(1, 4):
        own = own + er[o].astype(F32)
    u, xx, yy, zz, loss = two_steps(
        own[0:16], own[16:32], own[32:48], own[48:64, 0:16], obt, oo, bbm, bb, scale, ct, cnt
    )
    loss_o[0] = loss * (1 / 256)
    cm[0:16, :] = u.astype(BF)
    cm[16:32, :] = xx.astype(BF)
    cm[32:48, :] = yy.astype(BF)
    cm[48:64, :] = jnp.zeros((16, 256), BF)
    cm[48:64, 0:16] = zz.astype(BF)
    cc = []
    for o in range(1, 4):
        _, to = member(o)
        c = remote(cm, cr.at[me], e2s.at[o], e2r.at[o], to)
        c.start()
        cc.append(c)
    cr[me] = cm[...]
    for c in cc:
        c.wait_recv()

    allc = cr[...]
    us = allc[:, 0:16].reshape(64, 256)
    xs = allc[:, 16:32].reshape(64, 256)
    ys = allc[:, 32:48].reshape(64, 256)
    dat = mm(us, bp[...], 1, 0)
    for c in range(4):
        for d8 in range(8):
            ta[d8 * 16 : (d8 + 1) * 16, :] = dat[c * 16 : (c + 1) * 16, d8 * 128 : (d8 + 1) * 128]
        tx[c // 2, c % 2, 0:16] = jnp.transpose(ta[...]).astype(BF).reshape(16, 8, 128)
    dbs = mm(xs, outt[...], 1, 0) + mm(ys, byte[...], 1, 0)
    zdb = [mm(cr[c, 48:64, 0:16], lb[c * 16 : (c + 1) * 16, :], 1, 0) for c in range(4)]
    dbs = dbs + jnp.concatenate(zdb, axis=0)
    for j in range(8):
        xf[pl.ds(j, 64, stride=8), :] = dbs[:, j * 128 : (j + 1) * 128]
    for c in range(4):
        tx[c // 2, c % 2, 16:32] = xf[c * 128 : (c + 1) * 128, :].astype(BF).reshape(16, 8, 128)

    spot = x * 8 + z

    def giver(s):
        if_a = s < 16
        b = s // 2
        r = s - 16
        x_ = jnp.where(if_a, hi, 2 + r // 8)
        z_ = jnp.where(if_a, k * 4 + b // 2, r % 8)
        lo_ = jnp.where(if_a, 1 - b % 2, 1 - hi)
        hi_ = (p + lo_) % 2
        q_ = jnp.where(if_a, s % 2, k)
        return x_, z_, lo_, hi_, q_

    def give(i, _):
        s, k_ = i // 2, i % 2
        x_, z_, lo_, hi_, q_ = giver(s)
        same = (x_ == x) & (z_ == z) & (hi_ == hi) & (k_ == k)

        @pl.when(jnp.logical_not(same))
        def _():
            remote(
                tx.at[k_, :, s], g_in.at[q_ * 32 + spot], r4s, r4r, dev(x_, z_, lo_, hi_, k_)
            ).start()

        return 0

    lax.fori_loop(0, 64, give, 0)
    for q in range(2):

        @pl.when(mine[q])
        def _(q=q):
            g_in[q * 32 + spot] = tx[k, :, slots[q]]

    wait_all(n_self, r4r)

    c5 = []
    for n, to in enumerate((n1, n2)):
        c = remote(g_in, d_in.at[k, p], r5s.at[n], r5r.at[n], to)
        c.start()
        c5.append(c)
    c6 = []
    for n in range(2):
        c5[n].wait_recv()
        from_p = (p + 1 + n) % 2
        c = remote(d_in.at[k, from_p], d_in.at[k, from_p], r6s.at[n], r6r.at[n], partner)
        c.start()
        c6.append(c)
    for n in range(2):
        c6[n].wait_recv()
    for kp in range(4):
        xd = d_in[kp // 2, kp % 2].astype(F32).reshape(1024, 128)
        ft[0] = xd[0:512]
        ft[1] = xd[512:1024]
        for j in range(16):
            dn[kp * 64 : (kp + 1) * 64, j * 128 : (j + 1) * 128] = ft[
                j // 8, pl.ds(j % 8, 64, stride=8), :
            ].astype(BF)

    for i in range(4):
        rows = slice(i * 256, (i + 1) * 256)
        hb[rows, :] = mm(w[rows, :], dn[...], 1, 1).astype(BF)
    ca = []
    for o in range(1, 8):
        x_, lo_ = (x + o // 2) % 4, (lo + o % 2) % 2
        rows = pl.ds(pl.multiple_of(x_ * 256 + lo_ * 128, 128), 128)
        c = remote(hb.at[rows], a1.at[o], p1s.at[o], p1r.at[o], dev(x_, z, lo_, hi, k))
        c.start()
        ca.append(c)
    base = pl.multiple_of(x * 256 + lo * 128, 128)
    acc = hb[pl.ds(base, 128), :].astype(F32)
    for o in range(1, 8):
        ca[o - 1].wait_recv()
        acc = acc + a1[o].astype(F32)
    a1s[...] = acc.astype(BF)
    cb = []
    for o in range(1, 8):
        z_ = (z + o) % 8
        c = remote(
            a1s.at[pl.ds(pl.multiple_of(z_ * 16, 16), 16)], a2.at[o], p2s.at[o], p2r.at[o],
            dev(x, z_, lo, hi, k),
        )
        c.start()
        cb.append(c)
    total = a1s[pl.ds(pl.multiple_of(z * 16, 16), 16), :].astype(F32)
    for o in range(1, 8):
        cb[o - 1].wait_recv()
        total = total + a2[o].astype(F32)
    row0 = pl.multiple_of(base + z * 16, 16)
    total = jnp.where(hidt[pl.ds(row0, 16), :].astype(F32) > 0, total, 0.0)
    big = total.astype(BF)
    small = (total - big.astype(F32)).astype(BF)
    piece = mm(big, chosen_s[...], 1, 0) + mm(small, chosen_s[...], 1, 0)
    ag[pl.ds(row0, 16), :] = piece.astype(BF)
    cd = []
    for o in range(1, 8):
        own_rows = ag.at[pl.ds(row0, 16)]
        c = remote(own_rows, own_rows, p3s.at[o], p3r.at[o], dev(x, (z + o) % 8, lo, hi, k))
        c.start()
        cd.append(c)
    for c in cd:
        c.wait_recv()
    cf = []
    for o in range(1, 8):
        x_, lo_ = (x + o // 2) % 4, (lo + o % 2) % 2
        own_rows = ag.at[pl.ds(base, 128)]
        c = remote(own_rows, own_rows, p4s.at[o], p4r.at[o], dev(x_, z, lo_, hi, k))
        c.start()
        cf.append(c)
    for c in cf:
        c.wait_recv()
    ing_o[...] = jnp.transpose(ag[...].astype(F32))

    for c in c1 + [c for ab in c2 for c in ab] + ce + cc + c5 + c6 + ca + cb + cd + cf:
        c.wait_send()
    wait_all(n_self, r3s)
    wait_all(n_self, r4s)


def local(client_ids, client_table, in_weight, in_bias, head_weight, tokens, labels, byte_table, out_table):
    vmem = pl.BlockSpec(memory_space=pltpu.VMEM)
    dma = pltpu.SemaphoreType.DMA
    V = pltpu.VMEM
    in_grad, dn, hid, losses = pl.pallas_call(
        kernel,
        out_shape=(
            jax.ShapeDtypeStruct((256, 1024), F32),
            jax.ShapeDtypeStruct((256, 2048), BF),
            jax.ShapeDtypeStruct((256, 1024), BF),
            jax.ShapeDtypeStruct((1,), F32),
        ),
        in_specs=[vmem] * 4 + [pl.BlockSpec(memory_space=pl.ANY)] + [vmem] * 4,
        out_specs=(vmem, vmem, vmem, pl.BlockSpec(memory_space=pltpu.SMEM)),
        scratch_shapes=[
            V((1024, 2048), BF),
            V((256, 2048), F32),
            V((128, 2048), F32),
            V((128, 2048), BF),
            V((2, 64, 2048), BF),
            V((2, 512, 128), F32),
            V((64, 2, 8, 128), BF),
            V((2, 2, 32, 8, 128), BF),
            V((64, 1024), BF),
            V((64, 1024), BF),
            V((512, 128), F32),
            V((256, 1024), BF),
            V((768, 256), F32),
            V((768, 256), F32),
            V((768, 256), F32),
            V((4, 64, 256), BF),
            V((4, 64, 256), BF),
            V((64, 256), BF),
            V((4, 64, 256), BF),
            V((128, 128), F32),
            V((2, 2, 32, 8, 128), BF),
            V((64, 2, 8, 128), BF),
            V((2, 2, 64, 2, 8, 128), BF),
            V((1024, 256), BF),
            V((8, 128, 256), BF),
            V((128, 256), BF),
            V((8, 16, 256), BF),
            V((1024, 256), BF),
            V((1024, 256), BF),
            V((256, 256), BF),
            dma((CH,)),
            dma((CH,)), dma((CH,)),
            dma((2, CH)), dma((2, CH)),
            dma((3,)), dma((3,)),
            dma(()), dma(()),
            dma((4,)), dma((4,)), dma((4,)), dma((4,)),
            dma(()), dma(()),
            dma((2,)), dma((2,)), dma((2,)), dma((2,)),
            dma((8,)), dma((8,)), dma((8,)), dma((8,)),
            dma((8,)), dma((8,)), dma((8,)), dma((8,)),
        ],
        compiler_params=pltpu.CompilerParams(
            collective_id=0, has_side_effects=True, vmem_limit_bytes=56 * 1024 * 1024
        ),
        name="round",
    )(
        client_ids.reshape(1, 256), client_table, in_weight, in_bias.reshape(1, 1024), head_weight,
        tokens, labels, byte_table, out_table,
    )
    head_grad = lax.dot_general(hid, dn, (((0,), (0,)), ((), ())), preferred_element_type=F32)
    return head_grad.astype(BF), in_grad, losses


def solution(mesh):
    placed = (
        P(),
        P(),
        P(None, "client"),
        P("client"),
        P("client", "head"),
        P(("head", "client"), None),
        P(("head", "client"), None),
        P(None, "client"),
        P(None, "client"),
    )
    return jax.shard_map(
        local,
        mesh=mesh,
        in_specs=placed,
        out_specs=(P("client", "head"), P(None, "client"), P(("head", "client"))),
        check_vma=False,
    )
```

```python
import jax
import jax.numpy as jnp
from jax import lax
from jax.experimental import pallas as pl
from jax.experimental.pallas import tpu as pltpu
from jax.sharding import PartitionSpec as P

EPS = 1e-6
ETA = 0.1
F32 = jnp.float32
BF = jnp.bfloat16
MESH = pl.DeviceIdType.MESH
CH = 4
CW = 2048 // CH


def mm(a, b, ca, cb):
    return lax.dot_general(
        a.astype(BF), b.astype(BF), (((ca,), (cb,)), ((), ())), preferred_element_type=F32
    )


def iota(shape, dim):
    return lax.broadcasted_iota(jnp.int32, shape, dim)


def gradients(pt, qt, rt, s_mat, obt, bb, scale, ct, cnt):
    tt = pt * (scale * (1 / 256))
    st = mm(s_mat, tt, 1, 0)
    msq = (bb + jnp.sum(tt * (2 * rt + st), 0, keepdims=True)) * (1 / 4096)
    q = lax.rsqrt(msq + EPS)
    mt = obt + mm(qt, tt, 0, 0)
    lg = mt * (q * (1 / 16))
    top = jnp.max(lg, 0, keepdims=True)
    ex = jnp.exp(lg - top)
    total = jnp.sum(ex, 0, keepdims=True)
    gt = (ex * (cnt / total) - ct) * (1 / 16)
    along = jnp.sum(gt * mt, 0, keepdims=True)
    e = q * q * q * along * (1 / 4096)
    ht = gt * q
    dt = mm(qt, ht, 1, 0) - e * (rt + st)
    ut = dt * (scale * (1 / 256))
    xt = mm(tt, ht, 1, 1)
    yt = tt * e
    z = mm(yt, tt, 1, 1)
    loss = jnp.sum(cnt * (top + jnp.log(total)) - jnp.sum(ct * lg, 0, keepdims=True))
    return ut, xt, yt, z, loss


def two_steps(pt, qt, rt, s_mat, obt, oo, bbm, bb, scale, ct, cnt):
    u1, x1, y1, z1, loss = gradients(pt, qt, rt, s_mat, obt, bb, scale, ct, cnt)
    vo = -ETA * mm(x1, oo, 1, 0) + ETA * mm(y1, obt, 1, 1)
    vb = -ETA * mm(x1, obt, 1, 0) + ETA * mm(y1, bbm, 1, 0)
    z1 = ETA * z1
    p2 = pt - ETA * mm(u1, bbm, 1, 0)
    q2 = qt + mm(z1, qt, 1, 0) + vo
    r2 = rt + mm(z1, rt, 1, 0) + vb
    h = -ETA * mm(qt, x1, 1, 1) + ETA * mm(rt, y1, 1, 1)
    ht = -ETA * mm(x1, qt, 1, 1) + ETA * mm(y1, rt, 1, 1)
    vv = -ETA * mm(x1, vo, 1, 1) + ETA * mm(y1, vb, 1, 1)
    zs = mm(z1, s_mat, 1, 0)
    s2 = s_mat + zs + mm(s_mat, z1, 1, 1) + mm(zs, z1, 1, 1)
    s2 = s2 + h + mm(z1, h, 1, 0) + ht + mm(ht, z1, 1, 1) + vv
    u2, x2, y2, z2, _ = gradients(p2, q2, r2, s2, obt, bb, scale, ct, cnt)
    z2 = ETA * z2
    u = -ETA * (u1 + u2)
    x = -ETA * (x1 + mm(z2, x1, 1, 0) + x2)
    y = ETA * (y1 + mm(z2, y1, 1, 0) + y2)
    z = z1 + z2 + mm(z2, z1, 1, 0)
    return u, x, y, z, loss

def tail_kernel(hidt, dn, ag, hg_o, ing_o, hv, dv, av, gv, iv, sem, osem):
    cols = [pl.ds(i * 512, 512) for i in range(4)]
    loads = [pltpu.make_async_copy(hidt, hv, sem.at[0])]
    loads += [pltpu.make_async_copy(dn.at[:, cols[i]], dv.at[:, cols[i]], sem.at[1 + i]) for i in range(4)]
    loads.append(pltpu.make_async_copy(ag, av, sem.at[5]))
    for c in loads:
        c.start()
    loads[0].wait()
    outs = []
    for i in range(4):
        loads[1 + i].wait()
        gv[:, cols[i]] = jnp.dot(hv[...], dv[:, cols[i]], preferred_element_type=F32).astype(BF)
        outs.append(pltpu.make_async_copy(gv.at[:, cols[i]], hg_o.at[:, cols[i]], osem.at[i]))
        outs[-1].start()
        if i == 2:
            loads[5].wait()
            iv[...] = jnp.transpose(av[...].astype(F32))
            outs.append(pltpu.make_async_copy(iv, ing_o, osem.at[4]))
            outs[-1].start()
    for c in outs:
        c.wait()


FAR = (4, 3, 5, 2, 6, 1, 7, 0)
FAR_X = (2, 1, 3, 0)
BACK = (0, 1, 7, 4, 3, 5, 2, 6)
SOON = (0, 1, 7, 2, 6, 3, 5, 4)


def kernel(
    ids_h, table_h, inw_h, bias_h, w_hbm, tok_h, lab_h, byte_h, outt_h,
    ag_o, dn_o, hidt_o, loss_o,
    ids, bias, tok, lab, table, inw, byte, outt,
    w, hid, fs, fr, sb, r2, ft, f, rx, la, lb, xf, bp, gp, gq, ga, gb, na, nb, ms, er, cm, cr, ta, tx, g_in,
    d_in, dn, hb, a1, a1s, a2, ag, hidt, chosen_s, like,
    sl, sw, so, r1s, r1r, r2s, r2r, gs, gr, r3s, r3r, e1s, e1r, e2s, e2r, r4s, r4r, r5s, r5r, r6s, r6r,
    p1s, p1r, p2s, p2r, p3s, p3r, p4s, p4r,
):
    rem, div = lax.rem, lax.div
    head = lax.axis_index("head")
    grp = lax.axis_index("client")
    x, z, lo = div(head, 16), rem(div(head, 2), 8), rem(head, 2)
    hi, k = div(grp, 2), rem(grp, 2)
    p = rem(hi + lo, 2)
    xs = [rem(x + d, 4) for d in range(4)]
    zs = [rem(z + d, 8) for d in range(8)]
    ks = [k, 1 - k]
    his = [hi, 1 - hi]
    los = [lo, 1 - lo]
    xz16 = [[xs[dx] * 16 + zs[dz] * 2 for dz in range(8)] for dx in range(4)]

    def remote(src, dst, ss, rs, to):
        return pltpu.make_async_remote_copy(
            src_ref=src, dst_ref=dst, send_sem=ss, recv_sem=rs, device_id=to, device_id_type=MESH
        )

    def drain(like_ref, sem):
        pltpu.make_async_copy(like_ref, like_ref, sem).wait()

    partner = (head, hi * 2 + 1 - k)
    n1 = (xz16[0][0] + 1 - lo, grp)
    n2 = (xz16[0][0] + 1 - lo, (1 - hi) * 2 + k)

    ins = [
        pltpu.make_async_copy(src, dst, sl.at[i])
        for i, (src, dst) in enumerate(
            (
                (ids_h, ids), (table_h, table), (bias_h, bias), (inw_h, inw),
                (byte_h, byte), (outt_h, outt), (tok_h, tok), (lab_h, lab),
            )
        )
    ]
    wc = [
        pltpu.make_async_copy(w_hbm.at[:, pl.ds(i * CW, CW)], w.at[:, pl.ds(i * CW, CW)], sw.at[i])
        for i in range(CH)
    ]
    for c in ins[:4] + wc + ins[4:]:
        c.start()

    bar = pltpu.get_barrier_semaphore()
    for dz in FAR:
        for dx in FAR_X:
            for dh in range(2):
                for dk in range(2):
                    if dx or dz or dh or dk:
                        to = (xz16[dx][dz] + los[dh], his[dh] * 2 + ks[dk])
                        pl.semaphore_signal(bar, inc=1, device_id=to, device_id_type=MESH)
    for dx in range(4):
        pl.semaphore_signal(bar, inc=1, device_id=(xz16[dx][0] + 1 - lo, grp), device_id_type=MESH)

    m = iota((256, 256), 1)
    mhi, mx, mz, mp, mk = m % 2, (m // 2) % 4, (m // 8) % 8, (m // 64) % 2, m // 128
    owner = (mx * 16 + mz * 2 + (mp + mhi) % 2) * 4 + mhi * 2 + mk
    order = (iota((256, 256), 0) == owner).astype(BF)
    ins[0].wait()
    picks = (iota((1024, 256), 0) == ids[...]).astype(F32).astype(BF)
    picks = mm(picks, order, 1, 0)
    ins[1].wait()
    chosen = mm(picks, table[...], 0, 0).astype(BF)
    chosen_s[...] = chosen
    ins[2].wait()
    ins[3].wait()
    pre = mm(chosen, inw[...], 1, 0) + bias[...]
    hidden = jnp.maximum(pre, 0.0)
    hid[...] = hidden.astype(BF)

    for i in range(CH):
        cols = pl.ds(i * CW, CW)
        wc[i].wait()
        fs[:, :, :, :, cols] = jnp.dot(hid[...], w[:, cols], preferred_element_type=F32).reshape(
            2, 2, 8, 8, CW
        )

    pl.semaphore_wait(bar, 131)

    c1 = []
    for dz in FAR:
        c = remote(fs.at[1 - k, :, zs[dz]], fr.at[:, zs[dz]], r1s, r1r.at[dz], partner)
        c.start()
        c1.append(c)
    ins[4].wait()
    ins[5].wait()
    gp[0:256, :] = mm(outt[...], byte[...], 1, 1)
    gp[256:512, :] = mm(outt[...], outt[...], 1, 1)
    gp[512:768, :] = mm(byte[...], byte[...], 1, 1)
    cg = remote(gp, gq, gs.at[0], gr.at[0], partner)
    cg.start()
    diag = iota((256, 256), 0) == iota((256, 256), 1)
    ra = pl.ds(pl.multiple_of(k * 160 + x * 40, 8), 40)
    rb = pl.ds(pl.multiple_of(k * 256 + x * 64, 64), 64)
    cg2 = [
        remote(ga.at[ra], na.at[ra], gs.at[1], gr.at[1], n2),
        remote(gb.at[rb], nb.at[rb], gs.at[2], gr.at[2], n2),
    ]
    for i, dz in enumerate(FAR):
        c1[i].wait_recv()
        sb[:, zs[dz]] = (fs[k, :, zs[dz]] + fr[:, zs[dz]]).astype(BF)
        remote(sb.at[1 - p, zs[dz]], r2.at[0, zs[dz]], r2s, r2r.at[dz], n1).start()
        remote(sb.at[p, zs[dz]], r2.at[1, zs[dz]], r2s, r2r.at[dz], n2).start()
        if i == 5:
            cg.wait_recv()
            gsum = gp[...] + gq[...]
            ga[0:256, :] = gsum[0:256]
            ga[256:320, :] = jnp.broadcast_to(
                jnp.sum(jnp.where(diag, gsum[512:768], 0.0), 0, keepdims=True), (64, 256)
            )
            gb[...] = gsum[256:768].astype(BF)
            for c in cg2:
                c.start()

    for d8 in range(8):
        perm = (iota((1024, 128), 0) == 8 * iota((1024, 128), 1) + d8).astype(F32)
        bp[:, d8 * 128 : (d8 + 1) * 128] = mm(byte[...], perm, 1, 0).astype(BF)
    ins[6].wait()
    ins[7].wait()
    tok_hot = (iota((256, 256), 0) == tok[...]).astype(F32)
    lab_hot = (iota((256, 256), 0) == lab[...]).astype(F32)
    ct = mm(lab_hot, tok_hot, 1, 1)
    cnt = jnp.sum(ct, 0, keepdims=True)
    hidt[...] = jnp.transpose(hid[...].astype(F32)).astype(BF)
    co = [pltpu.make_async_copy(hidt, hidt_o, so.at[0])]
    co[0].start()

    is_a = x < 2
    slots = [jnp.where(is_a, (rem(z, 4) * 2 + 1 - lo) * 2 + q, 16 + 8 * (x - 2) + z) for q in range(2)]
    hi_d = jnp.where(is_a, x, 1 - lo)
    lo_d = rem(p + hi_d, 2)
    cores = [jnp.where(is_a, div(z, 4), q) for q in range(2)]
    to_c = [hi_d * 2 + cores[q] for q in range(2)]
    mine = [to_c[q] == grp for q in range(2)]
    n_self = mine[0].astype(jnp.int32) + mine[1].astype(jnp.int32)
    for i, dz in enumerate(FAR):
        drain(r2.at[:, zs[dz]], r2r.at[dz])
        both = r2[0, zs[dz]].astype(F32) + r2[1, zs[dz]].astype(F32)
        for q in range(2):
            for j in range(8):
                at = (q * 8 + j) * 128
                ft[q, pl.ds(j, 8, stride=8), :] = both[:, at : at + 128]
            f[q, zs[dz]] = ft[q, 0:64].astype(BF).reshape(4, 2, 8, 128)
        for dx in FAR_X:
            for q in range(2):
                c = remote(
                    f.at[q, zs[dz], xs[dx]], rx.at[k, :, slots[q]], r3s, r3r, (xz16[dx][dz] + lo_d, to_c[q])
                )
                if dz or dx:
                    c.start()
                else:
                    pl.when(jnp.logical_not(mine[q]))(c.start)
        if i == 6:
            for c in cg2:
                c.wait_recv()
            for dx in (2, 1, 3):
                to = (xz16[dx][0] + lo, grp)
                remote(na.at[ra], na.at[ra], gs.at[1], gr.at[3], to).start()
                remote(nb.at[rb], nb.at[rb], gs.at[2], gr.at[4], to).start()
    for q in range(2):

        @pl.when(mine[q])
        def _(q=q):
            rx[k, :, slots[q]] = f[q, z, x]

    def wait_all(sem):
        for n in range(3):

            @pl.when(n_self == n)
            def _(n=n):
                piece = like.at[pl.ds(0, 64 - n)]
                pltpu.make_async_copy(piece, piece, sem).wait()

    wait_all(r3r)

    drain(na.at[pl.ds(0, 120)], gr.at[3])
    drain(nb.at[pl.ds(0, 192)], gr.at[4])
    ha = pl.ds(pl.multiple_of(k * 160, 8), 160)
    hbb = pl.ds(pl.multiple_of(k * 256, 256), 256)
    cg3 = [
        remote(na.at[ha], na.at[ha], gs.at[1], gr.at[5], partner),
        remote(nb.at[hbb], nb.at[hbb], gs.at[2], gr.at[6], partner),
    ]
    for c in cg3:
        c.start()
    for c in range(4):
        at = jnp.transpose(rx[c // 2, c % 2, 0:16].astype(F32).reshape(128, 128))
        for d8 in range(8):
            la[c * 16 : (c + 1) * 16, d8 * 128 : (d8 + 1) * 128] = at[d8 * 16 : (d8 + 1) * 16].astype(BF)
        xf[c * 128 : (c + 1) * 128, :] = rx[c // 2, c % 2, 16:32].astype(F32).reshape(128, 128)
    for j in range(8):
        lb[:, j * 128 : (j + 1) * 128] = xf[pl.ds(j, 64, stride=8), :].astype(BF)
    pt = mm(la[...], bp[...], 1, 1)
    qt = mm(lb[...], outt[...], 1, 1)
    rt = mm(lb[...], byte[...], 1, 1)
    ss = mm(lb[...], lb[...], 1, 1)
    for c in range(4):
        rows = slice(c * 16, (c + 1) * 16)
        ms[c, 0:16, :] = pt[rows].astype(BF)
        ms[c, 16:32, :] = qt[rows].astype(BF)
        ms[c, 32:48, :] = rt[rows].astype(BF)
        ms[c, 48:64, :] = jnp.zeros((16, 256), BF)
        ms[c, 48:64, 0:16] = ss[rows, c * 16 : (c + 1) * 16].astype(BF)
    me = k * 2 + hi
    members = [
        (ks[o // 2] * 2 + his[o % 2], (xz16[0][0] + los[o % 2], his[o % 2] * 2 + ks[o // 2]))
        for o in range(4)
    ]
    for o in range(1, 4):
        c_, to = members[o]
        remote(ms.at[c_], er.at[o], e1s, e1r, to).start()
    for c in cg3:
        c.wait_recv()
    obt = ga[0:256, :] + na[0:256, :]
    bb = ga[256:257, :] + na[256:257, :]
    grams = gb[...].astype(F32) + nb[...].astype(F32)
    oo, bbm = grams[0:256].astype(BF), grams[256:512].astype(BF)
    scale = lax.rsqrt(bb * (1 / 4096) + EPS)
    own = ms[me].astype(F32)
    drain(er.at[pl.ds(1, 3)], e1r)
    for o in range(1, 4):
        own = own + er[o].astype(F32)
    u, xx, yy, zz, loss = two_steps(
        own[0:16], own[16:32], own[32:48], own[48:64, 0:16], obt, oo, bbm, bb, scale, ct, cnt
    )
    loss_o[0] = loss * (1 / 256)
    cm[0:16, :] = u.astype(BF)
    cm[16:32, :] = xx.astype(BF)
    cm[32:48, :] = yy.astype(BF)
    cm[48:64, :] = jnp.zeros((16, 256), BF)
    cm[48:64, 0:16] = zz.astype(BF)
    for o in range(1, 4):
        remote(cm, cr.at[me], e2s, e2r, members[o][1]).start()
    cr[me] = cm[...]
    drain(er.at[pl.ds(1, 3)], e2r)

    allc = cr[...]
    us = allc[:, 0:16].reshape(64, 256)
    xc = allc[:, 16:32].reshape(64, 256)
    yc = allc[:, 32:48].reshape(64, 256)
    dat = mm(us, bp[...], 1, 0)
    for c in range(4):
        for d8 in range(8):
            ta[d8 * 16 : (d8 + 1) * 16, :] = dat[c * 16 : (c + 1) * 16, d8 * 128 : (d8 + 1) * 128]
        tx[c // 2, c % 2, 0:16] = jnp.transpose(ta[...]).astype(BF).reshape(16, 8, 128)
    dbs = mm(xc, outt[...], 1, 0) + mm(yc, byte[...], 1, 0)
    zdb = [mm(cr[c, 48:64, 0:16], lb[c * 16 : (c + 1) * 16, :], 1, 0) for c in range(4)]
    dbs = dbs + jnp.concatenate(zdb, axis=0)
    for j in range(8):
        xf[pl.ds(j, 64, stride=8), :] = dbs[:, j * 128 : (j + 1) * 128]
    for c in range(4):
        tx[c // 2, c % 2, 16:32] = xf[c * 128 : (c + 1) * 128, :].astype(BF).reshape(16, 8, 128)

    def give(slot, k_, q_, to, back, near):
        c = remote(tx.at[k_, :, slot], g_in.at[q_, z, x], r4s, r4r.at[back], to)
        if near:
            pl.when(jnp.logical_not((to[0] == head) & (to[1] == grp)))(c.start)
        else:
            c.start()

    z4 = [rem(z + d, 4) for d in (0, 1, 3, 2)]
    his_a = [rem(p + 1 - par, 2) for par in range(2)]
    for step in range(8):
        dz = BACK[step]
        for xh in range(2):
            for dk in range(2):
                slot = 16 + xh * 8 + zs[dz]
                to = (32 + xh * 16 + zs[dz] * 2 + 1 - hi, (1 - lo) * 2 + ks[dk])
                give(slot, ks[dk], k, to, (8 - dz) % 8, dz == 0)
        zr = z4[step // 2]
        za = k * 4 + zr
        back = rem(z - za + 8, 8)
        par = step % 2
        for q in range(2):
            for dk in range(2):
                slot = (zr * 2 + par) * 2 + q
                to = (hi * 16 + za * 2 + 1 - par, his_a[par] * 2 + ks[dk])
                give(slot, ks[dk], q, to, back, step // 2 == 0)
    for q in range(2):

        @pl.when(mine[q])
        def _(q=q):
            g_in[q, z, x] = tx[k, :, slots[q]]

    for dz in SOON:
        if dz:
            drain(like.at[pl.ds(0, 8)], r4r.at[dz])
        else:
            for n in range(3):

                @pl.when(n_self == n)
                def _(n=n):
                    drain(like.at[pl.ds(0, 8 - n)], r4r.at[0])

        for to in (n1, n2):
            remote(g_in.at[:, zs[dz]], d_in.at[k, p, :, zs[dz]], r5s, r5r.at[dz], to).start()
    for dz in SOON:
        drain(d_in.at[k, :, :, zs[dz]], r5r.at[dz])
        region = d_in.at[k, :, :, zs[dz]]
        remote(region, region, r6s, r6r, partner).start()
    drain(d_in.at[1 - k], r6r)
    for kp in range(4):
        xd = d_in[kp // 2, kp % 2].astype(F32).reshape(1024, 128)
        ft[0] = xd[0:512]
        ft[1] = xd[512:1024]
        for j in range(16):
            dn[kp * 64 : (kp + 1) * 64, j * 128 : (j + 1) * 128] = ft[
                j // 8, pl.ds(j % 8, 64, stride=8), :
            ].astype(BF)
    co.append(pltpu.make_async_copy(dn, dn_o, so.at[1]))
    co[1].start()

    turn = [rem(zn - z + 14, 8) * 16 for zn in range(8)]
    for i in range(4):
        part = mm(w[i * 256 : (i + 1) * 256, :], dn[...], 1, 1).astype(BF)
        for l_ in range(2):
            for zn in range(8):
                at = l_ * 128 + zn * 16
                hb[i, l_, pl.ds(pl.multiple_of(turn[zn], 16), 16), :] = part[at : at + 16]
    peers = [(xs[o // 2], los[o % 2], (xz16[o // 2][0] + los[o % 2], grp)) for o in range(8)]
    for h in range(2):
        rows = pl.ds(h * 64, 64)
        for o in (4, 5, 2, 3, 6, 7, 1):
            x_, lo_, to = peers[o]
            remote(hb.at[x_, lo_, rows], a1.at[o, rows], p1s, p1r.at[h], to).start()
    for h in range(2):
        rows = pl.ds(h * 64, 64)
        acc = hb[x, lo, rows, :].astype(F32)
        drain(a1.at[pl.ds(1, 7), rows], p1r.at[h])
        for o in range(1, 8):
            acc = acc + a1[o, rows, :].astype(F32)
        a1s[rows, :] = acc.astype(BF)
        for t in ((2, 1, 3, 0), (4, 7, 5, 6))[h]:
            dz = (t + 2) % 8
            if dz:
                remote(a1s.at[pl.ds(t * 16, 16)], a2.at[dz], p2s, p2r, (xz16[0][dz] + lo, grp)).start()
    total = a1s[96:112, :].astype(F32)
    drain(a2.at[pl.ds(1, 7)], p2r)
    for dz in range(1, 8):
        total = total + a2[dz].astype(F32)
    base = pl.multiple_of(x * 256 + lo * 128, 128)
    row0 = pl.multiple_of(base + z * 16, 16)
    total = jnp.where(hidt[pl.ds(row0, 16), :].astype(F32) > 0, total, 0.0)
    big = total.astype(BF)
    small = (total - big.astype(F32)).astype(BF)
    piece = mm(big, chosen_s[...], 1, 0) + mm(small, chosen_s[...], 1, 0)
    ag[pl.ds(row0, 16), :] = piece.astype(BF)
    cd = {}
    own_rows = ag.at[pl.ds(row0, 16)]
    for dz in FAR[:7]:
        cd[dz] = remote(own_rows, own_rows, p3s, p3r.at[dz], (xz16[0][dz] + lo, grp))
        cd[dz].start()
    for dz in (0, 1, 7, 2, 6, 3, 5, 4):
        if dz:
            cd[dz].wait_recv()
        rows = ag.at[pl.ds(pl.multiple_of(base + zs[(8 - dz) % 8] * 16, 16), 16)]
        for o in (4, 5, 2, 3, 6, 7, 1):
            remote(rows, rows, p4s, p4r, peers[o][2]).start()
    drain(a1.at[pl.ds(1, 7)], p4r)
    co.append(pltpu.make_async_copy(ag, ag_o, so.at[2]))
    co[2].start()

    drain(fr, r1s)
    drain(r2, r2s)
    drain(gq, gs.at[0])
    drain(na, gs.at[1])
    drain(nb, gs.at[2])
    drain(er.at[pl.ds(1, 3)], e1s)
    drain(er.at[pl.ds(1, 3)], e2s)
    drain(d_in.at[0], r5s)
    drain(d_in.at[0], r6s)
    drain(a1.at[pl.ds(1, 7)], p1s)
    drain(a2.at[pl.ds(1, 7)], p2s)
    drain(a2.at[pl.ds(1, 7)], p3s)
    drain(a1.at[pl.ds(1, 7)], p4s)
    wait_all(r3s)
    wait_all(r4s)
    for c in co:
        c.wait()


def local(client_ids, client_table, in_weight, in_bias, head_weight, tokens, labels, byte_table, out_table):
    hbm = pl.BlockSpec(memory_space=pl.ANY)
    dma = pltpu.SemaphoreType.DMA
    V = pltpu.VMEM
    S = jax.ShapeDtypeStruct
    ag, dn, hidt, losses = pl.pallas_call(
        kernel,
        out_shape=(S((1024, 256), BF), S((256, 2048), BF), S((1024, 256), BF), S((1,), F32)),
        in_specs=[hbm] * 9,
        out_specs=(hbm, hbm, hbm, pl.BlockSpec(memory_space=pltpu.SMEM)),
        scratch_shapes=[
            V((1, 256), jnp.int32),
            V((1, 1024), F32),
            V((1, 256), jnp.int32),
            V((1, 256), jnp.int32),
            V((1024, 256), BF),
            V((256, 1024), BF),
            V((256, 1024), BF),
            V((256, 1024), BF),
            V((1024, 2048), BF),
            V((256, 1024), BF),
            V((2, 2, 8, 8, 2048), F32),
            V((2, 8, 8, 2048), F32),
            V((2, 8, 8, 2048), BF),
            V((2, 8, 8, 2048), BF),
            V((2, 512, 128), F32),
            V((2, 8, 4, 2, 8, 128), BF),
            V((2, 2, 32, 8, 128), BF),
            V((64, 1024), BF),
            V((64, 1024), BF),
            V((512, 128), F32),
            V((256, 1024), BF),
            V((768, 256), F32),
            V((768, 256), F32),
            V((320, 256), F32),
            V((512, 256), BF),
            V((320, 256), F32),
            V((512, 256), BF),
            V((4, 64, 256), BF),
            V((4, 64, 256), BF),
            V((64, 256), BF),
            V((4, 64, 256), BF),
            V((128, 128), F32),
            V((2, 2, 32, 8, 128), BF),
            V((2, 8, 4, 2, 8, 128), BF),
            V((2, 2, 2, 8, 4, 2, 8, 128), BF),
            V((256, 2048), BF),
            V((4, 2, 128, 256), BF),
            V((8, 128, 256), BF),
            V((128, 256), BF),
            V((8, 16, 256), BF),
            V((1024, 256), BF),
            V((1024, 256), BF),
            V((256, 256), BF),
            V((64, 2, 8, 128), BF),
            dma((8,)), dma((CH,)), dma((3,)),
            dma(()), dma((8,)),
            dma(()), dma((8,)),
            dma((3,)), dma((7,)),
            dma(()), dma(()),
            dma(()), dma(()), dma(()), dma(()),
            dma(()), dma((8,)),
            dma(()), dma((8,)), dma(()), dma(()),
            dma(()), dma((2,)), dma(()), dma(()),
            dma(()), dma((8,)), dma(()), dma(()),
        ],
        compiler_params=pltpu.CompilerParams(
            collective_id=0, has_side_effects=True, vmem_limit_bytes=60 * 1024 * 1024
        ),
        name="round",
    )(
        client_ids.reshape(1, 256), client_table, in_weight, in_bias.reshape(1, 1024), head_weight,
        tokens, labels, byte_table, out_table,
    )
    head_grad, in_grad = pl.pallas_call(
        tail_kernel,
        out_shape=(S((1024, 2048), BF), S((256, 1024), F32)),
        in_specs=[hbm] * 3,
        out_specs=(hbm, hbm),
        scratch_shapes=[
            V((1024, 256), BF), V((256, 2048), BF), V((1024, 256), BF),
            V((1024, 2048), BF), V((256, 1024), F32),
            dma((6,)), dma((5,)),
        ],
        compiler_params=pltpu.CompilerParams(vmem_limit_bytes=60 * 1024 * 1024),
        name="tail",
    )(hidt, dn, ag)
    return head_grad, in_grad, losses


def solution(mesh):
    placed = (
        P(),
        P(),
        P(None, "client"),
        P("client"),
        P("client", "head"),
        P(("head", "client"), None),
        P(("head", "client"), None),
        P(None, "client"),
        P(None, "client"),
    )
    return jax.shard_map(
        local,
        mesh=mesh,
        in_specs=placed,
        out_specs=(P("client", "head"), P(None, "client"), P(("head", "client"))),
        check_vma=False,
    )
```

```python
import jax
import jax.numpy as jnp
from jax import lax
from jax.experimental import pallas as pl
from jax.experimental.pallas import tpu as pltpu
from jax.sharding import PartitionSpec as P

EPS = 1e-6
ETA = 0.1
F32 = jnp.float32
BF = jnp.bfloat16
MESH = pl.DeviceIdType.MESH
CH = 4
CW = 2048 // CH


def mm(a, b, ca, cb):
    return lax.dot_general(
        a.astype(BF), b.astype(BF), (((ca,), (cb,)), ((), ())), preferred_element_type=F32
    )


def iota(shape, dim):
    return lax.broadcasted_iota(jnp.int32, shape, dim)


def gradients(pt, qt, rt, s_mat, obt, bb, scale, ct, cnt):
    tt = pt * (scale * (1 / 256))
    st = mm(s_mat, tt, 1, 0)
    msq = (bb + jnp.sum(tt * (2 * rt + st), 0, keepdims=True)) * (1 / 4096)
    q = lax.rsqrt(msq + EPS)
    mt = obt + mm(qt, tt, 0, 0)
    lg = mt * (q * (1 / 16))
    top = jnp.max(lg, 0, keepdims=True)
    ex = jnp.exp(lg - top)
    total = jnp.sum(ex, 0, keepdims=True)
    gt = (ex * (cnt / total) - ct) * (1 / 16)
    along = jnp.sum(gt * mt, 0, keepdims=True)
    e = q * q * q * along * (1 / 4096)
    ht = gt * q
    dt = mm(qt, ht, 1, 0) - e * (rt + st)
    ut = dt * (scale * (1 / 256))
    xt = mm(tt, ht, 1, 1)
    yt = tt * e
    z = mm(yt, tt, 1, 1)
    loss = jnp.sum(cnt * (top + jnp.log(total)) - jnp.sum(ct * lg, 0, keepdims=True))
    return ut, xt, yt, z, loss


def two_steps(pt, qt, rt, s_mat, obt, oo, bbm, bb, scale, ct, cnt):
    u1, x1, y1, z1, loss = gradients(pt, qt, rt, s_mat, obt, bb, scale, ct, cnt)
    vo = -ETA * mm(x1, oo, 1, 0) + ETA * mm(y1, obt, 1, 1)
    vb = -ETA * mm(x1, obt, 1, 0) + ETA * mm(y1, bbm, 1, 0)
    z1 = ETA * z1
    p2 = pt - ETA * mm(u1, bbm, 1, 0)
    q2 = qt + mm(z1, qt, 1, 0) + vo
    r2 = rt + mm(z1, rt, 1, 0) + vb
    h = -ETA * mm(qt, x1, 1, 1) + ETA * mm(rt, y1, 1, 1)
    ht = -ETA * mm(x1, qt, 1, 1) + ETA * mm(y1, rt, 1, 1)
    vv = -ETA * mm(x1, vo, 1, 1) + ETA * mm(y1, vb, 1, 1)
    zs = mm(z1, s_mat, 1, 0)
    s2 = s_mat + zs + mm(s_mat, z1, 1, 1) + mm(zs, z1, 1, 1)
    s2 = s2 + h + mm(z1, h, 1, 0) + ht + mm(ht, z1, 1, 1) + vv
    u2, x2, y2, z2, _ = gradients(p2, q2, r2, s2, obt, bb, scale, ct, cnt)
    z2 = ETA * z2
    u = -ETA * (u1 + u2)
    x = -ETA * (x1 + mm(z2, x1, 1, 0) + x2)
    y = ETA * (y1 + mm(z2, y1, 1, 0) + y2)
    z = z1 + z2 + mm(z2, z1, 1, 0)
    return u, x, y, z, loss

def tail_kernel(hidt, dn, ag, hg_o, ing_o, hv, dv, av, gv, iv, sem, osem):
    cols = [pl.ds(i * 512, 512) for i in range(4)]
    loads = [pltpu.make_async_copy(hidt, hv, sem.at[0])]
    loads += [pltpu.make_async_copy(dn.at[:, cols[i]], dv.at[:, cols[i]], sem.at[1 + i]) for i in range(4)]
    loads.append(pltpu.make_async_copy(ag, av, sem.at[5]))
    for c in loads[5:] + loads[:5]:
        c.start()
    loads[5].wait()
    iv[...] = jnp.transpose(av[...].astype(F32))
    outs = [pltpu.make_async_copy(iv, ing_o, osem.at[4])]
    outs[0].start()
    loads[0].wait()
    for i in range(4):
        loads[1 + i].wait()
        gv[:, cols[i]] = jnp.dot(hv[...], dv[:, cols[i]], preferred_element_type=F32).astype(BF)
        outs.append(pltpu.make_async_copy(gv.at[:, cols[i]], hg_o.at[:, cols[i]], osem.at[i]))
        outs[-1].start()
    for c in outs:
        c.wait()


FAR = (4, 3, 5, 2, 6, 1, 7, 0)
FAR_X = (2, 1, 3, 0)
NEAR = (0, 1, 7, 2, 6, 3, 5, 4)


def kernel(
    ids_h, table_h, inw_h, bias_h, w_hbm, tok_h, lab_h, byte_h, outt_h,
    ag_o, dn_o, hidt_o, loss_o,
    ids, bias, tok, lab, table, inw, byte, outt,
    w, hid, fs, fr, sb, r2, ft, f, rx, la, lb, xf, bp, gp, gq, ga, gb, na, nb, ms, er, cm, cr, ta, tx, g_in,
    d_in, dn, hb, a1, a1s, a2, ag, hidt, chosen_s, like,
    on_x, on_z, sl, sw, so, r1s, r1r, r2s, r2r, gs, gr, r3s, r3r, e1s, e1r, e2s, e2r, r4s, r4r, r5s, r5r, r6s, r6r,
    p1s, p1r, p2s, p2r, p3s, p3r, p4s, p4r,
):
    rem, div = lax.rem, lax.div
    head = lax.axis_index("head")
    grp = lax.axis_index("client")
    x, z, lo = div(head, 16), rem(div(head, 2), 8), rem(head, 2)
    hi, k = div(grp, 2), rem(grp, 2)
    p = rem(hi + lo, 2)
    xs = [rem(x + d, 4) for d in range(4)]
    zs = [rem(z + d, 8) for d in range(8)]
    ks = [k, 1 - k]
    his = [hi, 1 - hi]
    los = [lo, 1 - lo]
    xz16 = [[xs[dx] * 16 + zs[dz] * 2 for dz in range(8)] for dx in range(4)]

    def remote(src, dst, ss, rs, to):
        return pltpu.make_async_remote_copy(
            src_ref=src, dst_ref=dst, send_sem=ss, recv_sem=rs, device_id=to, device_id_type=MESH
        )

    def drain(like_ref, sem):
        pltpu.make_async_copy(like_ref, like_ref, sem).wait()

    partner = (head, hi * 2 + 1 - k)
    n1 = (xz16[0][0] + 1 - lo, grp)
    n2 = (xz16[0][0] + 1 - lo, (1 - hi) * 2 + k)

    ins = [
        pltpu.make_async_copy(src, dst, sl.at[i])
        for i, (src, dst) in enumerate(
            (
                (ids_h, ids), (table_h, table), (bias_h, bias), (inw_h, inw),
                (byte_h, byte), (outt_h, outt), (tok_h, tok), (lab_h, lab),
            )
        )
    ]
    wc = [
        pltpu.make_async_copy(w_hbm.at[:, pl.ds(i * CW, CW)], w.at[:, pl.ds(i * CW, CW)], sw.at[i])
        for i in range(CH)
    ]
    for c in ins[:4] + wc + ins[4:]:
        c.start()

    bar = pltpu.get_barrier_semaphore()
    along_x = [(xz16[dx][0] + lo, grp) for dx in (2, 1, 3)]
    along_z = [(xz16[0][dz] + lo, grp) for dz in FAR[:7]]
    beside = [
        (xz16[0][0] + los[dl], his[dh] * 2 + ks[dk])
        for dl in range(2) for dh in range(2) for dk in range(2) if dl or dh or dk
    ]
    for to in along_z + along_x + beside:
        pl.semaphore_signal(bar, inc=1, device_id=to, device_id_type=MESH)

    m = iota((256, 256), 1)
    mhi, mx, mz, mp, mk = m % 2, (m // 2) % 4, (m // 8) % 8, (m // 64) % 2, m // 128
    owner = (mx * 16 + mz * 2 + (mp + mhi) % 2) * 4 + mhi * 2 + mk
    order = (iota((256, 256), 0) == owner).astype(BF)
    ins[0].wait()
    upper = ids[...] // 32
    halves = jnp.concatenate([upper, ids[...] - upper * 32], axis=0)
    halves = mm(jnp.broadcast_to(halves[:, None], (2, 8, 256)).reshape(16, 256).astype(F32), order, 1, 0)
    sorted_ids = (halves[0:1] * 32 + halves[8:9]).astype(jnp.int32)
    picks = (iota((1024, 256), 0) == sorted_ids).astype(F32).astype(BF)
    ins[1].wait()
    chosen = mm(picks, table[...], 0, 0).astype(BF)
    chosen_s[...] = chosen
    ins[2].wait()
    ins[3].wait()
    pre = mm(chosen, inw[...], 1, 0) + bias[...]
    hidden = jnp.maximum(pre, 0.0)
    hid[...] = hidden.astype(BF)

    for i in range(CH):
        cols = pl.ds(i * CW, CW)
        wc[i].wait()
        fs[:, :, :, :, cols] = jnp.dot(hid[...], w[:, cols], preferred_element_type=F32).reshape(
            2, 2, 8, 8, CW
        )

    pl.semaphore_wait(bar, 17)
    for to in along_x:
        pl.semaphore_signal(on_x, inc=1, device_id=to, device_id_type=MESH)

    c1 = []
    for dz in FAR:
        c = remote(fs.at[1 - k, :, zs[dz]], fr.at[:, zs[dz]], r1s, r1r.at[dz], partner)
        c.start()
        c1.append(c)
    ins[4].wait()
    ins[5].wait()
    gp[0:256, :] = mm(outt[...], byte[...], 1, 1)
    gp[256:512, :] = mm(outt[...], outt[...], 1, 1)
    gp[512:768, :] = mm(byte[...], byte[...], 1, 1)
    cg = remote(gp, gq, gs.at[0], gr.at[0], partner)
    cg.start()
    pl.semaphore_wait(on_x, 3)
    for to in along_z:
        pl.semaphore_signal(on_z, inc=1, device_id=to, device_id_type=MESH)
    diag = iota((256, 256), 0) == iota((256, 256), 1)
    ra = pl.ds(pl.multiple_of(k * 160 + x * 40, 8), 40)
    rb = pl.ds(pl.multiple_of(k * 256 + x * 64, 64), 64)
    cg2 = [
        remote(ga.at[ra], na.at[ra], gs.at[1], gr.at[1], n2),
        remote(gb.at[rb], nb.at[rb], gs.at[2], gr.at[2], n2),
    ]
    for i, dz in enumerate(FAR):
        c1[i].wait_recv()
        sb[:, zs[dz]] = (fs[k, :, zs[dz]] + fr[:, zs[dz]]).astype(BF)
        remote(sb.at[1 - p, zs[dz]], r2.at[0, zs[dz]], r2s, r2r.at[dz], n1).start()
        remote(sb.at[p, zs[dz]], r2.at[1, zs[dz]], r2s, r2r.at[dz], n2).start()
        if i == 5:
            cg.wait_recv()
            gsum = gp[...] + gq[...]
            ga[0:256, :] = gsum[0:256]
            ga[256:320, :] = jnp.broadcast_to(
                jnp.sum(jnp.where(diag, gsum[512:768], 0.0), 0, keepdims=True), (64, 256)
            )
            gb[...] = gsum[256:768].astype(BF)
            for c in cg2:
                c.start()

    for d8 in range(8):
        perm = (iota((1024, 128), 0) == 8 * iota((1024, 128), 1) + d8).astype(F32)
        bp[:, d8 * 128 : (d8 + 1) * 128] = mm(byte[...], perm, 1, 0).astype(BF)
    ins[6].wait()
    ins[7].wait()
    tok_hot = (iota((256, 256), 0) == tok[...]).astype(F32)
    lab_hot = (iota((256, 256), 0) == lab[...]).astype(F32)
    ct = mm(lab_hot, tok_hot, 1, 1)
    cnt = jnp.sum(ct, 0, keepdims=True)
    hidt[...] = jnp.transpose(hid[...].astype(F32)).astype(BF)
    co = [pltpu.make_async_copy(hidt, hidt_o, so.at[0])]
    co[0].start()

    is_a = x < 2
    slots = [jnp.where(is_a, (rem(z, 4) * 2 + 1 - lo) * 2 + q, 16 + 8 * (x - 2) + z) for q in range(2)]
    hi_d = jnp.where(is_a, x, 1 - lo)
    lo_d = rem(p + hi_d, 2)
    cores = [jnp.where(is_a, div(z, 4), q) for q in range(2)]
    to_c = [hi_d * 2 + cores[q] for q in range(2)]
    mine = [to_c[q] == grp for q in range(2)]
    n_self = mine[0].astype(jnp.int32) + mine[1].astype(jnp.int32)
    pl.semaphore_wait(on_z, 7)
    for i, dz in enumerate(FAR):
        drain(r2.at[:, zs[dz]], r2r.at[dz])
        both = r2[0, zs[dz]].astype(F32) + r2[1, zs[dz]].astype(F32)
        for q in range(2):
            for j in range(8):
                at = (q * 8 + j) * 128
                ft[q, pl.ds(j, 8, stride=8), :] = both[:, at : at + 128]
            f[q, zs[dz]] = ft[q, 0:64].astype(BF).reshape(4, 2, 8, 128)
        for dx in FAR_X:
            for q in range(2):
                c = remote(
                    f.at[q, zs[dz], xs[dx]], rx.at[k, :, slots[q]], r3s, r3r, (xz16[dx][dz] + lo_d, to_c[q])
                )
                if dz or dx:
                    c.start()
                else:
                    pl.when(jnp.logical_not(mine[q]))(c.start)
        if i == 6:
            for c in cg2:
                c.wait_recv()
            for dx in (2, 1, 3):
                to = (xz16[dx][0] + lo, grp)
                remote(na.at[ra], na.at[ra], gs.at[1], gr.at[3], to).start()
                remote(nb.at[rb], nb.at[rb], gs.at[2], gr.at[4], to).start()
    for q in range(2):

        @pl.when(mine[q])
        def _(q=q):
            rx[k, :, slots[q]] = f[q, z, x]

    def wait_all(sem):
        for n in range(3):

            @pl.when(n_self == n)
            def _(n=n):
                piece = like.at[pl.ds(0, 64 - n)]
                pltpu.make_async_copy(piece, piece, sem).wait()

    wait_all(r3r)

    drain(na.at[pl.ds(0, 120)], gr.at[3])
    drain(nb.at[pl.ds(0, 192)], gr.at[4])
    ha = pl.ds(pl.multiple_of(k * 160, 8), 160)
    hbb = pl.ds(pl.multiple_of(k * 256, 256), 256)
    cg3 = [
        remote(na.at[ha], na.at[ha], gs.at[1], gr.at[5], partner),
        remote(nb.at[hbb], nb.at[hbb], gs.at[2], gr.at[6], partner),
    ]
    for c in cg3:
        c.start()
    for c in range(4):
        at = jnp.transpose(rx[c // 2, c % 2, 0:16].astype(F32).reshape(128, 128))
        for d8 in range(8):
            la[c * 16 : (c + 1) * 16, d8 * 128 : (d8 + 1) * 128] = at[d8 * 16 : (d8 + 1) * 16].astype(BF)
        xf[c * 128 : (c + 1) * 128, :] = rx[c // 2, c % 2, 16:32].astype(F32).reshape(128, 128)
    for j in range(8):
        lb[:, j * 128 : (j + 1) * 128] = xf[pl.ds(j, 64, stride=8), :].astype(BF)
    pt = mm(la[...], bp[...], 1, 1)
    qt = mm(lb[...], outt[...], 1, 1)
    rt = mm(lb[...], byte[...], 1, 1)
    ss = mm(lb[...], lb[...], 1, 1)
    for c in range(4):
        rows = slice(c * 16, (c + 1) * 16)
        ms[c, 0:16, :] = pt[rows].astype(BF)
        ms[c, 16:32, :] = qt[rows].astype(BF)
        ms[c, 32:48, :] = rt[rows].astype(BF)
        ms[c, 48:64, :] = jnp.zeros((16, 256), BF)
        ms[c, 48:64, 0:16] = ss[rows, c * 16 : (c + 1) * 16].astype(BF)
    me = k * 2 + hi
    members = [
        (ks[o // 2] * 2 + his[o % 2], (xz16[0][0] + los[o % 2], his[o % 2] * 2 + ks[o // 2]))
        for o in range(4)
    ]
    for o in range(1, 4):
        c_, to = members[o]
        remote(ms.at[c_], er.at[o], e1s, e1r, to).start()
    for c in cg3:
        c.wait_recv()
    obt = ga[0:256, :] + na[0:256, :]
    bb = ga[256:257, :] + na[256:257, :]
    grams = gb[...].astype(F32) + nb[...].astype(F32)
    oo, bbm = grams[0:256].astype(BF), grams[256:512].astype(BF)
    scale = lax.rsqrt(bb * (1 / 4096) + EPS)
    own = ms[me].astype(F32)
    drain(er.at[pl.ds(1, 3)], e1r)
    for o in range(1, 4):
        own = own + er[o].astype(F32)
    u, xx, yy, zz, loss = two_steps(
        own[0:16], own[16:32], own[32:48], own[48:64, 0:16], obt, oo, bbm, bb, scale, ct, cnt
    )
    loss_o[0] = loss * (1 / 256)
    cm[0:16, :] = u.astype(BF)
    cm[16:32, :] = xx.astype(BF)
    cm[32:48, :] = yy.astype(BF)
    cm[48:64, :] = jnp.zeros((16, 256), BF)
    cm[48:64, 0:16] = zz.astype(BF)
    for o in range(1, 4):
        remote(cm, cr.at[me], e2s, e2r, members[o][1]).start()
    cr[me] = cm[...]
    drain(er.at[pl.ds(1, 3)], e2r)

    allc = cr[...]
    us = allc[:, 0:16].reshape(64, 256)
    xc = allc[:, 16:32].reshape(64, 256)
    yc = allc[:, 32:48].reshape(64, 256)
    dat = mm(us, bp[...], 1, 0)
    for c in range(4):
        for d8 in range(8):
            ta[d8 * 16 : (d8 + 1) * 16, :] = dat[c * 16 : (c + 1) * 16, d8 * 128 : (d8 + 1) * 128]
        tx[c // 2, c % 2, 0:16] = jnp.transpose(ta[...]).astype(BF).reshape(16, 8, 128)
    dbs = mm(xc, outt[...], 1, 0) + mm(yc, byte[...], 1, 0)
    zdb = [mm(cr[c, 48:64, 0:16], lb[c * 16 : (c + 1) * 16, :], 1, 0) for c in range(4)]
    dbs = dbs + jnp.concatenate(zdb, axis=0)
    for j in range(8):
        xf[pl.ds(j, 64, stride=8), :] = dbs[:, j * 128 : (j + 1) * 128]
    for c in range(4):
        tx[c // 2, c % 2, 16:32] = xf[c * 128 : (c + 1) * 128, :].astype(BF).reshape(16, 8, 128)

    def give(slot, k_, q_, to, back, near):
        c = remote(tx.at[k_, :, slot], g_in.at[q_, z, x], r4s, r4r.at[back], to)
        if near:
            pl.when(jnp.logical_not((to[0] == head) & (to[1] == grp)))(c.start)
        else:
            c.start()

    his_a = [rem(p + 1 - par, 2) for par in range(2)]
    for dz in NEAR:
        for xh in range(2):
            for dk in range(2):
                slot = 16 + xh * 8 + zs[dz]
                to = (32 + xh * 16 + zs[dz] * 2 + 1 - hi, (1 - lo) * 2 + ks[dk])
                give(slot, ks[dk], k, to, (8 - dz) % 8, dz == 0)

        @pl.when(div(zs[dz], 4) == k)
        def _(dz=dz):
            for par in range(2):
                for q in range(2):
                    for dk in range(2):
                        slot = (rem(zs[dz], 4) * 2 + par) * 2 + q
                        to = (hi * 16 + zs[dz] * 2 + 1 - par, his_a[par] * 2 + ks[dk])
                        give(slot, ks[dk], q, to, (8 - dz) % 8, dz == 0)

    for q in range(2):

        @pl.when(mine[q])
        def _(q=q):
            g_in[q, z, x] = tx[k, :, slots[q]]

    for dz in NEAR:
        if dz:
            drain(like.at[pl.ds(0, 8)], r4r.at[dz])
        else:
            for n in range(3):

                @pl.when(n_self == n)
                def _(n=n):
                    drain(like.at[pl.ds(0, 8 - n)], r4r.at[0])

        for to in (n1, n2):
            remote(g_in.at[:, zs[dz]], d_in.at[k, p, :, zs[dz]], r5s, r5r.at[dz], to).start()
    for dz in NEAR:
        drain(d_in.at[k, :, :, zs[dz]], r5r.at[dz])
        region = d_in.at[k, :, :, zs[dz]]
        remote(region, region, r6s, r6r, partner).start()
    drain(d_in.at[1 - k], r6r)
    for kp in range(4):
        xd = d_in[kp // 2, kp % 2].astype(F32).reshape(1024, 128)
        ft[0] = xd[0:512]
        ft[1] = xd[512:1024]
        for j in range(16):
            dn[kp * 64 : (kp + 1) * 64, j * 128 : (j + 1) * 128] = ft[
                j // 8, pl.ds(j % 8, 64, stride=8), :
            ].astype(BF)
    co.append(pltpu.make_async_copy(dn, dn_o, so.at[1]))
    co[1].start()

    turn = [rem(zn - z + 14, 8) * 16 for zn in range(8)]
    for i in range(4):
        part = mm(w[i * 256 : (i + 1) * 256, :], dn[...], 1, 1).astype(BF)
        for l_ in range(2):
            for zn in range(8):
                at = l_ * 128 + zn * 16
                hb[i, l_, pl.ds(pl.multiple_of(turn[zn], 16), 16), :] = part[at : at + 16]
    peers = [(xs[o // 2], los[o % 2], (xz16[o // 2][0] + los[o % 2], grp)) for o in range(8)]
    for h in range(2):
        rows = pl.ds(h * 64, 64)
        for o in (4, 5, 2, 3, 6, 7, 1):
            x_, lo_, to = peers[o]
            remote(hb.at[x_, lo_, rows], a1.at[o, rows], p1s, p1r.at[h], to).start()
    for h in range(2):
        rows = pl.ds(h * 64, 64)
        acc = hb[x, lo, rows, :].astype(F32)
        drain(a1.at[pl.ds(1, 7), rows], p1r.at[h])
        for o in range(1, 8):
            acc = acc + a1[o, rows, :].astype(F32)
        a1s[rows, :] = acc.astype(BF)
        for t in ((2, 1, 3, 0), (4, 7, 5, 6))[h]:
            dz = (t + 2) % 8
            if dz:
                remote(a1s.at[pl.ds(t * 16, 16)], a2.at[dz], p2s, p2r, (xz16[0][dz] + lo, grp)).start()
    total = a1s[96:112, :].astype(F32)
    drain(a2.at[pl.ds(1, 7)], p2r)
    for dz in range(1, 8):
        total = total + a2[dz].astype(F32)
    base = pl.multiple_of(x * 256 + lo * 128, 128)
    row0 = pl.multiple_of(base + z * 16, 16)
    total = jnp.where(hidt[pl.ds(row0, 16), :].astype(F32) > 0, total, 0.0)
    big = total.astype(BF)
    small = (total - big.astype(F32)).astype(BF)
    piece = mm(big, chosen_s[...], 1, 0) + mm(small, chosen_s[...], 1, 0)
    ag[pl.ds(row0, 16), :] = piece.astype(BF)
    cd = {}
    own_rows = ag.at[pl.ds(row0, 16)]
    for dz in FAR[:7]:
        cd[dz] = remote(own_rows, own_rows, p3s, p3r.at[dz], (xz16[0][dz] + lo, grp))
        cd[dz].start()
    for dz in (0, 1, 7, 2, 6, 3, 5, 4):
        if dz:
            cd[dz].wait_recv()
        rows = ag.at[pl.ds(pl.multiple_of(base + zs[(8 - dz) % 8] * 16, 16), 16)]
        for o in (4, 5, 2, 3, 6, 7, 1):
            remote(rows, rows, p4s, p4r, peers[o][2]).start()
    drain(a1.at[pl.ds(1, 7)], p4r)
    co.append(pltpu.make_async_copy(ag, ag_o, so.at[2]))
    co[2].start()

    drain(fr, r1s)
    drain(r2, r2s)
    drain(gq, gs.at[0])
    drain(na, gs.at[1])
    drain(nb, gs.at[2])
    drain(er.at[pl.ds(1, 3)], e1s)
    drain(er.at[pl.ds(1, 3)], e2s)
    drain(d_in.at[0], r5s)
    drain(d_in.at[0], r6s)
    drain(a1.at[pl.ds(1, 7)], p1s)
    drain(a2.at[pl.ds(1, 7)], p2s)
    drain(a2.at[pl.ds(1, 7)], p3s)
    drain(a1.at[pl.ds(1, 7)], p4s)
    wait_all(r3s)
    wait_all(r4s)
    for c in co:
        c.wait()


def local(client_ids, client_table, in_weight, in_bias, head_weight, tokens, labels, byte_table, out_table):
    hbm = pl.BlockSpec(memory_space=pl.ANY)
    dma = pltpu.SemaphoreType.DMA
    V = pltpu.VMEM
    S = jax.ShapeDtypeStruct
    ag, dn, hidt, losses = pl.pallas_call(
        kernel,
        out_shape=(S((1024, 256), BF), S((256, 2048), BF), S((1024, 256), BF), S((1,), F32)),
        in_specs=[hbm] * 9,
        out_specs=(hbm, hbm, hbm, pl.BlockSpec(memory_space=pltpu.SMEM)),
        scratch_shapes=[
            V((1, 256), jnp.int32),
            V((1, 1024), F32),
            V((1, 256), jnp.int32),
            V((1, 256), jnp.int32),
            V((1024, 256), BF),
            V((256, 1024), BF),
            V((256, 1024), BF),
            V((256, 1024), BF),
            V((1024, 2048), BF),
            V((256, 1024), BF),
            V((2, 2, 8, 8, 2048), F32),
            V((2, 8, 8, 2048), F32),
            V((2, 8, 8, 2048), BF),
            V((2, 8, 8, 2048), BF),
            V((2, 512, 128), F32),
            V((2, 8, 4, 2, 8, 128), BF),
            V((2, 2, 32, 8, 128), BF),
            V((64, 1024), BF),
            V((64, 1024), BF),
            V((512, 128), F32),
            V((256, 1024), BF),
            V((768, 256), F32),
            V((768, 256), F32),
            V((320, 256), F32),
            V((512, 256), BF),
            V((320, 256), F32),
            V((512, 256), BF),
            V((4, 64, 256), BF),
            V((4, 64, 256), BF),
            V((64, 256), BF),
            V((4, 64, 256), BF),
            V((128, 128), F32),
            V((2, 2, 32, 8, 128), BF),
            V((2, 8, 4, 2, 8, 128), BF),
            V((2, 2, 2, 8, 4, 2, 8, 128), BF),
            V((256, 2048), BF),
            V((4, 2, 128, 256), BF),
            V((8, 128, 256), BF),
            V((128, 256), BF),
            V((8, 16, 256), BF),
            V((1024, 256), BF),
            V((1024, 256), BF),
            V((256, 256), BF),
            V((64, 2, 8, 128), BF),
            pltpu.SemaphoreType.REGULAR, pltpu.SemaphoreType.REGULAR,
            dma((8,)), dma((CH,)), dma((3,)),
            dma(()), dma((8,)),
            dma(()), dma((8,)),
            dma((3,)), dma((7,)),
            dma(()), dma(()),
            dma(()), dma(()), dma(()), dma(()),
            dma(()), dma((8,)),
            dma(()), dma((8,)), dma(()), dma(()),
            dma(()), dma((2,)), dma(()), dma(()),
            dma(()), dma((8,)), dma(()), dma(()),
        ],
        compiler_params=pltpu.CompilerParams(
            collective_id=0, has_side_effects=True, vmem_limit_bytes=60 * 1024 * 1024
        ),
        name="round",
    )(
        client_ids.reshape(1, 256), client_table, in_weight, in_bias.reshape(1, 1024), head_weight,
        tokens, labels, byte_table, out_table,
    )
    head_grad, in_grad = pl.pallas_call(
        tail_kernel,
        out_shape=(S((1024, 2048), BF), S((256, 1024), F32)),
        in_specs=[hbm] * 3,
        out_specs=(hbm, hbm),
        scratch_shapes=[
            V((1024, 256), BF), V((256, 2048), BF), V((1024, 256), BF),
            V((1024, 2048), BF), V((256, 1024), F32),
            dma((6,)), dma((5,)),
        ],
        compiler_params=pltpu.CompilerParams(vmem_limit_bytes=60 * 1024 * 1024),
        name="tail",
    )(hidt, dn, ag)
    return head_grad, in_grad, losses


def solution(mesh):
    placed = (
        P(),
        P(),
        P(None, "client"),
        P("client"),
        P("client", "head"),
        P(("head", "client"), None),
        P(("head", "client"), None),
        P(None, "client"),
        P(None, "client"),
    )
    return jax.shard_map(
        local,
        mesh=mesh,
        in_specs=placed,
        out_specs=(P("client", "head"), P(None, "client"), P(("head", "client"))),
        check_vma=False,
    )
```

```python
import jax
import jax.numpy as jnp
from jax import lax
from jax.experimental import pallas as pl
from jax.experimental.pallas import tpu as pltpu
from jax.sharding import PartitionSpec as P

EPS = 1e-6
ETA = 0.1
F32 = jnp.float32
BF = jnp.bfloat16
MESH = pl.DeviceIdType.MESH
CH = 4
CW = 2048 // CH


def mm(a, b, ca, cb):
    return lax.dot_general(
        a.astype(BF), b.astype(BF), (((ca,), (cb,)), ((), ())), preferred_element_type=F32
    )


def iota(shape, dim):
    return lax.broadcasted_iota(jnp.int32, shape, dim)


def gradients(pt, qt, rt, s_mat, obt, bb, scale, ct, cnt):
    tt = pt * (scale * (1 / 256))
    st = mm(s_mat, tt, 1, 0)
    msq = (bb + jnp.sum(tt * (2 * rt + st), 0, keepdims=True)) * (1 / 4096)
    q = lax.rsqrt(msq + EPS)
    mt = obt + mm(qt, tt, 0, 0)
    lg = mt * (q * (1 / 16))
    top = jnp.max(lg, 0, keepdims=True)
    ex = jnp.exp(lg - top)
    total = jnp.sum(ex, 0, keepdims=True)
    gt = (ex * (cnt / total) - ct) * (1 / 16)
    along = jnp.sum(gt * mt, 0, keepdims=True)
    e = q * q * q * along * (1 / 4096)
    ht = gt * q
    dt = mm(qt, ht, 1, 0) - e * (rt + st)
    ut = dt * (scale * (1 / 256))
    xt = mm(tt, ht, 1, 1)
    yt = tt * e
    z = mm(yt, tt, 1, 1)
    loss = jnp.sum(cnt * (top + jnp.log(total)) - jnp.sum(ct * lg, 0, keepdims=True))
    return ut, xt, yt, z, loss


def two_steps(pt, qt, rt, s_mat, obt, oo, bbm, bb, scale, ct, cnt):
    u1, x1, y1, z1, loss = gradients(pt, qt, rt, s_mat, obt, bb, scale, ct, cnt)
    vo = -ETA * mm(x1, oo, 1, 0) + ETA * mm(y1, obt, 1, 1)
    vb = -ETA * mm(x1, obt, 1, 0) + ETA * mm(y1, bbm, 1, 0)
    z1 = ETA * z1
    p2 = pt - ETA * mm(u1, bbm, 1, 0)
    q2 = qt + mm(z1, qt, 1, 0) + vo
    r2 = rt + mm(z1, rt, 1, 0) + vb
    h = -ETA * mm(qt, x1, 1, 1) + ETA * mm(rt, y1, 1, 1)
    ht = -ETA * mm(x1, qt, 1, 1) + ETA * mm(y1, rt, 1, 1)
    vv = -ETA * mm(x1, vo, 1, 1) + ETA * mm(y1, vb, 1, 1)
    zs = mm(z1, s_mat, 1, 0)
    s2 = s_mat + zs + mm(s_mat, z1, 1, 1) + mm(zs, z1, 1, 1)
    s2 = s2 + h + mm(z1, h, 1, 0) + ht + mm(ht, z1, 1, 1) + vv
    u2, x2, y2, z2, _ = gradients(p2, q2, r2, s2, obt, bb, scale, ct, cnt)
    z2 = ETA * z2
    u = -ETA * (u1 + u2)
    x = -ETA * (x1 + mm(z2, x1, 1, 0) + x2)
    y = ETA * (y1 + mm(z2, y1, 1, 0) + y2)
    z = z1 + z2 + mm(z2, z1, 1, 0)
    return u, x, y, z, loss

def tail_kernel(hidt, dn, ag, hg_o, ing_o, hv, dv, av, gv, iv, sem, osem):
    cols = [pl.ds(i * 512, 512) for i in range(4)]
    loads = [pltpu.make_async_copy(hidt, hv, sem.at[0])]
    loads += [pltpu.make_async_copy(dn.at[:, cols[i]], dv.at[:, cols[i]], sem.at[1 + i]) for i in range(4)]
    loads.append(pltpu.make_async_copy(ag, av, sem.at[5]))
    for c in loads:
        c.start()
    loads[0].wait()
    outs = []
    for i in range(4):
        loads[1 + i].wait()
        if i == 1:
            loads[5].wait()
            iv[...] = jnp.transpose(av[...].astype(F32))
        gv[:, cols[i]] = jnp.dot(hv[...], dv[:, cols[i]], preferred_element_type=F32).astype(BF)
        outs.append(pltpu.make_async_copy(gv.at[:, cols[i]], hg_o.at[:, cols[i]], osem.at[i]))
        outs[-1].start()
        if i == 1:
            outs.append(pltpu.make_async_copy(iv, ing_o, osem.at[4]))
            outs[-1].start()
    for c in outs:
        c.wait()


FAR = (4, 3, 5, 2, 6, 1, 7, 0)
FAR_X = (2, 1, 3, 0)
NEAR = (0, 1, 7, 2, 6, 3, 5, 4)


def kernel(
    ids_h, table_h, inw_h, bias_h, w_hbm, tok_h, lab_h, byte_h, outt_h,
    ag_o, dn_o, hidt_o, loss_o,
    ids, bias, tok, lab, table, inw, byte, outt,
    w, hid, fs, fr, sb, r2, ft, f, rx, la, lb, xf, bp, gp, gq, ga, gb, na, nb, gd, nd, ms, er, cm, cr, ta, tx, g_in,
    d_in, dn, hb, a1, a1s, a2, ag, hidt, chosen_s, like,
    on_x, on_z, sl, sw, so, r1s, r1r, r2s, r2r, gs, gr, r3s, r3r, e1s, e1r, e2s, e2r, r4s, r4r, r5s, r5r, r6s, r6r,
    p1s, p1r, p2s, p2r, p3s, p3r, p4s, p4r,
):
    rem, div = lax.rem, lax.div
    head = lax.axis_index("head")
    grp = lax.axis_index("client")
    x, z, lo = div(head, 16), rem(div(head, 2), 8), rem(head, 2)
    hi, k = div(grp, 2), rem(grp, 2)
    p = rem(hi + lo, 2)
    xs = [rem(x + d, 4) for d in range(4)]
    zs = [rem(z + d, 8) for d in range(8)]
    ks = [k, 1 - k]
    his = [hi, 1 - hi]
    los = [lo, 1 - lo]
    xz16 = [[xs[dx] * 16 + zs[dz] * 2 for dz in range(8)] for dx in range(4)]

    def remote(src, dst, ss, rs, to):
        return pltpu.make_async_remote_copy(
            src_ref=src, dst_ref=dst, send_sem=ss, recv_sem=rs, device_id=to, device_id_type=MESH
        )

    def drain(like_ref, sem):
        pltpu.make_async_copy(like_ref, like_ref, sem).wait()

    partner = (head, hi * 2 + 1 - k)
    n1 = (xz16[0][0] + 1 - lo, grp)
    n2 = (xz16[0][0] + 1 - lo, (1 - hi) * 2 + k)
    across = (head, (1 - hi) * 2 + k)

    ins = [
        pltpu.make_async_copy(src, dst, sl.at[i])
        for i, (src, dst) in enumerate(
            (
                (ids_h, ids), (table_h, table), (bias_h, bias), (inw_h, inw),
                (byte_h, byte), (outt_h, outt), (tok_h, tok), (lab_h, lab),
            )
        )
    ]
    wc = [
        pltpu.make_async_copy(w_hbm.at[:, pl.ds(i * CW, CW)], w.at[:, pl.ds(i * CW, CW)], sw.at[i])
        for i in range(CH)
    ]
    for c in ins[:4] + wc + ins[4:]:
        c.start()

    bar = pltpu.get_barrier_semaphore()
    along_x = [(xz16[dx][0] + lo, grp) for dx in (2, 1, 3)]
    along_z = [(xz16[0][dz] + lo, grp) for dz in FAR[:7]]
    beside = [
        (xz16[0][0] + los[dl], his[dh] * 2 + ks[dk])
        for dl in range(2) for dh in range(2) for dk in range(2) if dl or dh or dk
    ]
    for to in along_z + along_x + beside:
        pl.semaphore_signal(bar, inc=1, device_id=to, device_id_type=MESH)

    m = iota((256, 256), 1)
    mhi, mx, mz, mp, mk = m % 2, (m // 2) % 4, (m // 8) % 8, (m // 64) % 2, m // 128
    owner = (mx * 16 + mz * 2 + (mp + mhi) % 2) * 4 + mhi * 2 + mk
    order = (iota((256, 256), 0) == owner).astype(BF)
    ins[0].wait()
    upper = ids[...] // 32
    halves = jnp.concatenate([upper, ids[...] - upper * 32], axis=0)
    halves = mm(jnp.broadcast_to(halves[:, None], (2, 8, 256)).reshape(16, 256).astype(F32), order, 1, 0)
    sorted_ids = (halves[0:1] * 32 + halves[8:9]).astype(jnp.int32)
    picks = (iota((1024, 256), 0) == sorted_ids).astype(F32).astype(BF)
    ins[1].wait()
    chosen = mm(picks, table[...], 0, 0).astype(BF)
    chosen_s[...] = chosen
    ins[2].wait()
    ins[3].wait()
    pre = mm(chosen, inw[...], 1, 0) + bias[...]
    hidden = jnp.maximum(pre, 0.0)
    hid[...] = hidden.astype(BF)

    for i in range(CH):
        cols = pl.ds(i * CW, CW)
        wc[i].wait()
        fs[:, :, :, :, cols] = jnp.dot(hid[...], w[:, cols], preferred_element_type=F32).reshape(
            2, 2, 8, 8, CW
        )

    pl.semaphore_wait(bar, 17)
    for to in along_x:
        pl.semaphore_signal(on_x, inc=1, device_id=to, device_id_type=MESH)

    c1 = []
    for dz in FAR:
        c = remote(fs.at[1 - k, :, zs[dz]], fr.at[:, zs[dz]], r1s, r1r.at[dz], partner)
        c.start()
        c1.append(c)
    ins[4].wait()
    ins[5].wait()
    gp[0:256, :] = mm(outt[...], byte[...], 1, 1)
    gp[256:512, :] = mm(outt[...], outt[...], 1, 1)
    gp[512:768, :] = mm(byte[...], byte[...], 1, 1)
    cg = remote(gp, gq, gs.at[0], gr.at[0], partner)
    cg.start()
    pl.semaphore_wait(on_x, 3)
    for to in along_z:
        pl.semaphore_signal(on_z, inc=1, device_id=to, device_id_type=MESH)
    is_a = x < 2
    stays = jnp.logical_not(is_a) & (hi == lo)
    parts = jnp.logical_not(is_a) & (hi != lo)
    moves = jnp.logical_not(stays)
    lo_b = jnp.where(is_a, 1 - lo, hi)
    diag = iota((256, 256), 0) == iota((256, 256), 1)
    ra = pl.ds(pl.multiple_of(k * 128 + x * 32, 32), 32)
    rb = pl.ds(pl.multiple_of(k * 256 + x * 64, 64), 64)
    cg2 = [
        remote(ga.at[ra], na.at[ra], gs.at[1], gr.at[1], n2),
        remote(gb.at[rb], nb.at[rb], gs.at[2], gr.at[2], n2),
        remote(gd, nd, gs.at[3], gr.at[7], n2),
    ]
    for i, dz in enumerate(FAR):
        c1[i].wait_recv()
        sb[:, zs[dz]] = (fs[k, :, zs[dz]] + fr[:, zs[dz]]).astype(BF)
        half = sb.at[1 - p, zs[dz]]
        pl.when(parts)(remote(half, r2.at[1, zs[dz]], r2s, r2r.at[1, dz], across).start)
        pl.when(jnp.logical_not(parts))(remote(half, r2.at[0, zs[dz]], r2s, r2r.at[0, dz], n1).start)
        pl.when(is_a)(remote(sb.at[p, zs[dz]], r2.at[1, zs[dz]], r2s, r2r.at[1, dz], n2).start)
        pl.when(parts)(remote(sb.at[p, zs[dz]], r2.at[2, zs[dz]], r2s, r2r.at[2, dz], n2).start)
        if i == 5:
            cg.wait_recv()
            gsum = gp[...] + gq[...]
            ga[...] = gsum[0:256]
            gd[...] = jnp.broadcast_to(
                jnp.sum(jnp.where(diag, gsum[512:768], 0.0), 0, keepdims=True), (8, 256)
            )
            gb[...] = gsum[256:768].astype(BF)
            for c in cg2:
                c.start()

    for d8 in range(8):
        perm = (iota((1024, 128), 0) == 8 * iota((1024, 128), 1) + d8).astype(F32)
        bp[:, d8 * 128 : (d8 + 1) * 128] = mm(byte[...], perm, 1, 0).astype(BF)
    ins[6].wait()
    ins[7].wait()
    tok_hot = (iota((256, 256), 0) == tok[...]).astype(F32)
    lab_hot = (iota((256, 256), 0) == lab[...]).astype(F32)
    ct = mm(lab_hot, tok_hot, 1, 1)
    cnt = jnp.sum(ct, 0, keepdims=True)
    hidt[...] = jnp.transpose(hid[...].astype(F32)).astype(BF)
    co = [pltpu.make_async_copy(hidt, hidt_o, so.at[0])]
    co[0].start()

    slots = [jnp.where(is_a, (rem(z, 4) * 2 + lo_b) * 2 + q, 16 + 8 * (x - 2) + z) for q in range(2)]
    hi_d = jnp.where(is_a, x, hi)
    lo_d = rem(p + hi_d, 2)
    cores = [jnp.where(is_a, div(z, 4), q) for q in range(2)]
    to_c = [hi_d * 2 + cores[q] for q in range(2)]
    mine = [to_c[q] == grp for q in range(2)]
    n_self = mine[0].astype(jnp.int32) + mine[1].astype(jnp.int32)
    pl.semaphore_wait(on_z, 7)
    for i, dz in enumerate(FAR):
        first = r2.at[0, zs[dz]]
        pl.when(moves)(pltpu.make_async_copy(first, first, r2r.at[0, dz]).wait)
        pl.when(jnp.logical_not(parts))(pltpu.make_async_copy(first, first, r2r.at[1, dz]).wait)
        pl.when(parts)(pltpu.make_async_copy(first, first, r2r.at[2, dz]).wait)
        second = jnp.where(parts, r2[2, zs[dz]], r2[1, zs[dz]])
        both = jnp.where(stays, sb[p, zs[dz]], r2[0, zs[dz]]).astype(F32) + second.astype(F32)
        for q in range(2):
            for j in range(8):
                at = (q * 8 + j) * 128
                ft[q, pl.ds(j, 8, stride=8), :] = both[:, at : at + 128]
            f[q, zs[dz]] = ft[q, 0:64].astype(BF).reshape(4, 2, 8, 128)
        for dx in FAR_X:
            for q in range(2):
                c = remote(
                    f.at[q, zs[dz], xs[dx]], rx.at[k, :, slots[q]], r3s, r3r, (xz16[dx][dz] + lo_d, to_c[q])
                )
                if dz or dx:
                    c.start()
                else:
                    pl.when(jnp.logical_not(mine[q]))(c.start)
    for c in cg2:
        c.wait_recv()
    for dx in (2, 1, 3):
        to = (xz16[dx][0] + lo, grp)
        remote(na.at[ra], na.at[ra], gs.at[1], gr.at[3], to).start()
        remote(nb.at[rb], nb.at[rb], gs.at[2], gr.at[4], to).start()
    for q in range(2):

        @pl.when(mine[q])
        def _(q=q):
            rx[k, :, slots[q]] = f[q, z, x]

    def wait_all(sem):
        for n in range(3):

            @pl.when(n_self == n)
            def _(n=n):
                piece = like.at[pl.ds(0, 64 - n)]
                pltpu.make_async_copy(piece, piece, sem).wait()

    wait_all(r3r)

    for c in range(4):
        at = jnp.transpose(rx[c // 2, c % 2, 0:16].astype(F32).reshape(128, 128))
        for d8 in range(8):
            la[c * 16 : (c + 1) * 16, d8 * 128 : (d8 + 1) * 128] = at[d8 * 16 : (d8 + 1) * 16].astype(BF)
        xf[c * 128 : (c + 1) * 128, :] = rx[c // 2, c % 2, 16:32].astype(F32).reshape(128, 128)
    for j in range(8):
        lb[:, j * 128 : (j + 1) * 128] = xf[pl.ds(j, 64, stride=8), :].astype(BF)
    pt = mm(la[...], bp[...], 1, 1)
    qt = mm(lb[...], outt[...], 1, 1)
    rt = mm(lb[...], byte[...], 1, 1)
    ss = mm(lb[...], lb[...], 1, 1)
    for c in range(4):
        rows = slice(c * 16, (c + 1) * 16)
        ms[c, 0:16, :] = pt[rows].astype(BF)
        ms[c, 16:32, :] = qt[rows].astype(BF)
        ms[c, 32:48, :] = rt[rows].astype(BF)
        ms[c, 48:64, :] = jnp.zeros((16, 256), BF)
        ms[c, 48:64, 0:16] = ss[rows, c * 16 : (c + 1) * 16].astype(BF)
    me = k * 2 + hi
    members = [
        (ks[o // 2] * 2 + his[o % 2], (xz16[0][0] + los[o % 2], his[o % 2] * 2 + ks[o // 2]))
        for o in range(4)
    ]
    for o in range(1, 4):
        c_, to = members[o]
        remote(ms.at[c_], er.at[o], e1s, e1r, to).start()
    drain(na.at[pl.ds(0, 96)], gr.at[3])
    drain(nb.at[pl.ds(0, 192)], gr.at[4])
    ha = pl.ds(pl.multiple_of(k * 128, 128), 128)
    hbb = pl.ds(pl.multiple_of(k * 256, 256), 256)
    cg3 = [
        remote(na.at[ha], na.at[ha], gs.at[1], gr.at[5], partner),
        remote(nb.at[hbb], nb.at[hbb], gs.at[2], gr.at[6], partner),
    ]
    for c in cg3:
        c.start()
    for c in cg3:
        c.wait_recv()
    obt = ga[...] + na[...]
    bb = gd[0:1, :] + nd[0:1, :]
    grams = gb[...].astype(F32) + nb[...].astype(F32)
    oo, bbm = grams[0:256].astype(BF), grams[256:512].astype(BF)
    scale = lax.rsqrt(bb * (1 / 4096) + EPS)
    own = ms[me].astype(F32)
    drain(er.at[pl.ds(1, 3)], e1r)
    for o in range(1, 4):
        own = own + er[o].astype(F32)
    u, xx, yy, zz, loss = two_steps(
        own[0:16], own[16:32], own[32:48], own[48:64, 0:16], obt, oo, bbm, bb, scale, ct, cnt
    )
    loss_o[0] = loss * (1 / 256)
    cm[0:16, :] = u.astype(BF)
    cm[16:32, :] = xx.astype(BF)
    cm[32:48, :] = yy.astype(BF)
    cm[48:64, :] = jnp.zeros((16, 256), BF)
    cm[48:64, 0:16] = zz.astype(BF)
    for o in range(1, 4):
        remote(cm, cr.at[me], e2s, e2r, members[o][1]).start()
    cr[me] = cm[...]
    drain(er.at[pl.ds(1, 3)], e2r)

    allc = cr[...]
    us = allc[:, 0:16].reshape(64, 256)
    xc = allc[:, 16:32].reshape(64, 256)
    yc = allc[:, 32:48].reshape(64, 256)
    dat = mm(us, bp[...], 1, 0)
    for c in range(4):
        for d8 in range(8):
            ta[d8 * 16 : (d8 + 1) * 16, :] = dat[c * 16 : (c + 1) * 16, d8 * 128 : (d8 + 1) * 128]
        tx[c // 2, c % 2, 0:16] = jnp.transpose(ta[...]).astype(BF).reshape(16, 8, 128)
    dbs = mm(xc, outt[...], 1, 0) + mm(yc, byte[...], 1, 0)
    zdb = [mm(cr[c, 48:64, 0:16], lb[c * 16 : (c + 1) * 16, :], 1, 0) for c in range(4)]
    dbs = dbs + jnp.concatenate(zdb, axis=0)
    for j in range(8):
        xf[pl.ds(j, 64, stride=8), :] = dbs[:, j * 128 : (j + 1) * 128]
    for c in range(4):
        tx[c // 2, c % 2, 16:32] = xf[c * 128 : (c + 1) * 128, :].astype(BF).reshape(16, 8, 128)

    def give(slot, k_, q_, to, back, near):
        c = remote(tx.at[k_, :, slot], g_in.at[q_, z, x], r4s, r4r.at[back], to)
        if near:
            pl.when(jnp.logical_not((to[0] == head) & (to[1] == grp)))(c.start)
        else:
            c.start()

    his_a = [rem(p + 1 - par, 2) for par in range(2)]
    for dz in NEAR:
        for xh in range(2):
            for dk in range(2):
                slot = 16 + xh * 8 + zs[dz]
                to = (32 + xh * 16 + zs[dz] * 2 + lo, hi * 2 + ks[dk])
                give(slot, ks[dk], k, to, (8 - dz) % 8, dz == 0)

        @pl.when(div(zs[dz], 4) == k)
        def _(dz=dz):
            for par in range(2):
                for q in range(2):
                    for dk in range(2):
                        slot = (rem(zs[dz], 4) * 2 + par) * 2 + q
                        to = (hi * 16 + zs[dz] * 2 + 1 - par, his_a[par] * 2 + ks[dk])
                        give(slot, ks[dk], q, to, (8 - dz) % 8, dz == 0)

    for q in range(2):

        @pl.when(mine[q])
        def _(q=q):
            g_in[q, z, x] = tx[k, :, slots[q]]

    for dz in NEAR:
        if dz:
            drain(like.at[pl.ds(0, 8)], r4r.at[dz])
        else:
            for n in range(3):

                @pl.when(n_self == n)
                def _(n=n):
                    drain(like.at[pl.ds(0, 8 - n)], r4r.at[0])

        part, spot = g_in.at[:, zs[dz]], d_in.at[k, p, :, zs[dz]]
        pl.when(moves)(remote(part, spot, r5s, r5r.at[0, dz], n1).start)
        pl.when(moves)(remote(part, spot, r5s, r5r.at[1, dz], n2).start)
        pl.when(stays)(remote(part, spot, r5s, r5r.at[2, dz], across).start)

    @pl.when(stays)
    def _():
        d_in[k, p] = g_in[...]

    for dz in NEAR:
        region = d_in.at[k, :, :, zs[dz]]
        one = d_in.at[k, 0, :, zs[dz]]
        pl.when(jnp.logical_not(parts))(pltpu.make_async_copy(one, one, r5r.at[0, dz]).wait)
        pl.when(moves)(pltpu.make_async_copy(one, one, r5r.at[1, dz]).wait)
        pl.when(parts)(pltpu.make_async_copy(one, one, r5r.at[2, dz]).wait)
        remote(region, region, r6s, r6r, partner).start()
    drain(d_in.at[1 - k], r6r)
    for kp in range(4):
        xd = d_in[kp // 2, kp % 2].astype(F32).reshape(1024, 128)
        ft[0] = xd[0:512]
        ft[1] = xd[512:1024]
        for j in range(16):
            dn[kp * 64 : (kp + 1) * 64, j * 128 : (j + 1) * 128] = ft[
                j // 8, pl.ds(j % 8, 64, stride=8), :
            ].astype(BF)
    co.append(pltpu.make_async_copy(dn, dn_o, so.at[1]))
    co[1].start()

    turn = [rem(zn - z + 14, 8) * 16 for zn in range(8)]
    for i in range(4):
        part = mm(w[i * 256 : (i + 1) * 256, :], dn[...], 1, 1).astype(BF)
        for l_ in range(2):
            for zn in range(8):
                at = l_ * 128 + zn * 16
                hb[i, l_, pl.ds(pl.multiple_of(turn[zn], 16), 16), :] = part[at : at + 16]
    peers = [(xs[o // 2], los[o % 2], (xz16[o // 2][0] + los[o % 2], grp)) for o in range(8)]
    for h in range(2):
        rows = pl.ds(h * 64, 64)
        for o in (4, 5, 2, 3, 6, 7, 1):
            x_, lo_, to = peers[o]
            remote(hb.at[x_, lo_, rows], a1.at[o, rows], p1s, p1r.at[h], to).start()
    for h in range(2):
        rows = pl.ds(h * 64, 64)
        acc = hb[x, lo, rows, :].astype(F32)
        drain(a1.at[pl.ds(1, 7), rows], p1r.at[h])
        for o in range(1, 8):
            acc = acc + a1[o, rows, :].astype(F32)
        a1s[rows, :] = acc.astype(BF)
        for t in ((2, 1, 3, 0), (4, 7, 5, 6))[h]:
            dz = (t + 2) % 8
            if dz:
                remote(a1s.at[pl.ds(t * 16, 16)], a2.at[dz], p2s, p2r, (xz16[0][dz] + lo, grp)).start()
    total = a1s[96:112, :].astype(F32)
    drain(a2.at[pl.ds(1, 7)], p2r)
    for dz in range(1, 8):
        total = total + a2[dz].astype(F32)
    base = pl.multiple_of(x * 256 + lo * 128, 128)
    row0 = pl.multiple_of(base + z * 16, 16)
    total = jnp.where(hidt[pl.ds(row0, 16), :].astype(F32) > 0, total, 0.0)
    big = total.astype(BF)
    small = (total - big.astype(F32)).astype(BF)
    piece = mm(big, chosen_s[...], 1, 0) + mm(small, chosen_s[...], 1, 0)
    ag[pl.ds(row0, 16), :] = piece.astype(BF)
    cd = {}
    own_rows = ag.at[pl.ds(row0, 16)]
    for dz in FAR[:7]:
        cd[dz] = remote(own_rows, own_rows, p3s, p3r.at[dz], (xz16[0][dz] + lo, grp))
        cd[dz].start()
    for dz in (0, 1, 7, 2, 6, 3, 5, 4):
        if dz:
            cd[dz].wait_recv()
        rows = ag.at[pl.ds(pl.multiple_of(base + zs[(8 - dz) % 8] * 16, 16), 16)]
        for o in (4, 5, 2, 3, 6, 7, 1):
            remote(rows, rows, p4s, p4r, peers[o][2]).start()
    drain(a1.at[pl.ds(1, 7)], p4r)
    co.append(pltpu.make_async_copy(ag, ag_o, so.at[2]))
    co[2].start()

    drain(fr, r1s)
    pl.when(stays)(pltpu.make_async_copy(r2.at[0], r2.at[0], r2s).wait)
    pl.when(moves)(pltpu.make_async_copy(r2.at[pl.ds(0, 2)], r2.at[pl.ds(0, 2)], r2s).wait)
    drain(gq, gs.at[0])
    drain(na, gs.at[1])
    drain(nb, gs.at[2])
    drain(nd, gs.at[3])
    drain(er.at[pl.ds(1, 3)], e1s)
    drain(er.at[pl.ds(1, 3)], e2s)
    pl.when(stays)(pltpu.make_async_copy(g_in, g_in, r5s).wait)
    pl.when(moves)(pltpu.make_async_copy(d_in.at[0], d_in.at[0], r5s).wait)
    drain(d_in.at[0], r6s)
    drain(a1.at[pl.ds(1, 7)], p1s)
    drain(a2.at[pl.ds(1, 7)], p2s)
    drain(a2.at[pl.ds(1, 7)], p3s)
    drain(a1.at[pl.ds(1, 7)], p4s)
    wait_all(r3s)
    wait_all(r4s)
    for c in co:
        c.wait()


def local(client_ids, client_table, in_weight, in_bias, head_weight, tokens, labels, byte_table, out_table):
    hbm = pl.BlockSpec(memory_space=pl.ANY)
    dma = pltpu.SemaphoreType.DMA
    V = pltpu.VMEM
    S = jax.ShapeDtypeStruct
    ag, dn, hidt, losses = pl.pallas_call(
        kernel,
        out_shape=(S((1024, 256), BF), S((256, 2048), BF), S((1024, 256), BF), S((1,), F32)),
        in_specs=[hbm] * 9,
        out_specs=(hbm, hbm, hbm, pl.BlockSpec(memory_space=pltpu.SMEM)),
        scratch_shapes=[
            V((1, 256), jnp.int32),
            V((1, 1024), F32),
            V((1, 256), jnp.int32),
            V((1, 256), jnp.int32),
            V((1024, 256), BF),
            V((256, 1024), BF),
            V((256, 1024), BF),
            V((256, 1024), BF),
            V((1024, 2048), BF),
            V((256, 1024), BF),
            V((2, 2, 8, 8, 2048), F32),
            V((2, 8, 8, 2048), F32),
            V((2, 8, 8, 2048), BF),
            V((3, 8, 8, 2048), BF),
            V((2, 512, 128), F32),
            V((2, 8, 4, 2, 8, 128), BF),
            V((2, 2, 32, 8, 128), BF),
            V((64, 1024), BF),
            V((64, 1024), BF),
            V((512, 128), F32),
            V((256, 1024), BF),
            V((768, 256), F32),
            V((768, 256), F32),
            V((256, 256), F32),
            V((512, 256), BF),
            V((256, 256), F32),
            V((512, 256), BF),
            V((8, 256), F32),
            V((8, 256), F32),
            V((4, 64, 256), BF),
            V((4, 64, 256), BF),
            V((64, 256), BF),
            V((4, 64, 256), BF),
            V((128, 128), F32),
            V((2, 2, 32, 8, 128), BF),
            V((2, 8, 4, 2, 8, 128), BF),
            V((2, 2, 2, 8, 4, 2, 8, 128), BF),
            V((256, 2048), BF),
            V((4, 2, 128, 256), BF),
            V((8, 128, 256), BF),
            V((128, 256), BF),
            V((8, 16, 256), BF),
            V((1024, 256), BF),
            V((1024, 256), BF),
            V((256, 256), BF),
            V((64, 2, 8, 128), BF),
            pltpu.SemaphoreType.REGULAR, pltpu.SemaphoreType.REGULAR,
            dma((8,)), dma((CH,)), dma((3,)),
            dma(()), dma((8,)),
            dma(()), dma((3, 8)),
            dma((4,)), dma((8,)),
            dma(()), dma(()),
            dma(()), dma(()), dma(()), dma(()),
            dma(()), dma((8,)),
            dma(()), dma((3, 8)), dma(()), dma(()),
            dma(()), dma((2,)), dma(()), dma(()),
            dma(()), dma((8,)), dma(()), dma(()),
        ],
        compiler_params=pltpu.CompilerParams(
            collective_id=0, has_side_effects=True, vmem_limit_bytes=60 * 1024 * 1024
        ),
        name="round",
    )(
        client_ids.reshape(1, 256), client_table, in_weight, in_bias.reshape(1, 1024), head_weight,
        tokens, labels, byte_table, out_table,
    )
    head_grad, in_grad = pl.pallas_call(
        tail_kernel,
        out_shape=(S((1024, 2048), BF), S((256, 1024), F32)),
        in_specs=[hbm] * 3,
        out_specs=(hbm, hbm),
        scratch_shapes=[
            V((1024, 256), BF), V((256, 2048), BF), V((1024, 256), BF),
            V((1024, 2048), BF), V((256, 1024), F32),
            dma((6,)), dma((5,)),
        ],
        compiler_params=pltpu.CompilerParams(vmem_limit_bytes=60 * 1024 * 1024),
        name="tail",
    )(hidt, dn, ag)
    return head_grad, in_grad, losses


def solution(mesh):
    placed = (
        P(),
        P(),
        P(None, "client"),
        P("client"),
        P("client", "head"),
        P(("head", "client"), None),
        P(("head", "client"), None),
        P(None, "client"),
        P(None, "client"),
    )
    return jax.shard_map(
        local,
        mesh=mesh,
        in_specs=placed,
        out_specs=(P("client", "head"), P(None, "client"), P(("head", "client"))),
        check_vma=False,
    )
```

```python
import jax
import jax.numpy as jnp
from jax import lax
from jax.experimental import pallas as pl
from jax.experimental.pallas import tpu as pltpu
from jax.sharding import PartitionSpec as P

EPS = 1e-6
ETA = 0.1
F32 = jnp.float32
BF = jnp.bfloat16
MESH = pl.DeviceIdType.MESH
CH = 4
CW = 2048 // CH


def mm(a, b, ca, cb):
    return lax.dot_general(
        a.astype(BF), b.astype(BF), (((ca,), (cb,)), ((), ())), preferred_element_type=F32
    )


def iota(shape, dim):
    return lax.broadcasted_iota(jnp.int32, shape, dim)


def gradients(pt, qt, rt, s_mat, obt, bb, scale, ct, cnt):
    tt = pt * (scale * (1 / 256))
    st = mm(s_mat, tt, 1, 0)
    msq = (bb + jnp.sum(tt * (2 * rt + st), 0, keepdims=True)) * (1 / 4096)
    q = lax.rsqrt(msq + EPS)
    mt = obt + mm(qt, tt, 0, 0)
    lg = mt * (q * (1 / 16))
    top = jnp.max(lg, 0, keepdims=True)
    ex = jnp.exp(lg - top)
    total = jnp.sum(ex, 0, keepdims=True)
    gt = (ex * (cnt / total) - ct) * (1 / 16)
    along = jnp.sum(gt * mt, 0, keepdims=True)
    e = q * q * q * along * (1 / 4096)
    ht = gt * q
    dt = mm(qt, ht, 1, 0) - e * (rt + st)
    ut = dt * (scale * (1 / 256))
    xt = mm(tt, ht, 1, 1)
    yt = tt * e
    z = mm(yt, tt, 1, 1)
    loss = jnp.sum(cnt * (top + jnp.log(total)) - jnp.sum(ct * lg, 0, keepdims=True))
    return ut, xt, yt, z, loss


def two_steps(pt, qt, rt, s_mat, obt, oo, bbm, bb, scale, ct, cnt):
    u1, x1, y1, z1, loss = gradients(pt, qt, rt, s_mat, obt, bb, scale, ct, cnt)
    vo = -ETA * mm(x1, oo, 1, 0) + ETA * mm(y1, obt, 1, 1)
    vb = -ETA * mm(x1, obt, 1, 0) + ETA * mm(y1, bbm, 1, 0)
    z1 = ETA * z1
    p2 = pt - ETA * mm(u1, bbm, 1, 0)
    q2 = qt + mm(z1, qt, 1, 0) + vo
    r2 = rt + mm(z1, rt, 1, 0) + vb
    h = -ETA * mm(qt, x1, 1, 1) + ETA * mm(rt, y1, 1, 1)
    ht = -ETA * mm(x1, qt, 1, 1) + ETA * mm(y1, rt, 1, 1)
    vv = -ETA * mm(x1, vo, 1, 1) + ETA * mm(y1, vb, 1, 1)
    zs = mm(z1, s_mat, 1, 0)
    s2 = s_mat + zs + mm(s_mat, z1, 1, 1) + mm(zs, z1, 1, 1)
    s2 = s2 + h + mm(z1, h, 1, 0) + ht + mm(ht, z1, 1, 1) + vv
    u2, x2, y2, z2, _ = gradients(p2, q2, r2, s2, obt, bb, scale, ct, cnt)
    z2 = ETA * z2
    u = -ETA * (u1 + u2)
    x = -ETA * (x1 + mm(z2, x1, 1, 0) + x2)
    y = ETA * (y1 + mm(z2, y1, 1, 0) + y2)
    z = z1 + z2 + mm(z2, z1, 1, 0)
    return u, x, y, z, loss

def tail_kernel(hidt, dn, ag, hg_o, ing_o, hv, dv, av, gv, iv, sem, osem):
    cols = [pl.ds(i * 512, 512) for i in range(4)]
    loads = [pltpu.make_async_copy(hidt, hv, sem.at[0])]
    loads += [pltpu.make_async_copy(dn.at[:, cols[i]], dv.at[:, cols[i]], sem.at[1 + i]) for i in range(4)]
    loads.append(pltpu.make_async_copy(ag, av, sem.at[5]))
    for c in loads:
        c.start()
    loads[0].wait()
    outs = []
    for i in range(4):
        loads[1 + i].wait()
        if i == 1:
            loads[5].wait()
            iv[...] = jnp.transpose(av[...].astype(F32))
        gv[:, cols[i]] = jnp.dot(hv[...], dv[:, cols[i]], preferred_element_type=F32).astype(BF)
        outs.append(pltpu.make_async_copy(gv.at[:, cols[i]], hg_o.at[:, cols[i]], osem.at[i]))
        outs[-1].start()
        if i == 1:
            outs.append(pltpu.make_async_copy(iv, ing_o, osem.at[4]))
            outs[-1].start()
    for c in outs:
        c.wait()


FAR = (4, 3, 5, 2, 6, 1, 7, 0)
FAR_X = (2, 1, 3, 0)
NEAR = (0, 1, 7, 2, 6, 3, 5, 4)


def kernel(
    ids_h, table_h, inw_h, bias_h, w_hbm, tok_h, lab_h, byte_h, outt_h,
    ag_o, dn_o, hidt_o, loss_o,
    ids, bias, tok, lab, table, inw, byte, outt,
    w, hid, fs, fr, sb, r2, ft, f, rx, la, lb, xf, bp, gp, gq, ga, gb, na, nb, gd, nd, ms, er, cm, cr, ta, tx, g_in,
    d_in, dn, hb, a1, a1s, a2, ag, hidt, chosen_s, like,
    on_x, on_z, sl, sw, so, r1s, r1r, r2s, r2r, gs, gr, r3s, r3r, e1s, e1r, e2s, e2r, r4s, r4r, r5s, r5r, r6s, r6r,
    p1s, p1r, p2s, p2r, p3s, p3r, p4s, p4r,
):
    rem, div = lax.rem, lax.div
    head = lax.axis_index("head")
    grp = lax.axis_index("client")
    x, z, lo = div(head, 16), rem(div(head, 2), 8), rem(head, 2)
    hi, k = div(grp, 2), rem(grp, 2)
    p = rem(hi + lo, 2)
    xs = [rem(x + d, 4) for d in range(4)]
    zs = [rem(z + d, 8) for d in range(8)]
    ks = [k, 1 - k]
    his = [hi, 1 - hi]
    los = [lo, 1 - lo]
    xz16 = [[xs[dx] * 16 + zs[dz] * 2 for dz in range(8)] for dx in range(4)]

    def remote(src, dst, ss, rs, to):
        return pltpu.make_async_remote_copy(
            src_ref=src, dst_ref=dst, send_sem=ss, recv_sem=rs, device_id=to, device_id_type=MESH
        )

    def drain(like_ref, sem):
        pltpu.make_async_copy(like_ref, like_ref, sem).wait()

    partner = (head, hi * 2 + 1 - k)
    n1 = (xz16[0][0] + 1 - lo, grp)
    n2 = (xz16[0][0] + 1 - lo, (1 - hi) * 2 + k)
    across = (head, (1 - hi) * 2 + k)

    ins = [
        pltpu.make_async_copy(src, dst, sl.at[i])
        for i, (src, dst) in enumerate(
            (
                (ids_h, ids), (table_h, table), (bias_h, bias), (inw_h, inw),
                (byte_h, byte), (outt_h, outt), (tok_h, tok), (lab_h, lab),
            )
        )
    ]
    wc = [
        pltpu.make_async_copy(w_hbm.at[:, pl.ds(i * CW, CW)], w.at[:, pl.ds(i * CW, CW)], sw.at[i])
        for i in range(CH)
    ]
    for c in ins[:4] + wc + ins[4:]:
        c.start()

    bar = pltpu.get_barrier_semaphore()
    along_x = [(xz16[dx][0] + lo, grp) for dx in (2, 1, 3)]
    along_z = [(xz16[0][dz] + lo, grp) for dz in FAR[:7]]
    beside = [
        (xz16[0][0] + los[dl], his[dh] * 2 + ks[dk])
        for dl in range(2) for dh in range(2) for dk in range(2) if dl or dh or dk
    ]
    for to in along_z + along_x + beside:
        pl.semaphore_signal(bar, inc=1, device_id=to, device_id_type=MESH)

    m = iota((256, 256), 1)
    mhi, mx, mz, mp, mk = m % 2, (m // 2) % 4, (m // 8) % 8, (m // 64) % 2, m // 128
    owner = (mx * 16 + mz * 2 + (mp + mhi) % 2) * 4 + mhi * 2 + mk
    order = (iota((256, 256), 0) == owner).astype(BF)
    ins[0].wait()
    upper = ids[...] // 32
    halves = jnp.concatenate([upper, ids[...] - upper * 32], axis=0)
    halves = mm(jnp.broadcast_to(halves[:, None], (2, 8, 256)).reshape(16, 256).astype(F32), order, 1, 0)
    sorted_ids = (halves[0:1] * 32 + halves[8:9]).astype(jnp.int32)
    picks = (iota((1024, 256), 0) == sorted_ids).astype(F32).astype(BF)
    ins[1].wait()
    chosen = mm(picks, table[...], 0, 0).astype(BF)
    chosen_s[...] = chosen
    ins[2].wait()
    ins[3].wait()
    pre = mm(chosen, inw[...], 1, 0) + bias[...]
    hidden = jnp.maximum(pre, 0.0)
    hid[...] = hidden.astype(BF)

    for i in range(CH):
        cols = pl.ds(i * CW, CW)
        wc[i].wait()
        fs[:, :, :, :, cols] = jnp.dot(hid[...], w[:, cols], preferred_element_type=F32).reshape(
            2, 2, 8, 8, CW
        )

    pl.semaphore_wait(bar, 17)
    for to in along_x:
        pl.semaphore_signal(on_x, inc=1, device_id=to, device_id_type=MESH)

    c1 = []
    for dz in FAR:
        c = remote(fs.at[1 - k, :, zs[dz]], fr.at[:, zs[dz]], r1s, r1r.at[dz], partner)
        c.start()
        c1.append(c)
    ins[4].wait()
    ins[5].wait()
    gp[0:256, :] = mm(outt[...], byte[...], 1, 1)
    gp[256:512, :] = mm(outt[...], outt[...], 1, 1)
    gp[512:768, :] = mm(byte[...], byte[...], 1, 1)
    cg = remote(gp, gq, gs.at[0], gr.at[0], partner)
    cg.start()
    pl.semaphore_wait(on_x, 3)
    for to in along_z:
        pl.semaphore_signal(on_z, inc=1, device_id=to, device_id_type=MESH)
    is_a = x < 2
    stays = jnp.logical_not(is_a) & (hi == lo)
    parts = jnp.logical_not(is_a) & (hi != lo)
    moves = jnp.logical_not(stays)
    lo_b = jnp.where(is_a, 1 - lo, hi)
    diag = iota((256, 256), 0) == iota((256, 256), 1)
    ra = pl.ds(pl.multiple_of(k * 128 + x * 32, 32), 32)
    rb = pl.ds(pl.multiple_of(k * 256 + x * 64, 64), 64)
    cg2 = [
        remote(ga.at[ra], na.at[ra], gs.at[1], gr.at[1], n2),
        remote(gb.at[rb], nb.at[rb], gs.at[2], gr.at[2], n2),
        remote(gd, nd, gs.at[3], gr.at[7], n2),
    ]
    for i, dz in enumerate(FAR):
        c1[i].wait_recv()
        sb[:, zs[dz]] = (fs[k, :, zs[dz]] + fr[:, zs[dz]]).astype(BF)
        half = sb.at[1 - p, zs[dz]]
        pl.when(parts)(remote(half, r2.at[1, zs[dz]], r2s, r2r.at[1, dz], across).start)
        pl.when(jnp.logical_not(parts))(remote(half, r2.at[0, zs[dz]], r2s, r2r.at[0, dz], n1).start)
        pl.when(is_a)(remote(sb.at[p, zs[dz]], r2.at[1, zs[dz]], r2s, r2r.at[1, dz], n2).start)
        pl.when(parts)(remote(sb.at[p, zs[dz]], r2.at[2, zs[dz]], r2s, r2r.at[2, dz], n2).start)
        if i == 5:
            cg.wait_recv()
            gsum = gp[...] + gq[...]
            ga[...] = gsum[0:256]
            gd[...] = jnp.broadcast_to(
                jnp.sum(jnp.where(diag, gsum[512:768], 0.0), 0, keepdims=True), (8, 256)
            )
            gb[...] = gsum[256:768].astype(BF)
            for c in cg2:
                c.start()

    for d8 in range(8):
        perm = (iota((1024, 128), 0) == 8 * iota((1024, 128), 1) + d8).astype(F32)
        bp[:, d8 * 128 : (d8 + 1) * 128] = mm(byte[...], perm, 1, 0).astype(BF)
    ins[6].wait()
    ins[7].wait()
    tok_hot = (iota((256, 256), 0) == tok[...]).astype(F32)
    lab_hot = (iota((256, 256), 0) == lab[...]).astype(F32)
    ct = mm(lab_hot, tok_hot, 1, 1)
    cnt = jnp.sum(ct, 0, keepdims=True)
    hidt[...] = jnp.transpose(hid[...].astype(F32)).astype(BF)
    co = [pltpu.make_async_copy(hidt, hidt_o, so.at[0])]
    co[0].start()

    slots = [jnp.where(is_a, (rem(z, 4) * 2 + lo_b) * 2 + q, 16 + 8 * (x - 2) + z) for q in range(2)]
    hi_d = jnp.where(is_a, x, hi)
    lo_d = rem(p + hi_d, 2)
    cores = [jnp.where(is_a, div(z, 4), q) for q in range(2)]
    to_c = [hi_d * 2 + cores[q] for q in range(2)]
    mine = [to_c[q] == grp for q in range(2)]
    n_self = mine[0].astype(jnp.int32) + mine[1].astype(jnp.int32)
    pl.semaphore_wait(on_z, 7)
    for i, dz in enumerate(FAR):
        first = r2.at[0, zs[dz]]
        pl.when(moves)(pltpu.make_async_copy(first, first, r2r.at[0, dz]).wait)
        pl.when(jnp.logical_not(parts))(pltpu.make_async_copy(first, first, r2r.at[1, dz]).wait)
        pl.when(parts)(pltpu.make_async_copy(first, first, r2r.at[2, dz]).wait)
        second = jnp.where(parts, r2[2, zs[dz]], r2[1, zs[dz]])
        both = jnp.where(stays, sb[p, zs[dz]], r2[0, zs[dz]]).astype(F32) + second.astype(F32)
        for q in range(2):
            for j in range(8):
                at = (q * 8 + j) * 128
                ft[q, pl.ds(j, 8, stride=8), :] = both[:, at : at + 128]
            f[q, zs[dz]] = ft[q, 0:64].astype(BF).reshape(4, 2, 8, 128)
        for dx in FAR_X:
            for q in range(2):
                c = remote(
                    f.at[q, zs[dz], xs[dx]], rx.at[k, :, slots[q]], r3s, r3r, (xz16[dx][dz] + lo_d, to_c[q])
                )
                if dz or dx:
                    c.start()
                else:
                    pl.when(jnp.logical_not(mine[q]))(c.start)
    for c in cg2:
        c.wait_recv()
    for dx in (2, 1, 3):
        to = (xz16[dx][0] + lo, grp)
        remote(na.at[ra], na.at[ra], gs.at[1], gr.at[3], to).start()
        remote(nb.at[rb], nb.at[rb], gs.at[2], gr.at[4], to).start()
    for q in range(2):

        @pl.when(mine[q])
        def _(q=q):
            rx[k, :, slots[q]] = f[q, z, x]

    def wait_all(sem):
        for n in range(3):

            @pl.when(n_self == n)
            def _(n=n):
                piece = like.at[pl.ds(0, 64 - n)]
                pltpu.make_async_copy(piece, piece, sem).wait()

    wait_all(r3r)

    for c in range(4):
        at = jnp.transpose(rx[c // 2, c % 2, 0:16].astype(F32).reshape(128, 128))
        for d8 in range(8):
            la[c * 16 : (c + 1) * 16, d8 * 128 : (d8 + 1) * 128] = at[d8 * 16 : (d8 + 1) * 16].astype(BF)
        xf[c * 128 : (c + 1) * 128, :] = rx[c // 2, c % 2, 16:32].astype(F32).reshape(128, 128)
    for j in range(8):
        lb[:, j * 128 : (j + 1) * 128] = xf[pl.ds(j, 64, stride=8), :].astype(BF)
    pt = mm(la[...], bp[...], 1, 1)
    qt = mm(lb[...], outt[...], 1, 1)
    rt = mm(lb[...], byte[...], 1, 1)
    ss = mm(lb[...], lb[...], 1, 1)
    for c in range(4):
        rows = slice(c * 16, (c + 1) * 16)
        ms[c, 0:16, :] = pt[rows].astype(BF)
        ms[c, 16:32, :] = qt[rows].astype(BF)
        ms[c, 32:48, :] = rt[rows].astype(BF)
        ms[c, 48:64, :] = jnp.zeros((16, 256), BF)
        ms[c, 48:64, 0:16] = ss[rows, c * 16 : (c + 1) * 16].astype(BF)
    me = k * 2 + hi
    members = [
        (ks[o // 2] * 2 + his[o % 2], (xz16[0][0] + los[o % 2], his[o % 2] * 2 + ks[o // 2]))
        for o in range(4)
    ]
    for o in range(1, 4):
        c_, to = members[o]
        remote(ms.at[c_], er.at[o], e1s, e1r, to).start()
    drain(na.at[pl.ds(0, 96)], gr.at[3])
    drain(nb.at[pl.ds(0, 192)], gr.at[4])
    ha = pl.ds(pl.multiple_of(k * 128, 128), 128)
    hbb = pl.ds(pl.multiple_of(k * 256, 256), 256)
    cg3 = [
        remote(na.at[ha], na.at[ha], gs.at[1], gr.at[5], partner),
        remote(nb.at[hbb], nb.at[hbb], gs.at[2], gr.at[6], partner),
    ]
    for c in cg3:
        c.start()
    for c in cg3:
        c.wait_recv()
    obt = ga[...] + na[...]
    bb = gd[0:1, :] + nd[0:1, :]
    grams = gb[...].astype(F32) + nb[...].astype(F32)
    oo, bbm = grams[0:256].astype(BF), grams[256:512].astype(BF)
    scale = lax.rsqrt(bb * (1 / 4096) + EPS)
    own = ms[me].astype(F32)
    drain(er.at[pl.ds(1, 3)], e1r)
    for o in range(1, 4):
        own = own + er[o].astype(F32)
    u, xx, yy, zz, loss = two_steps(
        own[0:16], own[16:32], own[32:48], own[48:64, 0:16], obt, oo, bbm, bb, scale, ct, cnt
    )
    loss_o[0] = loss * (1 / 256)
    cm[0:16, :] = u.astype(BF)
    cm[16:32, :] = xx.astype(BF)
    cm[32:48, :] = yy.astype(BF)
    cm[48:64, :] = jnp.zeros((16, 256), BF)
    cm[48:64, 0:16] = zz.astype(BF)
    for o in range(1, 4):
        remote(cm, cr.at[me], e2s, e2r, members[o][1]).start()
    cr[me] = cm[...]
    drain(er.at[pl.ds(1, 3)], e2r)

    allc = cr[...]
    us = allc[:, 0:16].reshape(64, 256)
    xc = allc[:, 16:32].reshape(64, 256)
    yc = allc[:, 32:48].reshape(64, 256)
    dat = mm(us, bp[...], 1, 0)
    for c in range(4):
        for d8 in range(8):
            ta[d8 * 16 : (d8 + 1) * 16, :] = dat[c * 16 : (c + 1) * 16, d8 * 128 : (d8 + 1) * 128]
        tx[c // 2, c % 2, 0:16] = jnp.transpose(ta[...]).astype(BF).reshape(16, 8, 128)
    dbs = mm(xc, outt[...], 1, 0) + mm(yc, byte[...], 1, 0)
    zdb = [mm(cr[c, 48:64, 0:16], lb[c * 16 : (c + 1) * 16, :], 1, 0) for c in range(4)]
    dbs = dbs + jnp.concatenate(zdb, axis=0)
    for j in range(8):
        xf[pl.ds(j, 64, stride=8), :] = dbs[:, j * 128 : (j + 1) * 128]
    for c in range(4):
        tx[c // 2, c % 2, 16:32] = xf[c * 128 : (c + 1) * 128, :].astype(BF).reshape(16, 8, 128)

    def give(slot, k_, q_, to, back, near):
        c = remote(tx.at[k_, :, slot], g_in.at[q_, z, x], r4s, r4r.at[back], to)
        if near:
            pl.when(jnp.logical_not((to[0] == head) & (to[1] == grp)))(c.start)
        else:
            c.start()

    his_a = [rem(p + 1 - par, 2) for par in range(2)]
    for dz in NEAR:
        for xh in range(2):
            for dk in range(2):
                slot = 16 + xh * 8 + zs[dz]
                to = (32 + xh * 16 + zs[dz] * 2 + lo, hi * 2 + ks[dk])
                give(slot, ks[dk], k, to, (8 - dz) % 8, dz == 0)

        @pl.when(div(zs[dz], 4) == k)
        def _(dz=dz):
            for par in range(2):
                for q in range(2):
                    for dk in range(2):
                        slot = (rem(zs[dz], 4) * 2 + par) * 2 + q
                        to = (hi * 16 + zs[dz] * 2 + 1 - par, his_a[par] * 2 + ks[dk])
                        give(slot, ks[dk], q, to, (8 - dz) % 8, dz == 0)

    for q in range(2):

        @pl.when(mine[q])
        def _(q=q):
            g_in[q, z, x] = tx[k, :, slots[q]]

    for dz in NEAR:
        if dz:
            drain(like.at[pl.ds(0, 8)], r4r.at[dz])
        else:
            for n in range(3):

                @pl.when(n_self == n)
                def _(n=n):
                    drain(like.at[pl.ds(0, 8 - n)], r4r.at[0])

        part, spot = g_in.at[:, zs[dz]], d_in.at[k, p, :, zs[dz]]
        pl.when(moves)(remote(part, spot, r5s, r5r.at[0, dz], n1).start)
        pl.when(moves)(remote(part, spot, r5s, r5r.at[1, dz], n2).start)
        pl.when(stays)(remote(part, spot, r5s, r5r.at[2, dz], across).start)

    @pl.when(stays)
    def _():
        d_in[k, p] = g_in[...]

    for dz in NEAR:
        region = d_in.at[k, :, :, zs[dz]]
        one = d_in.at[k, 0, :, zs[dz]]
        pl.when(jnp.logical_not(parts))(pltpu.make_async_copy(one, one, r5r.at[0, dz]).wait)
        pl.when(moves)(pltpu.make_async_copy(one, one, r5r.at[1, dz]).wait)
        pl.when(parts)(pltpu.make_async_copy(one, one, r5r.at[2, dz]).wait)
        remote(region, region, r6s, r6r, partner).start()
    turn = [rem(zn - z + 14, 8) * 16 for zn in range(8)]
    peers = [(xs[o // 2], los[o % 2], (xz16[o // 2][0] + los[o % 2], grp)) for o in range(8)]
    for half in range(2):
        if half:
            drain(d_in.at[1 - k], r6r)
        row = pl.multiple_of(ks[half] * 128, 128)
        for p_ in range(2):
            xd = d_in[ks[half], p_].astype(F32).reshape(1024, 128)
            ft[0] = xd[0:512]
            ft[1] = xd[512:1024]
            for j in range(16):
                dn[pl.ds(row + p_ * 64, 64), j * 128 : (j + 1) * 128] = ft[
                    j // 8, pl.ds(j % 8, 64, stride=8), :
                ].astype(BF)
        for i in range(4):
            part = mm(w[i * 256 : (i + 1) * 256, :], dn[pl.ds(row, 128), :], 1, 1).astype(BF)
            for l_ in range(2):
                for zn in range(8):
                    at = l_ * 128 + zn * 16
                    hb[half, i, l_, pl.ds(pl.multiple_of(turn[zn], 16), 16), :] = part[at : at + 16]
        for h in range(2):
            rows = pl.ds(h * 64, 64)
            for o in (4, 5, 2, 3, 6, 7, 1):
                x_, lo_, to = peers[o]
                src = hb.at[half, x_, lo_, rows]
                remote(src, a1.at[half, o, rows], p1s, p1r.at[half, h], to).start()
    co.append(pltpu.make_async_copy(dn, dn_o, so.at[1]))
    co[1].start()
    for h in range(2):
        rows = pl.ds(h * 64, 64)
        for half in range(2):
            acc = hb[half, x, lo, rows, :].astype(F32)
            drain(a1.at[half, pl.ds(1, 7), rows], p1r.at[half, h])
            for o in range(1, 8):
                acc = acc + a1[half, o, rows, :].astype(F32)
            a1s[rows, pl.ds(pl.multiple_of(ks[half] * 128, 128), 128)] = acc.astype(BF)
        for t in ((2, 1, 3, 0), (4, 7, 5, 6))[h]:
            dz = (t + 2) % 8
            if dz:
                remote(a1s.at[pl.ds(t * 16, 16)], a2.at[dz], p2s, p2r, (xz16[0][dz] + lo, grp)).start()
    total = a1s[96:112, :].astype(F32)
    drain(a2.at[pl.ds(1, 7)], p2r)
    for dz in range(1, 8):
        total = total + a2[dz].astype(F32)
    base = pl.multiple_of(x * 256 + lo * 128, 128)
    row0 = pl.multiple_of(base + z * 16, 16)
    total = jnp.where(hidt[pl.ds(row0, 16), :].astype(F32) > 0, total, 0.0)
    big = total.astype(BF)
    small = (total - big.astype(F32)).astype(BF)
    piece = mm(big, chosen_s[...], 1, 0) + mm(small, chosen_s[...], 1, 0)
    ag[pl.ds(row0, 16), :] = piece.astype(BF)
    cd = {}
    own_rows = ag.at[pl.ds(row0, 16)]
    for dz in FAR[:7]:
        cd[dz] = remote(own_rows, own_rows, p3s, p3r.at[dz], (xz16[0][dz] + lo, grp))
        cd[dz].start()
    for dz in (0, 1, 7, 2, 6, 3, 5, 4):
        if dz:
            cd[dz].wait_recv()
        rows = ag.at[pl.ds(pl.multiple_of(base + zs[(8 - dz) % 8] * 16, 16), 16)]
        for o in (4, 5, 2, 3, 6, 7, 1):
            remote(rows, rows, p4s, p4r, peers[o][2]).start()
    drain(a1.at[:, pl.ds(1, 7)], p4r)
    co.append(pltpu.make_async_copy(ag, ag_o, so.at[2]))
    co[2].start()

    drain(fr, r1s)
    pl.when(stays)(pltpu.make_async_copy(r2.at[0], r2.at[0], r2s).wait)
    pl.when(moves)(pltpu.make_async_copy(r2.at[pl.ds(0, 2)], r2.at[pl.ds(0, 2)], r2s).wait)
    drain(gq, gs.at[0])
    drain(na, gs.at[1])
    drain(nb, gs.at[2])
    drain(nd, gs.at[3])
    drain(er.at[pl.ds(1, 3)], e1s)
    drain(er.at[pl.ds(1, 3)], e2s)
    pl.when(stays)(pltpu.make_async_copy(g_in, g_in, r5s).wait)
    pl.when(moves)(pltpu.make_async_copy(d_in.at[0], d_in.at[0], r5s).wait)
    drain(d_in.at[0], r6s)
    drain(a1.at[:, pl.ds(1, 7)], p1s)
    drain(a2.at[pl.ds(1, 7)], p2s)
    drain(a2.at[pl.ds(1, 7)], p3s)
    drain(a1.at[:, pl.ds(1, 7)], p4s)
    wait_all(r3s)
    wait_all(r4s)
    for c in co:
        c.wait()


def local(client_ids, client_table, in_weight, in_bias, head_weight, tokens, labels, byte_table, out_table):
    hbm = pl.BlockSpec(memory_space=pl.ANY)
    dma = pltpu.SemaphoreType.DMA
    V = pltpu.VMEM
    S = jax.ShapeDtypeStruct
    ag, dn, hidt, losses = pl.pallas_call(
        kernel,
        out_shape=(S((1024, 256), BF), S((256, 2048), BF), S((1024, 256), BF), S((1,), F32)),
        in_specs=[hbm] * 9,
        out_specs=(hbm, hbm, hbm, pl.BlockSpec(memory_space=pltpu.SMEM)),
        scratch_shapes=[
            V((1, 256), jnp.int32),
            V((1, 1024), F32),
            V((1, 256), jnp.int32),
            V((1, 256), jnp.int32),
            V((1024, 256), BF),
            V((256, 1024), BF),
            V((256, 1024), BF),
            V((256, 1024), BF),
            V((1024, 2048), BF),
            V((256, 1024), BF),
            V((2, 2, 8, 8, 2048), F32),
            V((2, 8, 8, 2048), F32),
            V((2, 8, 8, 2048), BF),
            V((3, 8, 8, 2048), BF),
            V((2, 512, 128), F32),
            V((2, 8, 4, 2, 8, 128), BF),
            V((2, 2, 32, 8, 128), BF),
            V((64, 1024), BF),
            V((64, 1024), BF),
            V((512, 128), F32),
            V((256, 1024), BF),
            V((768, 256), F32),
            V((768, 256), F32),
            V((256, 256), F32),
            V((512, 256), BF),
            V((256, 256), F32),
            V((512, 256), BF),
            V((8, 256), F32),
            V((8, 256), F32),
            V((4, 64, 256), BF),
            V((4, 64, 256), BF),
            V((64, 256), BF),
            V((4, 64, 256), BF),
            V((128, 128), F32),
            V((2, 2, 32, 8, 128), BF),
            V((2, 8, 4, 2, 8, 128), BF),
            V((2, 2, 2, 8, 4, 2, 8, 128), BF),
            V((256, 2048), BF),
            V((2, 4, 2, 128, 128), BF),
            V((2, 8, 128, 128), BF),
            V((128, 256), BF),
            V((8, 16, 256), BF),
            V((1024, 256), BF),
            V((1024, 256), BF),
            V((256, 256), BF),
            V((64, 2, 8, 128), BF),
            pltpu.SemaphoreType.REGULAR, pltpu.SemaphoreType.REGULAR,
            dma((8,)), dma((CH,)), dma((3,)),
            dma(()), dma((8,)),
            dma(()), dma((3, 8)),
            dma((4,)), dma((8,)),
            dma(()), dma(()),
            dma(()), dma(()), dma(()), dma(()),
            dma(()), dma((8,)),
            dma(()), dma((3, 8)), dma(()), dma(()),
            dma(()), dma((2, 2)), dma(()), dma(()),
            dma(()), dma((8,)), dma(()), dma(()),
        ],
        compiler_params=pltpu.CompilerParams(
            collective_id=0, has_side_effects=True, vmem_limit_bytes=60 * 1024 * 1024
        ),
        name="round",
    )(
        client_ids.reshape(1, 256), client_table, in_weight, in_bias.reshape(1, 1024), head_weight,
        tokens, labels, byte_table, out_table,
    )
    head_grad, in_grad = pl.pallas_call(
        tail_kernel,
        out_shape=(S((1024, 2048), BF), S((256, 1024), F32)),
        in_specs=[hbm] * 3,
        out_specs=(hbm, hbm),
        scratch_shapes=[
            V((1024, 256), BF), V((256, 2048), BF), V((1024, 256), BF),
            V((1024, 2048), BF), V((256, 1024), F32),
            dma((6,)), dma((5,)),
        ],
        compiler_params=pltpu.CompilerParams(vmem_limit_bytes=60 * 1024 * 1024),
        name="tail",
    )(hidt, dn, ag)
    return head_grad, in_grad, losses


def solution(mesh):
    placed = (
        P(),
        P(),
        P(None, "client"),
        P("client"),
        P("client", "head"),
        P(("head", "client"), None),
        P(("head", "client"), None),
        P(None, "client"),
        P(None, "client"),
    )
    return jax.shard_map(
        local,
        mesh=mesh,
        in_specs=placed,
        out_specs=(P("client", "head"), P(None, "client"), P(("head", "client"))),
        check_vma=False,
    )
```

```python
import jax
import jax.numpy as jnp
from jax import lax
from jax.experimental import pallas as pl
from jax.experimental.pallas import tpu as pltpu
from jax.sharding import PartitionSpec as P

EPS = 1e-6
ETA = 0.1
F32 = jnp.float32
BF = jnp.bfloat16
MESH = pl.DeviceIdType.MESH
CH = 4
CW = 2048 // CH


def mm(a, b, ca, cb):
    return lax.dot_general(
        a.astype(BF), b.astype(BF), (((ca,), (cb,)), ((), ())), preferred_element_type=F32
    )


def iota(shape, dim):
    return lax.broadcasted_iota(jnp.int32, shape, dim)


def gradients(pt, qt, rt, s_mat, obt, bb, scale, ct, cnt):
    tt = pt * (scale * (1 / 256))
    st = mm(s_mat, tt, 1, 0)
    msq = (bb + jnp.sum(tt * (2 * rt + st), 0, keepdims=True)) * (1 / 4096)
    q = lax.rsqrt(msq + EPS)
    mt = obt + mm(qt, tt, 0, 0)
    lg = mt * (q * (1 / 16))
    top = jnp.max(lg, 0, keepdims=True)
    ex = jnp.exp(lg - top)
    total = jnp.sum(ex, 0, keepdims=True)
    gt = (ex * (cnt / total) - ct) * (1 / 16)
    along = jnp.sum(gt * mt, 0, keepdims=True)
    e = q * q * q * along * (1 / 4096)
    ht = gt * q
    dt = mm(qt, ht, 1, 0) - e * (rt + st)
    ut = dt * (scale * (1 / 256))
    xt = mm(tt, ht, 1, 1)
    yt = tt * e
    z = mm(yt, tt, 1, 1)
    loss = jnp.sum(cnt * (top + jnp.log(total)) - jnp.sum(ct * lg, 0, keepdims=True))
    return ut, xt, yt, z, loss


def two_steps(pt, qt, rt, s_mat, obt, oo, bbm, bb, scale, ct, cnt):
    u1, x1, y1, z1, loss = gradients(pt, qt, rt, s_mat, obt, bb, scale, ct, cnt)
    vo = -ETA * mm(x1, oo, 1, 0) + ETA * mm(y1, obt, 1, 1)
    vb = -ETA * mm(x1, obt, 1, 0) + ETA * mm(y1, bbm, 1, 0)
    z1 = ETA * z1
    p2 = pt - ETA * mm(u1, bbm, 1, 0)
    q2 = qt + mm(z1, qt, 1, 0) + vo
    r2 = rt + mm(z1, rt, 1, 0) + vb
    h = -ETA * mm(qt, x1, 1, 1) + ETA * mm(rt, y1, 1, 1)
    ht = -ETA * mm(x1, qt, 1, 1) + ETA * mm(y1, rt, 1, 1)
    vv = -ETA * mm(x1, vo, 1, 1) + ETA * mm(y1, vb, 1, 1)
    zs = mm(z1, s_mat, 1, 0)
    s2 = s_mat + zs + mm(s_mat, z1, 1, 1) + mm(zs, z1, 1, 1)
    s2 = s2 + h + mm(z1, h, 1, 0) + ht + mm(ht, z1, 1, 1) + vv
    u2, x2, y2, z2, _ = gradients(p2, q2, r2, s2, obt, bb, scale, ct, cnt)
    z2 = ETA * z2
    u = -ETA * (u1 + u2)
    x = -ETA * (x1 + mm(z2, x1, 1, 0) + x2)
    y = ETA * (y1 + mm(z2, y1, 1, 0) + y2)
    z = z1 + z2 + mm(z2, z1, 1, 0)
    return u, x, y, z, loss

def tail_kernel(hidt, dn, ag, hg_o, ing_o, hv, dv, av, gv, iv, sem, osem):
    cols = [pl.ds(i * 512, 512) for i in range(4)]
    loads = [pltpu.make_async_copy(hidt, hv, sem.at[0])]
    loads += [pltpu.make_async_copy(dn.at[:, cols[i]], dv.at[:, cols[i]], sem.at[1 + i]) for i in range(4)]
    loads.append(pltpu.make_async_copy(ag, av, sem.at[5]))
    for c in loads:
        c.start()
    loads[0].wait()
    outs = []
    for i in range(4):
        loads[1 + i].wait()
        if i == 1:
            loads[5].wait()
            iv[...] = jnp.transpose(av[...].astype(F32))
        gv[:, cols[i]] = jnp.dot(hv[...], dv[:, cols[i]], preferred_element_type=F32).astype(BF)
        outs.append(pltpu.make_async_copy(gv.at[:, cols[i]], hg_o.at[:, cols[i]], osem.at[i]))
        outs[-1].start()
        if i == 1:
            outs.append(pltpu.make_async_copy(iv, ing_o, osem.at[4]))
            outs[-1].start()
    for c in outs:
        c.wait()


FAR = (4, 3, 5, 2, 6, 1, 7, 0)
FAR_X = (2, 1, 3, 0)
NEAR = (0, 1, 7, 2, 6, 3, 5, 4)


def kernel(
    ids_h, table_h, inw_h, bias_h, w_hbm, tok_h, lab_h, byte_h, outt_h,
    ag_o, dn_o, hidt_o, loss_o,
    ids, bias, tok, lab, table, inw, byte, outt,
    w, hid, fs, fr, sb, r2, ft, f, rx, la, lb, xf, bp, gp, gq, ga, gb, na, nb, gd, nd, ms, er, cm, cr, ta, tx, g_in,
    d_in, dn, hb, a1, a1s, a2, ag, hidt, chosen_s, like,
    on_x, on_z, sl, sw, so, r1s, r1r, r2s, r2r, gs, gr, r3s, r3r, e1s, e1r, e2s, e2r, r4s, r4r, r5s, r5r, r6s, r6r,
    p1s, p1r, p2s, p2r, p3s, p3r, p4s, p4r,
):
    rem, div = lax.rem, lax.div
    head = lax.axis_index("head")
    grp = lax.axis_index("client")
    x, z, lo = div(head, 16), rem(div(head, 2), 8), rem(head, 2)
    hi, k = div(grp, 2), rem(grp, 2)
    p = rem(hi + lo, 2)
    xs = [rem(x + d, 4) for d in range(4)]
    zs = [rem(z + d, 8) for d in range(8)]
    ks = [k, 1 - k]
    his = [hi, 1 - hi]
    los = [lo, 1 - lo]
    xz16 = [[xs[dx] * 16 + zs[dz] * 2 for dz in range(8)] for dx in range(4)]

    def remote(src, dst, ss, rs, to):
        return pltpu.make_async_remote_copy(
            src_ref=src, dst_ref=dst, send_sem=ss, recv_sem=rs, device_id=to, device_id_type=MESH
        )

    def drain(like_ref, sem):
        pltpu.make_async_copy(like_ref, like_ref, sem).wait()

    partner = (head, hi * 2 + 1 - k)
    n1 = (xz16[0][0] + 1 - lo, grp)
    n2 = (xz16[0][0] + 1 - lo, (1 - hi) * 2 + k)
    across = (head, (1 - hi) * 2 + k)

    ins = [
        pltpu.make_async_copy(src, dst, sl.at[i])
        for i, (src, dst) in enumerate(
            (
                (ids_h, ids), (table_h, table), (bias_h, bias), (inw_h, inw),
                (byte_h, byte), (outt_h, outt), (tok_h, tok), (lab_h, lab),
            )
        )
    ]
    wc = [
        pltpu.make_async_copy(w_hbm.at[:, pl.ds(i * CW, CW)], w.at[:, pl.ds(i * CW, CW)], sw.at[i])
        for i in range(CH)
    ]
    for c in ins[:4] + wc + ins[4:]:
        c.start()

    bar = pltpu.get_barrier_semaphore()
    along_x = [(xz16[dx][0] + lo, grp) for dx in (2, 1, 3)]
    along_z = [(xz16[0][dz] + lo, grp) for dz in FAR[:7]]
    beside = [
        (xz16[0][0] + los[dl], his[dh] * 2 + ks[dk])
        for dl in range(2) for dh in range(2) for dk in range(2) if dl or dh or dk
    ]
    for to in along_z + along_x + beside:
        pl.semaphore_signal(bar, inc=1, device_id=to, device_id_type=MESH)

    m = iota((256, 256), 1)
    mhi, mx, mz, mp, mk = m % 2, (m // 2) % 4, (m // 8) % 8, (m // 64) % 2, m // 128
    owner = (mx * 16 + mz * 2 + (mp + mhi) % 2) * 4 + mhi * 2 + mk
    order = (iota((256, 256), 0) == owner).astype(BF)
    ins[0].wait()
    upper = ids[...] // 32
    halves = jnp.concatenate([upper, ids[...] - upper * 32], axis=0)
    halves = mm(jnp.broadcast_to(halves[:, None], (2, 8, 256)).reshape(16, 256).astype(F32), order, 1, 0)
    sorted_ids = (halves[0:1] * 32 + halves[8:9]).astype(jnp.int32)
    picks = (iota((1024, 256), 0) == sorted_ids).astype(F32).astype(BF)
    ins[1].wait()
    chosen = mm(picks, table[...], 0, 0).astype(BF)
    chosen_s[...] = chosen
    ins[2].wait()
    ins[3].wait()
    pre = mm(chosen, inw[...], 1, 0) + bias[...]
    hidden = jnp.maximum(pre, 0.0)
    hid[...] = hidden.astype(BF)

    qcols = [pl.ds(q * 1024, 1024) for q in range(2)]
    for q in range(2):
        for i in range(q * CH // 2, (q + 1) * CH // 2):
            cols = pl.ds(i * CW, CW)
            wc[i].wait()
            fs[:, :, :, :, cols] = jnp.dot(hid[...], w[:, cols], preferred_element_type=F32).reshape(
                2, 2, 8, 8, CW
            )
        if q == 0:
            pl.semaphore_wait(bar, 17)
            for to in along_x:
                pl.semaphore_signal(on_x, inc=1, device_id=to, device_id_type=MESH)
        for dz in FAR:
            remote(
                fs.at[1 - k, :, zs[dz], :, qcols[q]], fr.at[:, zs[dz], :, qcols[q]], r1s, r1r.at[q, dz], partner
            ).start()
    pl.semaphore_wait(on_x, 3)
    for to in along_z:
        pl.semaphore_signal(on_z, inc=1, device_id=to, device_id_type=MESH)
    is_a = x < 2
    stays = jnp.logical_not(is_a) & (hi == lo)
    parts = jnp.logical_not(is_a) & (hi != lo)
    moves = jnp.logical_not(stays)
    lo_b = jnp.where(is_a, 1 - lo, hi)
    diag = iota((256, 256), 0) == iota((256, 256), 1)
    ra = pl.ds(pl.multiple_of(k * 128 + x * 32, 32), 32)
    rb = pl.ds(pl.multiple_of(k * 256 + x * 64, 64), 64)
    cg2 = [
        remote(ga.at[ra], na.at[ra], gs.at[1], gr.at[1], n2),
        remote(gb.at[rb], nb.at[rb], gs.at[2], gr.at[2], n2),
        remote(gd, nd, gs.at[3], gr.at[7], n2),
    ]
    for i in range(16):
        q, dz = i // 8, FAR[i % 8]
        got = fr.at[:, zs[dz], :, qcols[q]]
        drain(got, r1r.at[q, dz])
        sb[:, zs[dz], :, qcols[q]] = (fs[k, :, zs[dz], :, qcols[q]] + fr[:, zs[dz], :, qcols[q]]).astype(BF)
        half, own = sb.at[1 - p, zs[dz], :, qcols[q]], sb.at[p, zs[dz], :, qcols[q]]
        to_0, to_1 = r2.at[0, zs[dz], :, qcols[q]], r2.at[1, zs[dz], :, qcols[q]]
        pl.when(parts)(remote(half, to_1, r2s, r2r.at[q, 1, dz], across).start)
        pl.when(jnp.logical_not(parts))(remote(half, to_0, r2s, r2r.at[q, 0, dz], n1).start)
        pl.when(moves)(remote(own, to_1, r2s, r2r.at[q, 1, dz], n2).start)
        if i == 7:
            ins[4].wait()
            ins[5].wait()
            gp[0:256, :] = mm(outt[...], byte[...], 1, 1)
            gp[256:512, :] = mm(outt[...], outt[...], 1, 1)
            gp[512:768, :] = mm(byte[...], byte[...], 1, 1)
            cg = remote(gp, gq, gs.at[0], gr.at[0], partner)
            cg.start()
    cg.wait_recv()
    gsum = gp[...] + gq[...]
    ga[...] = gsum[0:256]
    gd[...] = jnp.broadcast_to(jnp.sum(jnp.where(diag, gsum[512:768], 0.0), 0, keepdims=True), (8, 256))
    gb[...] = gsum[256:768].astype(BF)
    for c in cg2:
        c.start()

    for d8 in range(8):
        perm = (iota((1024, 128), 0) == 8 * iota((1024, 128), 1) + d8).astype(F32)
        bp[:, d8 * 128 : (d8 + 1) * 128] = mm(byte[...], perm, 1, 0).astype(BF)
    ins[6].wait()
    ins[7].wait()
    tok_hot = (iota((256, 256), 0) == tok[...]).astype(F32)
    lab_hot = (iota((256, 256), 0) == lab[...]).astype(F32)
    ct = mm(lab_hot, tok_hot, 1, 1)
    cnt = jnp.sum(ct, 0, keepdims=True)
    hidt[...] = jnp.transpose(hid[...].astype(F32)).astype(BF)
    co = [pltpu.make_async_copy(hidt, hidt_o, so.at[0])]
    co[0].start()

    slots = [jnp.where(is_a, (rem(z, 4) * 2 + lo_b) * 2 + q, 16 + 8 * (x - 2) + z) for q in range(2)]
    hi_d = jnp.where(is_a, x, hi)
    lo_d = rem(p + hi_d, 2)
    cores = [jnp.where(is_a, div(z, 4), q) for q in range(2)]
    to_c = [hi_d * 2 + cores[q] for q in range(2)]
    mine = [to_c[q] == grp for q in range(2)]
    n_self = mine[0].astype(jnp.int32) + mine[1].astype(jnp.int32)
    pl.semaphore_wait(on_z, 7)
    for i in range(16):
        q, dz = i // 8, FAR[i % 8]
        first = r2.at[0, zs[dz], :, qcols[q]]
        pl.when(moves)(pltpu.make_async_copy(first, first, r2r.at[q, 0, dz]).wait)
        drain(first, r2r.at[q, 1, dz])
        both = jnp.where(stays, sb[p, zs[dz], :, qcols[q]], r2[0, zs[dz], :, qcols[q]]).astype(F32)
        both = both + r2[1, zs[dz], :, qcols[q]].astype(F32)
        for j in range(8):
            ft[q, pl.ds(j, 8, stride=8), :] = both[:, j * 128 : (j + 1) * 128]
        f[q, zs[dz]] = ft[q, 0:64].astype(BF).reshape(4, 2, 8, 128)
        for dx in FAR_X:
            c = remote(
                f.at[q, zs[dz], xs[dx]], rx.at[k, :, slots[q]], r3s, r3r, (xz16[dx][dz] + lo_d, to_c[q])
            )
            if dz or dx:
                c.start()
            else:
                pl.when(jnp.logical_not(mine[q]))(c.start)
    for c in cg2:
        c.wait_recv()
    for dx in (2, 1, 3):
        to = (xz16[dx][0] + lo, grp)
        remote(na.at[ra], na.at[ra], gs.at[1], gr.at[3], to).start()
        remote(nb.at[rb], nb.at[rb], gs.at[2], gr.at[4], to).start()
    for q in range(2):

        @pl.when(mine[q])
        def _(q=q):
            rx[k, :, slots[q]] = f[q, z, x]

    def wait_all(sem):
        for n in range(3):

            @pl.when(n_self == n)
            def _(n=n):
                piece = like.at[pl.ds(0, 64 - n)]
                pltpu.make_async_copy(piece, piece, sem).wait()

    wait_all(r3r)

    for c in range(4):
        at = jnp.transpose(rx[c // 2, c % 2, 0:16].astype(F32).reshape(128, 128))
        for d8 in range(8):
            la[c * 16 : (c + 1) * 16, d8 * 128 : (d8 + 1) * 128] = at[d8 * 16 : (d8 + 1) * 16].astype(BF)
        xf[c * 128 : (c + 1) * 128, :] = rx[c // 2, c % 2, 16:32].astype(F32).reshape(128, 128)
    for j in range(8):
        lb[:, j * 128 : (j + 1) * 128] = xf[pl.ds(j, 64, stride=8), :].astype(BF)
    pt = mm(la[...], bp[...], 1, 1)
    qt = mm(lb[...], outt[...], 1, 1)
    rt = mm(lb[...], byte[...], 1, 1)
    ss = mm(lb[...], lb[...], 1, 1)
    for c in range(4):
        rows = slice(c * 16, (c + 1) * 16)
        ms[c, 0:16, :] = pt[rows].astype(BF)
        ms[c, 16:32, :] = qt[rows].astype(BF)
        ms[c, 32:48, :] = rt[rows].astype(BF)
        ms[c, 48:64, :] = jnp.zeros((16, 256), BF)
        ms[c, 48:64, 0:16] = ss[rows, c * 16 : (c + 1) * 16].astype(BF)
    me = k * 2 + hi
    members = [
        (ks[o // 2] * 2 + his[o % 2], (xz16[0][0] + los[o % 2], his[o % 2] * 2 + ks[o // 2]))
        for o in range(4)
    ]
    for o in range(1, 4):
        c_, to = members[o]
        remote(ms.at[c_], er.at[o], e1s, e1r, to).start()
    drain(na.at[pl.ds(0, 96)], gr.at[3])
    drain(nb.at[pl.ds(0, 192)], gr.at[4])
    ha = pl.ds(pl.multiple_of(k * 128, 128), 128)
    hbb = pl.ds(pl.multiple_of(k * 256, 256), 256)
    cg3 = [
        remote(na.at[ha], na.at[ha], gs.at[1], gr.at[5], partner),
        remote(nb.at[hbb], nb.at[hbb], gs.at[2], gr.at[6], partner),
    ]
    for c in cg3:
        c.start()
    for c in cg3:
        c.wait_recv()
    obt = ga[...] + na[...]
    bb = gd[0:1, :] + nd[0:1, :]
    grams = gb[...].astype(F32) + nb[...].astype(F32)
    oo, bbm = grams[0:256].astype(BF), grams[256:512].astype(BF)
    scale = lax.rsqrt(bb * (1 / 4096) + EPS)
    own = ms[me].astype(F32)
    drain(er.at[pl.ds(1, 3)], e1r)
    for o in range(1, 4):
        own = own + er[o].astype(F32)
    u, xx, yy, zz, loss = two_steps(
        own[0:16], own[16:32], own[32:48], own[48:64, 0:16], obt, oo, bbm, bb, scale, ct, cnt
    )
    loss_o[0] = loss * (1 / 256)
    cm[0:16, :] = u.astype(BF)
    cm[16:32, :] = xx.astype(BF)
    cm[32:48, :] = yy.astype(BF)
    cm[48:64, :] = jnp.zeros((16, 256), BF)
    cm[48:64, 0:16] = zz.astype(BF)
    for o in range(1, 4):
        remote(cm, cr.at[me], e2s, e2r, members[o][1]).start()
    cr[me] = cm[...]
    drain(er.at[pl.ds(1, 3)], e2r)

    allc = cr[...]
    us = allc[:, 0:16].reshape(64, 256)
    xc = allc[:, 16:32].reshape(64, 256)
    yc = allc[:, 32:48].reshape(64, 256)
    dat = mm(us, bp[...], 1, 0)
    for c in range(4):
        for d8 in range(8):
            ta[d8 * 16 : (d8 + 1) * 16, :] = dat[c * 16 : (c + 1) * 16, d8 * 128 : (d8 + 1) * 128]
        tx[c // 2, c % 2, 0:16] = jnp.transpose(ta[...]).astype(BF).reshape(16, 8, 128)
    dbs = mm(xc, outt[...], 1, 0) + mm(yc, byte[...], 1, 0)
    zdb = [mm(cr[c, 48:64, 0:16], lb[c * 16 : (c + 1) * 16, :], 1, 0) for c in range(4)]
    dbs = dbs + jnp.concatenate(zdb, axis=0)
    for j in range(8):
        xf[pl.ds(j, 64, stride=8), :] = dbs[:, j * 128 : (j + 1) * 128]
    for c in range(4):
        tx[c // 2, c % 2, 16:32] = xf[c * 128 : (c + 1) * 128, :].astype(BF).reshape(16, 8, 128)

    def give(slot, k_, q_, to, back, near):
        c = remote(tx.at[k_, :, slot], g_in.at[q_, z, x], r4s, r4r.at[back], to)
        if near:
            pl.when(jnp.logical_not((to[0] == head) & (to[1] == grp)))(c.start)
        else:
            c.start()

    his_a = [rem(p + 1 - par, 2) for par in range(2)]
    for dz in NEAR:
        for xh in range(2):
            for dk in range(2):
                slot = 16 + xh * 8 + zs[dz]
                to = (32 + xh * 16 + zs[dz] * 2 + lo, hi * 2 + ks[dk])
                give(slot, ks[dk], k, to, (8 - dz) % 8, dz == 0)

        @pl.when(div(zs[dz], 4) == k)
        def _(dz=dz):
            for par in range(2):
                for q in range(2):
                    for dk in range(2):
                        slot = (rem(zs[dz], 4) * 2 + par) * 2 + q
                        to = (hi * 16 + zs[dz] * 2 + 1 - par, his_a[par] * 2 + ks[dk])
                        give(slot, ks[dk], q, to, (8 - dz) % 8, dz == 0)

    for q in range(2):

        @pl.when(mine[q])
        def _(q=q):
            g_in[q, z, x] = tx[k, :, slots[q]]

    for dz in NEAR:
        if dz:
            drain(like.at[pl.ds(0, 8)], r4r.at[dz])
        else:
            for n in range(3):

                @pl.when(n_self == n)
                def _(n=n):
                    drain(like.at[pl.ds(0, 8 - n)], r4r.at[0])

        part, spot = g_in.at[:, zs[dz]], d_in.at[k, p, :, zs[dz]]
        pl.when(moves)(remote(part, spot, r5s, r5r.at[0, dz], n1).start)
        pl.when(moves)(remote(part, spot, r5s, r5r.at[1, dz], n2).start)
        pl.when(stays)(remote(part, spot, r5s, r5r.at[0, dz], across).start)

    @pl.when(stays)
    def _():
        d_in[k, p] = g_in[...]

    for dz in NEAR:
        region = d_in.at[k, :, :, zs[dz]]
        one = d_in.at[k, 0, :, zs[dz]]
        drain(one, r5r.at[0, dz])
        pl.when(moves)(pltpu.make_async_copy(one, one, r5r.at[1, dz]).wait)
        remote(region, region, r6s, r6r, partner).start()
    turn = [rem(zn - z + 14, 8) * 16 for zn in range(8)]
    peers = [(xs[o // 2], los[o % 2], (xz16[o // 2][0] + los[o % 2], grp)) for o in range(8)]
    for half in range(2):
        if half:
            drain(d_in.at[1 - k], r6r)
        row = pl.multiple_of(ks[half] * 128, 128)
        for p_ in range(2):
            xd = d_in[ks[half], p_].astype(F32).reshape(1024, 128)
            ft[0] = xd[0:512]
            ft[1] = xd[512:1024]
            for j in range(16):
                dn[pl.ds(row + p_ * 64, 64), j * 128 : (j + 1) * 128] = ft[
                    j // 8, pl.ds(j % 8, 64, stride=8), :
                ].astype(BF)
        for i in range(4):
            part = mm(w[i * 256 : (i + 1) * 256, :], dn[pl.ds(row, 128), :], 1, 1).astype(BF)
            for l_ in range(2):
                for zn in range(8):
                    at = l_ * 128 + zn * 16
                    hb[half, i, l_, pl.ds(pl.multiple_of(turn[zn], 16), 16), :] = part[at : at + 16]
        for h in range(2):
            rows = pl.ds(h * 64, 64)
            for o in (4, 5, 2, 3, 6, 7, 1):
                x_, lo_, to = peers[o]
                src = hb.at[half, x_, lo_, rows]
                remote(src, a1.at[half, o, rows], p1s, p1r.at[half, h], to).start()
    co.append(pltpu.make_async_copy(dn, dn_o, so.at[1]))
    co[1].start()
    for h in range(2):
        rows = pl.ds(h * 64, 64)
        for half in range(2):
            acc = hb[half, x, lo, rows, :].astype(F32)
            drain(a1.at[half, pl.ds(1, 7), rows], p1r.at[half, h])
            for o in range(1, 8):
                acc = acc + a1[half, o, rows, :].astype(F32)
            a1s[rows, pl.ds(pl.multiple_of(ks[half] * 128, 128), 128)] = acc.astype(BF)
        for t in ((2, 1, 3, 0), (4, 7, 5, 6))[h]:
            dz = (t + 2) % 8
            if dz:
                remote(a1s.at[pl.ds(t * 16, 16)], a2.at[dz], p2s, p2r, (xz16[0][dz] + lo, grp)).start()
    total = a1s[96:112, :].astype(F32)
    drain(a2.at[pl.ds(1, 7)], p2r)
    for dz in range(1, 8):
        total = total + a2[dz].astype(F32)
    base = pl.multiple_of(x * 256 + lo * 128, 128)
    row0 = pl.multiple_of(base + z * 16, 16)
    total = jnp.where(hidt[pl.ds(row0, 16), :].astype(F32) > 0, total, 0.0)
    big = total.astype(BF)
    small = (total - big.astype(F32)).astype(BF)
    piece = mm(big, chosen_s[...], 1, 0) + mm(small, chosen_s[...], 1, 0)
    ag[pl.ds(row0, 16), :] = piece.astype(BF)
    cd = {}
    own_rows = ag.at[pl.ds(row0, 16)]
    for dz in FAR[:7]:
        cd[dz] = remote(own_rows, own_rows, p3s, p3r.at[dz], (xz16[0][dz] + lo, grp))
        cd[dz].start()
    for dz in (0, 1, 7, 2, 6, 3, 5, 4):
        if dz:
            cd[dz].wait_recv()
        rows = ag.at[pl.ds(pl.multiple_of(base + zs[(8 - dz) % 8] * 16, 16), 16)]
        for o in (4, 5, 2, 3, 6, 7, 1):
            remote(rows, rows, p4s, p4r, peers[o][2]).start()
    drain(a1.at[:, pl.ds(1, 7)], p4r)
    co.append(pltpu.make_async_copy(ag, ag_o, so.at[2]))
    co[2].start()

    drain(fr, r1s)
    pl.when(stays)(pltpu.make_async_copy(r2.at[0], r2.at[0], r2s).wait)
    pl.when(moves)(pltpu.make_async_copy(r2, r2, r2s).wait)
    drain(gq, gs.at[0])
    drain(na, gs.at[1])
    drain(nb, gs.at[2])
    drain(nd, gs.at[3])
    drain(er.at[pl.ds(1, 3)], e1s)
    drain(er.at[pl.ds(1, 3)], e2s)
    pl.when(stays)(pltpu.make_async_copy(g_in, g_in, r5s).wait)
    pl.when(moves)(pltpu.make_async_copy(d_in.at[0], d_in.at[0], r5s).wait)
    drain(d_in.at[0], r6s)
    drain(a1.at[:, pl.ds(1, 7)], p1s)
    drain(a2.at[pl.ds(1, 7)], p2s)
    drain(a2.at[pl.ds(1, 7)], p3s)
    drain(a1.at[:, pl.ds(1, 7)], p4s)
    wait_all(r3s)
    wait_all(r4s)
    for c in co:
        c.wait()


def local(client_ids, client_table, in_weight, in_bias, head_weight, tokens, labels, byte_table, out_table):
    hbm = pl.BlockSpec(memory_space=pl.ANY)
    dma = pltpu.SemaphoreType.DMA
    V = pltpu.VMEM
    S = jax.ShapeDtypeStruct
    ag, dn, hidt, losses = pl.pallas_call(
        kernel,
        out_shape=(S((1024, 256), BF), S((256, 2048), BF), S((1024, 256), BF), S((1,), F32)),
        in_specs=[hbm] * 9,
        out_specs=(hbm, hbm, hbm, pl.BlockSpec(memory_space=pltpu.SMEM)),
        scratch_shapes=[
            V((1, 256), jnp.int32),
            V((1, 1024), F32),
            V((1, 256), jnp.int32),
            V((1, 256), jnp.int32),
            V((1024, 256), BF),
            V((256, 1024), BF),
            V((256, 1024), BF),
            V((256, 1024), BF),
            V((1024, 2048), BF),
            V((256, 1024), BF),
            V((2, 2, 8, 8, 2048), F32),
            V((2, 8, 8, 2048), F32),
            V((2, 8, 8, 2048), BF),
            V((2, 8, 8, 2048), BF),
            V((2, 512, 128), F32),
            V((2, 8, 4, 2, 8, 128), BF),
            V((2, 2, 32, 8, 128), BF),
            V((64, 1024), BF),
            V((64, 1024), BF),
            V((512, 128), F32),
            V((256, 1024), BF),
            V((768, 256), F32),
            V((768, 256), F32),
            V((256, 256), F32),
            V((512, 256), BF),
            V((256, 256), F32),
            V((512, 256), BF),
            V((8, 256), F32),
            V((8, 256), F32),
            V((4, 64, 256), BF),
            V((4, 64, 256), BF),
            V((64, 256), BF),
            V((4, 64, 256), BF),
            V((128, 128), F32),
            V((2, 2, 32, 8, 128), BF),
            V((2, 8, 4, 2, 8, 128), BF),
            V((2, 2, 2, 8, 4, 2, 8, 128), BF),
            V((256, 2048), BF),
            V((2, 4, 2, 128, 128), BF),
            V((2, 8, 128, 128), BF),
            V((128, 256), BF),
            V((8, 16, 256), BF),
            V((1024, 256), BF),
            V((1024, 256), BF),
            V((256, 256), BF),
            V((64, 2, 8, 128), BF),
            pltpu.SemaphoreType.REGULAR, pltpu.SemaphoreType.REGULAR,
            dma((8,)), dma((CH,)), dma((3,)),
            dma(()), dma((2, 8)),
            dma(()), dma((2, 2, 8)),
            dma((4,)), dma((8,)),
            dma(()), dma(()),
            dma(()), dma(()), dma(()), dma(()),
            dma(()), dma((8,)),
            dma(()), dma((2, 8)), dma(()), dma(()),
            dma(()), dma((2, 2)), dma(()), dma(()),
            dma(()), dma((8,)), dma(()), dma(()),
        ],
        compiler_params=pltpu.CompilerParams(
            collective_id=0, has_side_effects=True, vmem_limit_bytes=60 * 1024 * 1024
        ),
        name="round",
    )(
        client_ids.reshape(1, 256), client_table, in_weight, in_bias.reshape(1, 1024), head_weight,
        tokens, labels, byte_table, out_table,
    )
    head_grad, in_grad = pl.pallas_call(
        tail_kernel,
        out_shape=(S((1024, 2048), BF), S((256, 1024), F32)),
        in_specs=[hbm] * 3,
        out_specs=(hbm, hbm),
        scratch_shapes=[
            V((1024, 256), BF), V((256, 2048), BF), V((1024, 256), BF),
            V((1024, 2048), BF), V((256, 1024), F32),
            dma((6,)), dma((5,)),
        ],
        compiler_params=pltpu.CompilerParams(vmem_limit_bytes=60 * 1024 * 1024),
        name="tail",
    )(hidt, dn, ag)
    return head_grad, in_grad, losses


def solution(mesh):
    placed = (
        P(),
        P(),
        P(None, "client"),
        P("client"),
        P("client", "head"),
        P(("head", "client"), None),
        P(("head", "client"), None),
        P(None, "client"),
        P(None, "client"),
    )
    return jax.shard_map(
        local,
        mesh=mesh,
        in_specs=placed,
        out_specs=(P("client", "head"), P(None, "client"), P(("head", "client"))),
        check_vma=False,
    )
```

```python
import jax
import jax.numpy as jnp
from jax import lax
from jax.experimental import pallas as pl
from jax.experimental.pallas import tpu as pltpu
from jax.sharding import PartitionSpec as P

EPS = 1e-6
ETA = 0.1
F32 = jnp.float32
BF = jnp.bfloat16
MESH = pl.DeviceIdType.MESH
CH = 4
CW = 2048 // CH


def mm(a, b, ca, cb):
    return lax.dot_general(
        a.astype(BF), b.astype(BF), (((ca,), (cb,)), ((), ())), preferred_element_type=F32
    )


def iota(shape, dim):
    return lax.broadcasted_iota(jnp.int32, shape, dim)


def gradients(pt, qt, rt, s_mat, obt, bb, scale, ct, cnt):
    tt = pt * (scale * (1 / 256))
    st = mm(s_mat, tt, 1, 0)
    msq = (bb + jnp.sum(tt * (2 * rt + st), 0, keepdims=True)) * (1 / 4096)
    q = lax.rsqrt(msq + EPS)
    mt = obt + mm(qt, tt, 0, 0)
    lg = mt * (q * (1 / 16))
    top = jnp.max(lg, 0, keepdims=True)
    ex = jnp.exp(lg - top)
    total = jnp.sum(ex, 0, keepdims=True)
    gt = (ex * (cnt / total) - ct) * (1 / 16)
    along = jnp.sum(gt * mt, 0, keepdims=True)
    e = q * q * q * along * (1 / 4096)
    ht = gt * q
    dt = mm(qt, ht, 1, 0) - e * (rt + st)
    ut = dt * (scale * (1 / 256))
    xt = mm(tt, ht, 1, 1)
    yt = tt * e
    z = mm(yt, tt, 1, 1)
    loss = jnp.sum(cnt * (top + jnp.log(total)) - jnp.sum(ct * lg, 0, keepdims=True))
    return ut, xt, yt, z, loss


def two_steps(pt, qt, rt, s_mat, obt, oo, bbm, bb, scale, ct, cnt):
    u1, x1, y1, z1, loss = gradients(pt, qt, rt, s_mat, obt, bb, scale, ct, cnt)
    vo = -ETA * mm(x1, oo, 1, 0) + ETA * mm(y1, obt, 1, 1)
    vb = -ETA * mm(x1, obt, 1, 0) + ETA * mm(y1, bbm, 1, 0)
    z1 = ETA * z1
    p2 = pt - ETA * mm(u1, bbm, 1, 0)
    q2 = qt + mm(z1, qt, 1, 0) + vo
    r2 = rt + mm(z1, rt, 1, 0) + vb
    h = -ETA * mm(qt, x1, 1, 1) + ETA * mm(rt, y1, 1, 1)
    ht = -ETA * mm(x1, qt, 1, 1) + ETA * mm(y1, rt, 1, 1)
    vv = -ETA * mm(x1, vo, 1, 1) + ETA * mm(y1, vb, 1, 1)
    zs = mm(z1, s_mat, 1, 0)
    s2 = s_mat + zs + mm(s_mat, z1, 1, 1) + mm(zs, z1, 1, 1)
    s2 = s2 + h + mm(z1, h, 1, 0) + ht + mm(ht, z1, 1, 1) + vv
    u2, x2, y2, z2, _ = gradients(p2, q2, r2, s2, obt, bb, scale, ct, cnt)
    z2 = ETA * z2
    u = -ETA * (u1 + u2)
    x = -ETA * (x1 + mm(z2, x1, 1, 0) + x2)
    y = ETA * (y1 + mm(z2, y1, 1, 0) + y2)
    z = z1 + z2 + mm(z2, z1, 1, 0)
    return u, x, y, z, loss

def tail_kernel(hidt, dn, ag, hg_o, ing_o, hv, dv, av, gv, iv, sem, osem):
    cols = [pl.ds(0, 256), pl.ds(256, 256)] + [pl.ds(i * 512, 512) for i in range(1, 4)]
    loads = [pltpu.make_async_copy(hidt, hv, sem.at[0])]
    loads += [pltpu.make_async_copy(dn.at[:, cols[i]], dv.at[:, cols[i]], sem.at[1 + i]) for i in range(5)]
    loads.append(pltpu.make_async_copy(ag, av, sem.at[6]))
    for c in loads:
        c.start()
    loads[0].wait()
    outs = []
    for i in range(5):
        loads[1 + i].wait()
        if i == 1:
            loads[6].wait()
            iv[...] = jnp.transpose(av[...].astype(F32))
        gv[:, cols[i]] = jnp.dot(hv[...], dv[:, cols[i]], preferred_element_type=F32).astype(BF)
        outs.append(pltpu.make_async_copy(gv.at[:, cols[i]], hg_o.at[:, cols[i]], osem.at[i]))
        outs[-1].start()
        if i == 1:
            outs.append(pltpu.make_async_copy(iv, ing_o, osem.at[5]))
            outs[-1].start()
    for c in outs:
        c.wait()


FAR = (4, 3, 5, 2, 6, 1, 7, 0)
FAR_X = (2, 1, 3, 0)
NEAR = (0, 1, 7, 2, 6, 3, 5, 4)


def kernel(
    ids_h, table_h, inw_h, bias_h, w_hbm, tok_h, lab_h, byte_h, outt_h,
    ag_o, dn_o, hidt_o, loss_o,
    ids, bias, tok, lab, table, inw, byte, outt,
    w, hid, fs, fr, sb, r2, ft, f, rx, la, lb, xf, bp, gp, gq, ga, gb, na, nb, gd, nd, ms, er, cm, cr, ta, tx, g_in,
    d_in, dn, hb, a1, a1s, a2, ag, hidt, chosen_s, like,
    on_x, on_z, sl, sw, so, r1s, r1r, r2s, r2r, gs, gr, r3s, r3r, e1s, e1r, e2s, e2r, r4s, r4r, r5s, r5r, r6s, r6r,
    p1s, p1r, p2s, p2r, p3s, p3r, p4s, p4r,
):
    rem, div = lax.rem, lax.div
    head = lax.axis_index("head")
    grp = lax.axis_index("client")
    x, z, lo = div(head, 16), rem(div(head, 2), 8), rem(head, 2)
    hi, k = div(grp, 2), rem(grp, 2)
    p = rem(hi + lo, 2)
    xs = [rem(x + d, 4) for d in range(4)]
    zs = [rem(z + d, 8) for d in range(8)]
    ks = [k, 1 - k]
    his = [hi, 1 - hi]
    los = [lo, 1 - lo]
    xz16 = [[xs[dx] * 16 + zs[dz] * 2 for dz in range(8)] for dx in range(4)]

    def remote(src, dst, ss, rs, to):
        return pltpu.make_async_remote_copy(
            src_ref=src, dst_ref=dst, send_sem=ss, recv_sem=rs, device_id=to, device_id_type=MESH
        )

    def drain(like_ref, sem):
        pltpu.make_async_copy(like_ref, like_ref, sem).wait()

    partner = (head, hi * 2 + 1 - k)
    n1 = (xz16[0][0] + 1 - lo, grp)
    n2 = (xz16[0][0] + 1 - lo, (1 - hi) * 2 + k)
    across = (head, (1 - hi) * 2 + k)

    ins = [
        pltpu.make_async_copy(src, dst, sl.at[i])
        for i, (src, dst) in enumerate(
            (
                (ids_h, ids), (table_h, table), (bias_h, bias), (inw_h, inw),
                (byte_h, byte), (outt_h, outt), (tok_h, tok), (lab_h, lab),
            )
        )
    ]
    wc = [
        pltpu.make_async_copy(w_hbm.at[:, pl.ds(i * CW, CW)], w.at[:, pl.ds(i * CW, CW)], sw.at[i])
        for i in range(CH)
    ]
    for c in ins[:4] + wc + ins[4:]:
        c.start()

    bar = pltpu.get_barrier_semaphore()
    along_x = [(xz16[dx][0] + lo, grp) for dx in (2, 1, 3)]
    along_z = [(xz16[0][dz] + lo, grp) for dz in FAR[:7]]
    beside = [
        (xz16[0][0] + los[dl], his[dh] * 2 + ks[dk])
        for dl in range(2) for dh in range(2) for dk in range(2) if dl or dh or dk
    ]
    for to in along_z + along_x + beside:
        pl.semaphore_signal(bar, inc=1, device_id=to, device_id_type=MESH)

    m = iota((256, 256), 1)
    mhi, mx, mz, mp, mk = m % 2, (m // 2) % 4, (m // 8) % 8, (m // 64) % 2, m // 128
    owner = (mx * 16 + mz * 2 + (mp + mhi) % 2) * 4 + mhi * 2 + mk
    order = (iota((256, 256), 0) == owner).astype(BF)
    ins[0].wait()
    upper = ids[...] // 32
    halves = jnp.concatenate([upper, ids[...] - upper * 32], axis=0)
    halves = mm(jnp.broadcast_to(halves[:, None], (2, 8, 256)).reshape(16, 256).astype(F32), order, 1, 0)
    sorted_ids = (halves[0:1] * 32 + halves[8:9]).astype(jnp.int32)
    picks = (iota((1024, 256), 0) == sorted_ids).astype(F32).astype(BF)
    ins[1].wait()
    chosen = mm(picks, table[...], 0, 0).astype(BF)
    chosen_s[...] = chosen
    ins[2].wait()
    ins[3].wait()
    pre = mm(chosen, inw[...], 1, 0) + bias[...]
    hidden = jnp.maximum(pre, 0.0)
    hid[...] = hidden.astype(BF)

    qcols = [pl.ds(q * 1024, 1024) for q in range(2)]
    for q in range(2):
        for i in range(q * CH // 2, (q + 1) * CH // 2):
            cols = pl.ds(i * CW, CW)
            wc[i].wait()
            fs[:, :, :, :, cols] = jnp.dot(hid[...], w[:, cols], preferred_element_type=F32).reshape(
                2, 2, 8, 8, CW
            )
        if q == 0:
            pl.semaphore_wait(bar, 17)
            for to in along_x:
                pl.semaphore_signal(on_x, inc=1, device_id=to, device_id_type=MESH)
        for dz in FAR:
            remote(
                fs.at[1 - k, :, zs[dz], :, qcols[q]], fr.at[:, zs[dz], :, qcols[q]], r1s, r1r.at[q, dz], partner
            ).start()
    pl.semaphore_wait(on_x, 3)
    for to in along_z:
        pl.semaphore_signal(on_z, inc=1, device_id=to, device_id_type=MESH)
    is_a = x < 2
    stays = jnp.logical_not(is_a) & (hi == lo)
    parts = jnp.logical_not(is_a) & (hi != lo)
    moves = jnp.logical_not(stays)
    lo_b = jnp.where(is_a, 1 - lo, hi)
    diag = iota((256, 256), 0) == iota((256, 256), 1)
    ra = pl.ds(pl.multiple_of(k * 128 + x * 32, 32), 32)
    rb = pl.ds(pl.multiple_of(k * 256 + x * 64, 64), 64)
    cg2 = [
        remote(ga.at[ra], na.at[ra], gs.at[1], gr.at[1], n2),
        remote(gb.at[rb], nb.at[rb], gs.at[2], gr.at[2], n2),
        remote(gd, nd, gs.at[3], gr.at[7], n2),
    ]
    for i in range(16):
        q, dz = i // 8, FAR[i % 8]
        got = fr.at[:, zs[dz], :, qcols[q]]
        drain(got, r1r.at[q, dz])
        sb[:, zs[dz], :, qcols[q]] = (fs[k, :, zs[dz], :, qcols[q]] + fr[:, zs[dz], :, qcols[q]]).astype(BF)
        half, own = sb.at[1 - p, zs[dz], :, qcols[q]], sb.at[p, zs[dz], :, qcols[q]]
        to_0, to_1 = r2.at[0, zs[dz], :, qcols[q]], r2.at[1, zs[dz], :, qcols[q]]
        pl.when(parts)(remote(half, to_1, r2s, r2r.at[q, 1, dz], across).start)
        pl.when(jnp.logical_not(parts))(remote(half, to_0, r2s, r2r.at[q, 0, dz], n1).start)
        pl.when(moves)(remote(own, to_1, r2s, r2r.at[q, 1, dz], n2).start)
        if i == 7:
            ins[4].wait()
            ins[5].wait()
            gp[0:256, :] = mm(outt[...], byte[...], 1, 1)
            gp[256:512, :] = mm(outt[...], outt[...], 1, 1)
            gp[512:768, :] = mm(byte[...], byte[...], 1, 1)
            cg = remote(gp, gq, gs.at[0], gr.at[0], partner)
            cg.start()
    cg.wait_recv()
    gsum = gp[...] + gq[...]
    ga[...] = gsum[0:256]
    gd[...] = jnp.broadcast_to(jnp.sum(jnp.where(diag, gsum[512:768], 0.0), 0, keepdims=True), (8, 256))
    gb[...] = gsum[256:768].astype(BF)
    for c in cg2:
        c.start()

    for d8 in range(8):
        perm = (iota((1024, 128), 0) == 8 * iota((1024, 128), 1) + d8).astype(F32)
        bp[:, d8 * 128 : (d8 + 1) * 128] = mm(byte[...], perm, 1, 0).astype(BF)
    ins[6].wait()
    ins[7].wait()
    tok_hot = (iota((256, 256), 0) == tok[...]).astype(F32)
    lab_hot = (iota((256, 256), 0) == lab[...]).astype(F32)
    ct = mm(lab_hot, tok_hot, 1, 1)
    cnt = jnp.sum(ct, 0, keepdims=True)
    hidt[...] = jnp.transpose(hid[...].astype(F32)).astype(BF)
    co = [pltpu.make_async_copy(hidt, hidt_o, so.at[0])]
    co[0].start()

    slots = [jnp.where(is_a, (rem(z, 4) * 2 + lo_b) * 2 + q, 16 + 8 * (x - 2) + z) for q in range(2)]
    hi_d = jnp.where(is_a, x, hi)
    lo_d = rem(p + hi_d, 2)
    cores = [jnp.where(is_a, div(z, 4), q) for q in range(2)]
    to_c = [hi_d * 2 + cores[q] for q in range(2)]
    mine = [to_c[q] == grp for q in range(2)]
    n_self = mine[0].astype(jnp.int32) + mine[1].astype(jnp.int32)
    pl.semaphore_wait(on_z, 7)
    for i in range(16):
        q, dz = i // 8, FAR[i % 8]
        first = r2.at[0, zs[dz], :, qcols[q]]
        pl.when(moves)(pltpu.make_async_copy(first, first, r2r.at[q, 0, dz]).wait)
        drain(first, r2r.at[q, 1, dz])
        both = jnp.where(stays, sb[p, zs[dz], :, qcols[q]], r2[0, zs[dz], :, qcols[q]]).astype(F32)
        both = both + r2[1, zs[dz], :, qcols[q]].astype(F32)
        for j in range(8):
            ft[q, pl.ds(j, 8, stride=8), :] = both[:, j * 128 : (j + 1) * 128]
        f[q, zs[dz]] = ft[q, 0:64].astype(BF).reshape(4, 2, 8, 128)
        for dx in FAR_X:
            c = remote(
                f.at[q, zs[dz], xs[dx]], rx.at[k, :, slots[q]], r3s, r3r, (xz16[dx][dz] + lo_d, to_c[q])
            )
            if dz or dx:
                c.start()
            else:
                pl.when(jnp.logical_not(mine[q]))(c.start)
    for c in cg2:
        c.wait_recv()
    for dx in (2, 1, 3):
        to = (xz16[dx][0] + lo, grp)
        remote(na.at[ra], na.at[ra], gs.at[1], gr.at[3], to).start()
        remote(nb.at[rb], nb.at[rb], gs.at[2], gr.at[4], to).start()
    for q in range(2):

        @pl.when(mine[q])
        def _(q=q):
            rx[k, :, slots[q]] = f[q, z, x]

    def wait_all(sem):
        for n in range(3):

            @pl.when(n_self == n)
            def _(n=n):
                piece = like.at[pl.ds(0, 64 - n)]
                pltpu.make_async_copy(piece, piece, sem).wait()

    wait_all(r3r)

    for c in range(4):
        at = jnp.transpose(rx[c // 2, c % 2, 0:16].astype(F32).reshape(128, 128))
        for d8 in range(8):
            la[c * 16 : (c + 1) * 16, d8 * 128 : (d8 + 1) * 128] = at[d8 * 16 : (d8 + 1) * 16].astype(BF)
        xf[c * 128 : (c + 1) * 128, :] = rx[c // 2, c % 2, 16:32].astype(F32).reshape(128, 128)
    for j in range(8):
        lb[:, j * 128 : (j + 1) * 128] = xf[pl.ds(j, 64, stride=8), :].astype(BF)
    pt = mm(la[...], bp[...], 1, 1)
    qt = mm(lb[...], outt[...], 1, 1)
    rt = mm(lb[...], byte[...], 1, 1)
    ss = mm(lb[...], lb[...], 1, 1)
    for c in range(4):
        rows = slice(c * 16, (c + 1) * 16)
        ms[c, 0:16, :] = pt[rows].astype(BF)
        ms[c, 16:32, :] = qt[rows].astype(BF)
        ms[c, 32:48, :] = rt[rows].astype(BF)
        ms[c, 48:64, :] = jnp.zeros((16, 256), BF)
        ms[c, 48:64, 0:16] = ss[rows, c * 16 : (c + 1) * 16].astype(BF)
    me = k * 2 + hi
    members = [
        (ks[o // 2] * 2 + his[o % 2], (xz16[0][0] + los[o % 2], his[o % 2] * 2 + ks[o // 2]))
        for o in range(4)
    ]
    for o in (1, 3, 2):
        c_, to = members[o]
        remote(ms.at[c_], er.at[o], e1s, e1r, to).start()
    drain(na.at[pl.ds(0, 96)], gr.at[3])
    drain(nb.at[pl.ds(0, 192)], gr.at[4])
    ha = pl.ds(pl.multiple_of(k * 128, 128), 128)
    hbb = pl.ds(pl.multiple_of(k * 256, 256), 256)
    cg3 = [
        remote(na.at[ha], na.at[ha], gs.at[1], gr.at[5], partner),
        remote(nb.at[hbb], nb.at[hbb], gs.at[2], gr.at[6], partner),
    ]
    for c in cg3:
        c.start()
    for c in cg3:
        c.wait_recv()
    obt = ga[...] + na[...]
    bb = gd[0:1, :] + nd[0:1, :]
    grams = gb[...].astype(F32) + nb[...].astype(F32)
    oo, bbm = grams[0:256].astype(BF), grams[256:512].astype(BF)
    scale = lax.rsqrt(bb * (1 / 4096) + EPS)
    own = ms[me].astype(F32)
    drain(er.at[pl.ds(1, 3)], e1r)
    for o in range(1, 4):
        own = own + er[o].astype(F32)
    u, xx, yy, zz, loss = two_steps(
        own[0:16], own[16:32], own[32:48], own[48:64, 0:16], obt, oo, bbm, bb, scale, ct, cnt
    )
    loss_o[0] = loss * (1 / 256)
    cm[0:16, :] = u.astype(BF)
    cm[16:32, :] = xx.astype(BF)
    cm[32:48, :] = yy.astype(BF)
    cm[48:64, :] = jnp.zeros((16, 256), BF)
    cm[48:64, 0:16] = zz.astype(BF)
    for o in (1, 3, 2):
        remote(cm, cr.at[me], e2s, e2r, members[o][1]).start()
    cr[me] = cm[...]
    drain(er.at[pl.ds(1, 3)], e2r)

    allc = cr[...]
    us = allc[:, 0:16].reshape(64, 256)
    xc = allc[:, 16:32].reshape(64, 256)
    yc = allc[:, 32:48].reshape(64, 256)
    dat = mm(us, bp[...], 1, 0)
    for c in range(4):
        for d8 in range(8):
            ta[d8 * 16 : (d8 + 1) * 16, :] = dat[c * 16 : (c + 1) * 16, d8 * 128 : (d8 + 1) * 128]
        tx[c // 2, c % 2, 0:16] = jnp.transpose(ta[...]).astype(BF).reshape(16, 8, 128)
    dbs = mm(xc, outt[...], 1, 0) + mm(yc, byte[...], 1, 0)
    zdb = [mm(cr[c, 48:64, 0:16], lb[c * 16 : (c + 1) * 16, :], 1, 0) for c in range(4)]
    dbs = dbs + jnp.concatenate(zdb, axis=0)
    for j in range(8):
        xf[pl.ds(j, 64, stride=8), :] = dbs[:, j * 128 : (j + 1) * 128]
    for c in range(4):
        tx[c // 2, c % 2, 16:32] = xf[c * 128 : (c + 1) * 128, :].astype(BF).reshape(16, 8, 128)

    def give(slot, k_, q_, to, back, near):
        c = remote(tx.at[k_, :, slot], g_in.at[q_, z, x], r4s, r4r.at[back], to)
        if near:
            pl.when(jnp.logical_not((to[0] == head) & (to[1] == grp)))(c.start)
        else:
            c.start()

    his_a = [rem(p + 1 - par, 2) for par in range(2)]
    for dz in NEAR:
        for xh in range(2):
            for dk in range(2):
                slot = 16 + xh * 8 + zs[dz]
                to = (32 + xh * 16 + zs[dz] * 2 + lo, hi * 2 + ks[dk])
                give(slot, ks[dk], k, to, (8 - dz) % 8, dz == 0)

        @pl.when(div(zs[dz], 4) == k)
        def _(dz=dz):
            for par in range(2):
                for q in range(2):
                    for dk in range(2):
                        slot = (rem(zs[dz], 4) * 2 + par) * 2 + q
                        to = (hi * 16 + zs[dz] * 2 + 1 - par, his_a[par] * 2 + ks[dk])
                        give(slot, ks[dk], q, to, (8 - dz) % 8, dz == 0)

    for q in range(2):

        @pl.when(mine[q])
        def _(q=q):
            g_in[q, z, x] = tx[k, :, slots[q]]

    for dz in NEAR:
        if dz:
            drain(like.at[pl.ds(0, 8)], r4r.at[dz])
        else:
            for n in range(3):

                @pl.when(n_self == n)
                def _(n=n):
                    drain(like.at[pl.ds(0, 8 - n)], r4r.at[0])

        part, spot = g_in.at[:, zs[dz]], d_in.at[k, p, :, zs[dz]]
        pl.when(moves)(remote(part, spot, r5s, r5r.at[1, dz], n2).start)
        pl.when(moves)(remote(part, spot, r5s, r5r.at[0, dz], n1).start)
        pl.when(stays)(remote(part, spot, r5s, r5r.at[0, dz], across).start)

    @pl.when(stays)
    def _():
        d_in[k, p] = g_in[...]

    for dz in NEAR:
        region = d_in.at[k, :, :, zs[dz]]
        one = d_in.at[k, 0, :, zs[dz]]
        drain(one, r5r.at[0, dz])
        pl.when(moves)(pltpu.make_async_copy(one, one, r5r.at[1, dz]).wait)
        remote(region, region, r6s, r6r, partner).start()
    turn = [rem(zn - z + 14, 8) * 16 for zn in range(8)]
    peers = [(xs[o // 2], los[o % 2], (xz16[o // 2][0] + los[o % 2], grp)) for o in range(8)]
    for half in range(2):
        if half:
            drain(d_in.at[1 - k], r6r)
        row = pl.multiple_of(ks[half] * 128, 128)
        for p_ in range(2):
            xd = d_in[ks[half], p_].astype(F32).reshape(1024, 128)
            ft[0] = xd[0:512]
            ft[1] = xd[512:1024]
            for j in range(16):
                dn[pl.ds(row + p_ * 64, 64), j * 128 : (j + 1) * 128] = ft[
                    j // 8, pl.ds(j % 8, 64, stride=8), :
                ].astype(BF)
        for i in range(4):
            part = mm(w[i * 256 : (i + 1) * 256, :], dn[pl.ds(row, 128), :], 1, 1).astype(BF)
            for l_ in range(2):
                for zn in range(8):
                    at = l_ * 128 + zn * 16
                    hb[half, i, l_, pl.ds(pl.multiple_of(turn[zn], 16), 16), :] = part[at : at + 16]
        for h in range(2):
            rows = pl.ds(h * 64, 64)
            for o in (4, 5, 2, 3, 6, 7, 1):
                x_, lo_, to = peers[o]
                src = hb.at[half, x_, lo_, rows]
                remote(src, a1.at[half, o, rows], p1s, p1r.at[half, h], to).start()
    co.append(pltpu.make_async_copy(dn, dn_o, so.at[1]))
    co[1].start()
    for h in range(2):
        rows = pl.ds(h * 64, 64)
        for half in range(2):
            acc = hb[half, x, lo, rows, :].astype(F32)
            drain(a1.at[half, pl.ds(1, 7), rows], p1r.at[half, h])
            for o in range(1, 8):
                acc = acc + a1[half, o, rows, :].astype(F32)
            a1s[rows, pl.ds(pl.multiple_of(ks[half] * 128, 128), 128)] = acc.astype(BF)
        for t in ((2, 1, 3, 0), (4, 7, 5, 6))[h]:
            dz = (t + 2) % 8
            if dz:
                remote(a1s.at[pl.ds(t * 16, 16)], a2.at[dz], p2s, p2r, (xz16[0][dz] + lo, grp)).start()
    total = a1s[96:112, :].astype(F32)
    drain(a2.at[pl.ds(1, 7)], p2r)
    for dz in range(1, 8):
        total = total + a2[dz].astype(F32)
    base = pl.multiple_of(x * 256 + lo * 128, 128)
    row0 = pl.multiple_of(base + z * 16, 16)
    total = jnp.where(hidt[pl.ds(row0, 16), :].astype(F32) > 0, total, 0.0)
    big = total.astype(BF)
    small = (total - big.astype(F32)).astype(BF)
    piece = mm(big, chosen_s[...], 1, 0) + mm(small, chosen_s[...], 1, 0)
    ag[pl.ds(row0, 16), :] = piece.astype(BF)
    cd = {}
    own_rows = ag.at[pl.ds(row0, 16)]
    for dz in FAR[:7]:
        cd[dz] = remote(own_rows, own_rows, p3s, p3r.at[dz], (xz16[0][dz] + lo, grp))
        cd[dz].start()
    for dz in (0, 1, 7, 2, 6, 3, 5, 4):
        if dz:
            cd[dz].wait_recv()
        rows = ag.at[pl.ds(pl.multiple_of(base + zs[(8 - dz) % 8] * 16, 16), 16)]
        for o in (4, 5, 2, 3, 6, 7, 1):
            remote(rows, rows, p4s, p4r.at[o], peers[o][2]).start()
    def leave(x_, lo_):
        rows = pl.ds(pl.multiple_of(x_ * 256 + lo_ * 128, 128), 128)
        c = pltpu.make_async_copy(ag.at[rows], ag_o.at[rows], so.at[2])
        c.start()

    leave(x, lo)
    for o in (1, 2, 6, 3, 7, 4, 5):
        drain(a1s, p4r.at[o])
        x_, lo_, _ = peers[8 - 2 * (o // 2) + o % 2 if o > 1 else o]
        leave(x_, lo_)
    co.append(pltpu.make_async_copy(ag, ag_o, so.at[2]))

    drain(fr, r1s)
    pl.when(stays)(pltpu.make_async_copy(r2.at[0], r2.at[0], r2s).wait)
    pl.when(moves)(pltpu.make_async_copy(r2, r2, r2s).wait)
    drain(gq, gs.at[0])
    drain(na, gs.at[1])
    drain(nb, gs.at[2])
    drain(nd, gs.at[3])
    drain(er.at[pl.ds(1, 3)], e1s)
    drain(er.at[pl.ds(1, 3)], e2s)
    pl.when(stays)(pltpu.make_async_copy(g_in, g_in, r5s).wait)
    pl.when(moves)(pltpu.make_async_copy(d_in.at[0], d_in.at[0], r5s).wait)
    drain(d_in.at[0], r6s)
    drain(a1.at[:, pl.ds(1, 7)], p1s)
    drain(a2.at[pl.ds(1, 7)], p2s)
    drain(a2.at[pl.ds(1, 7)], p3s)
    drain(a1.at[:, pl.ds(1, 7)], p4s)
    wait_all(r3s)
    wait_all(r4s)
    for c in co:
        c.wait()


def local(client_ids, client_table, in_weight, in_bias, head_weight, tokens, labels, byte_table, out_table):
    hbm = pl.BlockSpec(memory_space=pl.ANY)
    dma = pltpu.SemaphoreType.DMA
    V = pltpu.VMEM
    S = jax.ShapeDtypeStruct
    ag, dn, hidt, losses = pl.pallas_call(
        kernel,
        out_shape=(S((1024, 256), BF), S((256, 2048), BF), S((1024, 256), BF), S((1,), F32)),
        in_specs=[hbm] * 9,
        out_specs=(hbm, hbm, hbm, pl.BlockSpec(memory_space=pltpu.SMEM)),
        scratch_shapes=[
            V((1, 256), jnp.int32),
            V((1, 1024), F32),
            V((1, 256), jnp.int32),
            V((1, 256), jnp.int32),
            V((1024, 256), BF),
            V((256, 1024), BF),
            V((256, 1024), BF),
            V((256, 1024), BF),
            V((1024, 2048), BF),
            V((256, 1024), BF),
            V((2, 2, 8, 8, 2048), F32),
            V((2, 8, 8, 2048), F32),
            V((2, 8, 8, 2048), BF),
            V((2, 8, 8, 2048), BF),
            V((2, 512, 128), F32),
            V((2, 8, 4, 2, 8, 128), BF),
            V((2, 2, 32, 8, 128), BF),
            V((64, 1024), BF),
            V((64, 1024), BF),
            V((512, 128), F32),
            V((256, 1024), BF),
            V((768, 256), F32),
            V((768, 256), F32),
            V((256, 256), F32),
            V((512, 256), BF),
            V((256, 256), F32),
            V((512, 256), BF),
            V((8, 256), F32),
            V((8, 256), F32),
            V((4, 64, 256), BF),
            V((4, 64, 256), BF),
            V((64, 256), BF),
            V((4, 64, 256), BF),
            V((128, 128), F32),
            V((2, 2, 32, 8, 128), BF),
            V((2, 8, 4, 2, 8, 128), BF),
            V((2, 2, 2, 8, 4, 2, 8, 128), BF),
            V((256, 2048), BF),
            V((2, 4, 2, 128, 128), BF),
            V((2, 8, 128, 128), BF),
            V((128, 256), BF),
            V((8, 16, 256), BF),
            V((1024, 256), BF),
            V((1024, 256), BF),
            V((256, 256), BF),
            V((64, 2, 8, 128), BF),
            pltpu.SemaphoreType.REGULAR, pltpu.SemaphoreType.REGULAR,
            dma((8,)), dma((CH,)), dma((3,)),
            dma(()), dma((2, 8)),
            dma(()), dma((2, 2, 8)),
            dma((4,)), dma((8,)),
            dma(()), dma(()),
            dma(()), dma(()), dma(()), dma(()),
            dma(()), dma((8,)),
            dma(()), dma((2, 8)), dma(()), dma(()),
            dma(()), dma((2, 2)), dma(()), dma(()),
            dma(()), dma((8,)), dma(()), dma((8,)),
        ],
        compiler_params=pltpu.CompilerParams(
            collective_id=0, has_side_effects=True, vmem_limit_bytes=60 * 1024 * 1024
        ),
        name="round",
    )(
        client_ids.reshape(1, 256), client_table, in_weight, in_bias.reshape(1, 1024), head_weight,
        tokens, labels, byte_table, out_table,
    )
    head_grad, in_grad = pl.pallas_call(
        tail_kernel,
        out_shape=(S((1024, 2048), BF), S((256, 1024), F32)),
        in_specs=[hbm] * 3,
        out_specs=(hbm, hbm),
        scratch_shapes=[
            V((1024, 256), BF), V((256, 2048), BF), V((1024, 256), BF),
            V((1024, 2048), BF), V((256, 1024), F32),
            dma((7,)), dma((6,)),
        ],
        compiler_params=pltpu.CompilerParams(vmem_limit_bytes=60 * 1024 * 1024),
        name="tail",
    )(hidt, dn, ag)
    return head_grad, in_grad, losses


def solution(mesh):
    placed = (
        P(),
        P(),
        P(None, "client"),
        P("client"),
        P("client", "head"),
        P(("head", "client"), None),
        P(("head", "client"), None),
        P(None, "client"),
        P(None, "client"),
    )
    return jax.shard_map(
        local,
        mesh=mesh,
        in_specs=placed,
        out_specs=(P("client", "head"), P(None, "client"), P(("head", "client"))),
        check_vma=False,
    )
```
